32 devices in a mesh: member: 2 (over y), slab: 4 (over z), chan: 2 (over x), mode: 2 (over core).
Axes of the slice: x: 2, y: 2, z: 4, core: 2. Of those that a mesh axis runs over, the one named last changes fastest.
Arguments:
- source_field: float32 [128, 1024, 1024], P(('member', 'chan'), 'slab', 'mode'), parts along dimension 0, may hold values from -6 to 6
- cotangent: float32 [128, 1024, 1024], P(('member', 'chan'), 'slab', 'mode'), parts along dimension 0, may hold values from -6 to 6
- spectral_weight: float32 [128, 64, 32, 2, 64], P(('member', 'chan'), None, 'mode', None, 'slab'), parts along dimension 0, may hold values from -12 to 12
- skip_gain: float32 [128], P(('member', 'chan')), parts along dimension 0, may hold values from 0.5 to 2
- channel_bias: float32 [128], P(('member', 'chan')), parts along dimension 0, may hold values from -0.5 to 0.5
- mode_limit: int32 [128, 2], P('member'), parts along dimension 0, may hold values from 16 to 32
- width_limit: int32 [128], P('member'), parts along dimension 0, may hold values from 32 to 64
Outputs:
- output: float32 [128, 1024, 1024], P(('member', 'chan'), 'slab', 'mode'), parts along dimension 0
- field_grad: float32 [128, 1024, 1024], P(('member', 'chan'), 'slab', 'mode'), parts along dimension 0
- spectral_grad: float32 [128, 64, 32, 2, 64], P(('member', 'chan'), None, 'mode', None, 'slab'), parts along dimension 0
- gate_grad: float32 [128], P(('member', 'chan')), parts along dimension 0
- bias_grad: float32 [128], P(('member', 'chan')), parts along dimension 0
The draws below stay inside these ranges and needn't reach their ends.
There are 2 independent parts, one for each index of `member`. The reference program is written for one: setup_inputs(seed, part) draws one part's arguments, and reference() takes and returns one part's arrays. A program takes and returns all parts, laid end to end along the dimension named above; each array names one. Nothing has to cross between parts.
Inputs may be any that keep to these rules, and one draw needn't show every extreme that they name: `mode_limit`: never more than 32. `width_limit`: never more than 64.
All inputs are finite; a program needn't handle non-finite values.
Results may differ from the reference program's by a relative error of at most 0.00018.
Values sent between devices are 32-bit elements; how exact they have to be, the bound alone decides.
A program may use at most 192 MiB of HBM per device.

```python
import math
import jax
import jax.numpy as jnp
from jax import lax

C = 64
H = 1024
W = 1024
M = 32
KX = 64


def plant(values, stream_key, low, high):
    longest = values.shape.index(max(values.shape))
    spots = []
    for shift in (0, 1):
        where = [jax.random.randint(jax.random.fold_in(stream_key, axis), (), 0, length) for axis, length in enumerate(values.shape)]
        where[longest] = (where[longest] + shift) % values.shape[longest]
        spots.append(tuple(where))
    return values.at[spots[0]].set(low).at[spots[1]].set(high)


def levels(rng, shape, split, least, largest):
    factor_of = 1.0
    for dim, parts in split:
        steps = jax.random.uniform(jax.random.fold_in(jax.random.fold_in(rng, 6), dim), (parts,), jnp.float32, least / len(split), largest / len(split))
        factor_of = factor_of * jnp.repeat(jnp.exp(steps), shape[dim] // parts).reshape((-1,) + (1,) * (len(shape) - 1 - dim))
    return factor_of


def scatter_about(rng, dims, width, most, pieces=(), kind=jnp.bfloat16):
    entries = jax.random.normal(rng, dims, jnp.float32) * width
    if len(pieces) > 0:
        entries = levels(rng, dims, pieces, -0.22, 0.18) * entries
    return jnp.clip(entries, min=-most, max=most).astype(kind)


def setup_inputs(seed: int = 0, part: int = 0) -> dict:
    seeds = jax.random.split(jax.random.key(seed), 8)
    part_keys = jax.random.split(jax.random.fold_in(seeds[7], part), 8)
    return {
        "source_field": scatter_about(part_keys[0], (C, H, W), 1.0, 6.0, ((0, 2), (1, 4), (2, 2)), jnp.float32),
        "cotangent": scatter_about(part_keys[1], (C, H, W), 1.0, 6.0, ((0, 2), (1, 4), (2, 2)), jnp.float32),
        "spectral_weight": scatter_about(part_keys[2], (C, C, M, 2, KX), 2.0, 12.0, ((0, 2), (2, 2), (4, 4)), jnp.float32),
        "skip_gain": jnp.clip(jnp.exp(math.log(2.0) - 1.3862944 * jax.random.uniform(part_keys[3], (C,), jnp.float32) ** levels(part_keys[3], (C,), ((0, 2),), -0.2, 0.2)), 0.5, 2.0),
        "channel_bias": jnp.clip(jax.random.uniform(part_keys[4], (C,), jnp.float32, -0.5, 0.5) * levels(part_keys[4], (C,), ((0, 2),), -0.4, 0.0), -0.5, 0.5),
        "mode_limit": plant(jax.random.randint(part_keys[5], (C, 2), M // 2, M + 1), jax.random.fold_in(part_keys[5], 1), M // 2, M).astype(jnp.int32),
        "width_limit": plant(jax.random.randint(part_keys[6], (C,), C // 2, C + 1), jax.random.fold_in(part_keys[6], 1), C // 2, C).astype(jnp.int32),
    }


precise = lax.Precision.HIGHEST

def column_table(extent, freq_count, first_cell, cell_count):
    cell_index = first_cell + jnp.arange(cell_count, dtype=jnp.int32)
    wave_index = jnp.arange(freq_count, dtype=jnp.int32)
    products = (cell_index[:, None] * wave_index[None, :] % extent).astype(jnp.float32)
    angles = products * (2.0 * math.pi / extent)
    return jnp.stack([jnp.cos(angles), -jnp.sin(angles)], axis=-1).reshape(cell_count, 2 * freq_count)

def row_tables(extent, freq_count, first_cell, cell_count):
    cell_index = first_cell + jnp.arange(cell_count, dtype=jnp.int32)
    column = jnp.arange(2 * freq_count, dtype=jnp.int32)
    wave_index = (column + jnp.where(column >= freq_count, extent - 2 * freq_count, 0)).astype(jnp.int32)
    products = (cell_index[:, None] * wave_index[None, :] % extent).astype(jnp.float32)
    angles = products * (2.0 * math.pi / extent)
    return (jnp.cos(angles), jnp.sin(angles))

def spectrum(values, column_tab, row_cos, row_sin):
    channels, row_count, col_count = values.shape
    freq_count = column_tab.shape[1] // 2
    halves = jnp.einsum('chw,wk->chk', values, column_tab, precision=precise).reshape(channels, row_count, freq_count, 2)
    real_part = halves[..., 0]
    imag_part = halves[..., 1]
    out_real = jnp.einsum('chy,hx->cyx', real_part, row_cos, precision=precise) + jnp.einsum('chy,hx->cyx', imag_part, row_sin, precision=precise)
    out_imag = jnp.einsum('chy,hx->cyx', imag_part, row_cos, precision=precise) - jnp.einsum('chy,hx->cyx', real_part, row_sin, precision=precise)
    return jnp.stack([out_real, out_imag], axis=2)

def synthesis(modes_in, column_tab, row_cos, row_sin):
    channels = modes_in.shape[0]
    real_part = modes_in[:, :, 0]
    imag_part = modes_in[:, :, 1]
    back_real = jnp.einsum('cyx,hx->cyh', real_part, row_cos, precision=precise) - jnp.einsum('cyx,hx->cyh', imag_part, row_sin, precision=precise)
    back_imag = jnp.einsum('cyx,hx->cyh', real_part, row_sin, precision=precise) + jnp.einsum('cyx,hx->cyh', imag_part, row_cos, precision=precise)
    joined = jnp.stack([back_real, back_imag], axis=2).reshape(channels, -1, row_cos.shape[0])
    return jnp.einsum('ckh,wk->chw', joined, column_tab, precision=precise)

def contract(spectra, weight):
    spec_real = spectra[:, :, 0]
    spec_imag = spectra[:, :, 1]
    weight_real = weight[:, :, :, 0]
    weight_imag = weight[:, :, :, 1]
    out_real = jnp.einsum('iyx,ioyx->oyx', spec_real, weight_real, precision=precise) - jnp.einsum('iyx,ioyx->oyx', spec_imag, weight_imag, precision=precise)
    out_imag = jnp.einsum('iyx,ioyx->oyx', spec_real, weight_imag, precision=precise) + jnp.einsum('iyx,ioyx->oyx', spec_imag, weight_real, precision=precise)
    return jnp.stack([out_real, out_imag], axis=2)

def contract_back(grads, weight):
    grad_real = grads[:, :, 0]
    grad_imag = grads[:, :, 1]
    weight_real = weight[:, :, :, 0]
    weight_imag = weight[:, :, :, 1]
    back_real = jnp.einsum('oyx,ioyx->iyx', grad_real, weight_real, precision=precise) + jnp.einsum('oyx,ioyx->iyx', grad_imag, weight_imag, precision=precise)
    back_imag = jnp.einsum('oyx,ioyx->iyx', grad_imag, weight_real, precision=precise) - jnp.einsum('oyx,ioyx->iyx', grad_real, weight_imag, precision=precise)
    return jnp.stack([back_real, back_imag], axis=2)

def outer_grad(spectra, grads):
    spec_real = spectra[:, :, 0]
    spec_imag = spectra[:, :, 1]
    grad_real = grads[:, :, 0]
    grad_imag = grads[:, :, 1]
    real_side = jnp.einsum('iyx,oyx->ioyx', spec_real, grad_real) + jnp.einsum('iyx,oyx->ioyx', spec_imag, grad_imag)
    imag_side = jnp.einsum('iyx,oyx->ioyx', spec_real, grad_imag) - jnp.einsum('iyx,oyx->ioyx', spec_imag, grad_real)
    return jnp.stack([real_side, imag_side], axis=3)

def mode_weights(limit_rows, col_freq, row_freq, kx_count, cells_total):
    keep_cols = col_freq[None, :] < limit_rows[:, 0:1]
    keep_rows = (row_freq[None, :] < limit_rows[:, 1:2]) | ((kx_count - row_freq)[None, :] < limit_rows[:, 1:2])
    scales = jnp.where(col_freq == 0, 1.0, 2.0).astype(jnp.float32) / cells_total
    joined = keep_cols[:, :, None] & keep_rows[:, None, :]
    return (joined.astype(jnp.float32) * scales[None, :, None])[:, :, None, :]

def read_mask(in_index, width_limit):
    return (in_index[:, None] < width_limit[None, :]).astype(jnp.float32)[:, :, None, None, None]

def reference(source_field, cotangent, spectral_weight, skip_gain, channel_bias, mode_limit, width_limit):
    channels, row_count, col_count = source_field.shape
    freq_count = spectral_weight.shape[2]
    kx_count = spectral_weight.shape[4]
    column_tab = column_table(col_count, freq_count, 0, col_count)
    row_cos, row_sin = row_tables(row_count, freq_count, 0, row_count)
    weights = mode_weights(mode_limit, jnp.arange(freq_count, dtype=jnp.int32), jnp.arange(kx_count, dtype=jnp.int32), kx_count, row_count * col_count)
    reads = read_mask(jnp.arange(channels, dtype=jnp.int32), width_limit)
    masked_weight = spectral_weight * reads
    spectra = spectrum(source_field, column_tab, row_cos, row_sin)
    out_modes = contract(spectra, masked_weight) * weights
    branch = synthesis(out_modes, column_tab, row_cos, row_sin)
    skip_scale = skip_gain[:, None, None]
    summed = branch + skip_scale * source_field + channel_bias[:, None, None]
    output, gelu_back = jax.vjp(jax.nn.gelu, summed)
    grad_sum = gelu_back(cotangent)[0]
    grad_modes = spectrum(grad_sum, column_tab, row_cos, row_sin) * weights
    spectral_grad = outer_grad(spectra, grad_modes) * reads
    field_grad = synthesis(contract_back(grad_modes, masked_weight), column_tab, row_cos, row_sin) + skip_scale * grad_sum
    gate_grad = lax.optimization_barrier(jnp.sum(grad_sum * source_field, axis=(1, 2)))
    bias_grad = lax.optimization_barrier(jnp.sum(grad_sum, axis=(1, 2)))
    return (output, field_grad, spectral_grad, gate_grad, bias_grad)
```

```python
import functools
import math

import jax
import jax.numpy as jnp
import ml_dtypes
import numpy as np
from jax import lax
from jax.experimental import pallas as pl
from jax.experimental.pallas import tpu as pltpu
from jax.sharding import PartitionSpec as P

LANES = 128
BIG = 60 * 1024 * 1024


def split_table(table):
    high = lax.reduce_precision(table, 8, 7)
    return high.astype(jnp.bfloat16), (table - high).astype(jnp.bfloat16)


def split_block(values):
    high = values.astype(jnp.bfloat16)
    return high, (values - high.astype(jnp.float32)).astype(jnp.bfloat16)


def dot_pair(left, right):
    left_high, left_low = left
    right_high, right_low = right
    mul = functools.partial(jnp.dot, preferred_element_type=jnp.float32)
    return mul(left_high, right_high) + mul(left_low, right_high) + mul(left_high, right_low)


def tables(extent, waves, first_cell, cell_count):
    cell_index = first_cell + jnp.arange(cell_count, dtype=jnp.int32)
    products = (cell_index[:, None] * waves[None, :] % extent).astype(jnp.float32)
    angles = products * (2.0 * math.pi / extent)
    return jnp.cos(angles), jnp.sin(angles)


def store_spectrum(values, col_pair, row_pair, out_ref):
    block, rows, cols = values.shape
    lines = dot_pair(split_block(values.reshape(block * rows, cols)), col_pair)
    all_kx = row_pair[0].shape[0] // 2
    kx, lanes = out_ref.shape[2:]
    span = lanes // block
    mode_count = lines.shape[1] // span
    slabs = out_ref.shape[0] // mode_count
    done = []
    for c in range(block):
        mixed = dot_pair(row_pair, split_block(lines[c * rows : (c + 1) * rows]))
        done.append(mixed[:all_kx] - turn(mixed[all_kx:], span))
    for m in range(mode_count):
        packed = jnp.concatenate([one[:, m * span : (m + 1) * span] for one in done], axis=1)
        for s in range(slabs):
            out_ref[m * slabs + s, 0] = packed[s * kx : (s + 1) * kx]


def turn(values, span):
    half = span // 2
    pieces = []
    for first in range(0, values.shape[1], span):
        pieces.append(-values[:, first + half : first + span])
        pieces.append(values[:, first : first + half])
    return jnp.concatenate(pieces, axis=1)


def all_modes(modes_ref, mode_count, c, block):
    span = modes_ref.shape[3] // block
    slabs = modes_ref.shape[0] // mode_count
    columns = []
    for m in range(mode_count):
        stack = [modes_ref[m * slabs + s, 0] for s in range(slabs)]
        columns.append(jnp.concatenate(stack, axis=0)[:, c * span : (c + 1) * span])
    return jnp.concatenate(columns, axis=1), span


def synth(modes_and_span, row_pair, col_pair):
    modes, span = modes_and_span
    stacked = jnp.concatenate([modes, turn(modes, span)], axis=0)
    lines = dot_pair(row_pair, split_block(stacked))
    return dot_pair(split_block(lines), col_pair)


def spectrum_kernel(x_ref, ch_ref, cl_ref, rh_ref, rl_ref, out_ref):
    store_spectrum(x_ref[...], (ch_ref[...], cl_ref[...]), (rh_ref[...], rl_ref[...]), out_ref)


def middle_kernel(
    mode_count, x_ref, cot_ref, modes_ref, gain_ref, bias_ref, ch_ref, cl_ref, rh_ref, rl_ref,
    cth_ref, ctl_ref, ih_ref, il_ref, out_ref, grad_ref, spec_ref, sums_ref,
):
    block = x_ref.shape[0]
    row_back = (ih_ref[...], il_ref[...])
    col_back = (cth_ref[...], ctl_ref[...])
    scale = math.sqrt(2.0 / math.pi)
    for c in range(block):
        source = x_ref[c]
        gain = gain_ref[c]
        v = synth(all_modes(modes_ref, mode_count, c, block), row_back, col_back) + gain[:, :1] * source + bias_ref[c][:, :1]
        square = v * v
        t = jnp.tanh(scale * v * (1.0 + 0.044715 * square))
        half_up = 0.5 * (1.0 + t)
        out_ref[c] = v * half_up
        slope = half_up + 0.5 * v * (1.0 - t * t) * (scale * (1.0 + 3.0 * 0.044715 * square))
        grad = cot_ref[c] * slope
        grad_ref[c] = grad
        gate = jnp.sum(jnp.sum(grad * source, axis=0, keepdims=True), axis=1, keepdims=True)
        bias = jnp.sum(jnp.sum(grad, axis=0, keepdims=True), axis=1, keepdims=True)
        lane = lax.broadcasted_iota(jnp.int32, (1, LANES), 1)
        sums_ref[c] = jnp.where(lane == 0, gate, bias)
    store_spectrum(
        grad_ref[...], (ch_ref[...], cl_ref[...]), (rh_ref[...], rl_ref[...]), spec_ref
    )


def last_kernel(mode_count, grad_ref, modes_ref, gain_ref, cth_ref, ctl_ref, ih_ref, il_ref, out_ref):
    block = grad_ref.shape[0]
    for c in range(block):
        modes = all_modes(modes_ref, mode_count, c, block)
        branch = synth(modes, (ih_ref[...], il_ref[...]), (cth_ref[...], ctl_ref[...]))
        out_ref[c] = branch + gain_ref[c][:, :1] * grad_ref[c]


def contract_kernel(w_ref, spec_ref, limit_ref, out_ref):
    block, freqs, _, kx, outs = w_ref.shape
    first = lax.axis_index("chan") * (block * pl.num_programs(0)) + pl.program_id(0) * block

    @pl.when(pl.program_id(0) == 0)
    def _():
        out_ref[...] = jnp.zeros_like(out_ref)

    limit = limit_ref[...]
    for y in range(freqs):
        real = out_ref[y, 0]
        imag = out_ref[y, 1]
        for i in range(block):
            keep = first + i < limit
            spec = spec_ref[0]
            at = 2 * freqs * i + y
            s_real = jnp.where(keep, spec[:, at : at + 1], 0.0)
            s_imag = jnp.where(keep, spec[:, freqs + at : freqs + at + 1], 0.0)
            w_real = w_ref[i, y, 0]
            w_imag = w_ref[i, y, 1]
            real = real + (s_real * w_real - s_imag * w_imag)
            imag = imag + (s_real * w_imag + s_imag * w_real)
        out_ref[y, 0] = real
        out_ref[y, 1] = imag


def back_kernel(w_ref, spec_ref, grads_ref, limit_ref, wgrad_ref, out_ref):
    block, freqs, _, kx, outs = w_ref.shape
    first = lax.axis_index("chan") * (block * pl.num_programs(0)) + pl.program_id(0) * block
    limit = limit_ref[...]
    lane = lax.broadcasted_iota(jnp.int32, out_ref.shape[1:], 1)
    spec = spec_ref[0]
    back = jnp.zeros(out_ref.shape[1:], jnp.float32)
    for i in range(block):
        keep = first + i < limit
        for y in range(freqs):
            at = 2 * freqs * i + y
            g_real = jnp.where(keep, grads_ref[y, 0], 0.0)
            g_imag = jnp.where(keep, grads_ref[y, 1], 0.0)
            s_real = spec[:, at : at + 1]
            s_imag = spec[:, freqs + at : freqs + at + 1]
            wgrad_ref[i, y, 0] = s_real * g_real + s_imag * g_imag
            wgrad_ref[i, y, 1] = s_real * g_imag - s_imag * g_real
            w_real = w_ref[i, y, 0]
            w_imag = w_ref[i, y, 1]
            b_real = jnp.sum(g_real * w_real + g_imag * w_imag, axis=1, keepdims=True)
            b_imag = jnp.sum(g_imag * w_real - g_real * w_imag, axis=1, keepdims=True)
            back = jnp.where(lane == at, b_real, back)
            back = jnp.where(lane == freqs + at, b_imag, back)
    out_ref[0] = back


def exchange_kernel(axes, sizes, gather, x_ref, out_ref, send_sem, recv_sem, own_sem):
    total = math.prod(sizes)
    me = lax.axis_index(axes[0])
    for axis, size in zip(axes[1:], sizes[1:]):
        me = me * size + lax.axis_index(axis)

    def place(index):
        coords = {}
        for axis, size in reversed(list(zip(axes, sizes))):
            coords[axis] = lax.rem(index, size)
            index = lax.div(index, size)
        return coords

    barrier = pltpu.get_barrier_semaphore()
    for step in range(1, total):
        pl.semaphore_signal(
            barrier, inc=1, device_id=place(lax.rem(me + step, total)),
            device_id_type=pl.DeviceIdType.MESH,
        )
    pl.semaphore_wait(barrier, total - 1)
    copies = []
    for step in range(1, total):
        peer = lax.rem(me + step, total)
        copy = pltpu.make_async_remote_copy(
            src_ref=x_ref if gather else x_ref.at[peer],
            dst_ref=out_ref.at[me],
            send_sem=send_sem.at[step],
            recv_sem=recv_sem.at[step],
            device_id=place(peer),
            device_id_type=pl.DeviceIdType.MESH,
        )
        copy.start()
        copies.append(copy)
    own = pltpu.make_async_copy(x_ref if gather else x_ref.at[me], out_ref.at[me], own_sem)
    own.start()
    own.wait()
    for copy in copies:
        copy.wait()


def exchange(values, axes, gather, ident):
    sizes = tuple(lax.axis_size(axis) for axis in axes)
    total = math.prod(sizes)
    piece = values.shape if gather else values.shape[1:]
    flat = values.reshape((-1, LANES) if gather else (total, -1, LANES))
    out = pl.pallas_call(
        functools.partial(exchange_kernel, axes, sizes, gather),
        out_shape=jax.ShapeDtypeStruct((total,) + flat.shape[-2:], jnp.float32),
        in_specs=[pl.BlockSpec(memory_space=pltpu.VMEM)],
        out_specs=pl.BlockSpec(memory_space=pltpu.VMEM),
        scratch_shapes=[
            pltpu.SemaphoreType.DMA((total,)),
            pltpu.SemaphoreType.DMA((total,)),
            pltpu.SemaphoreType.DMA,
        ],
        compiler_params=pltpu.CompilerParams(collective_id=ident, has_side_effects=True),
        name="exchange" + str(ident),
    )(flat)
    return out.reshape((total,) + piece)


def mode_weights(limit_rows, col_freq, row_freq, kx_count, cells_total):
    keep_cols = col_freq[None, :] < limit_rows[:, 0:1]
    keep_rows = (row_freq[None, :] < limit_rows[:, 1:2]) | (
        (kx_count - row_freq)[None, :] < limit_rows[:, 1:2]
    )
    scales = jnp.where(col_freq == 0, 1.0, 2.0).astype(jnp.float32) / cells_total
    joined = keep_rows[:, :, None] & keep_cols[:, None, :]
    return (joined.astype(jnp.float32) * scales[None, None, :])[:, :, None, :]


def local_plain(
    source_field, cotangent, spectral_weight, skip_gain, channel_bias, mode_limit, width_limit
):
    channels, row_count, col_count = source_field.shape
    slabs = lax.axis_size("slab")
    modes = lax.axis_size("mode")
    chans = lax.axis_size("chan")
    slab_index = lax.axis_index("slab")
    mode_index = lax.axis_index("mode")
    chan_index = lax.axis_index("chan")
    outs = spectral_weight.shape[1]
    freqs = spectral_weight.shape[2]
    kx = spectral_weight.shape[4]
    all_freqs = freqs * modes
    all_kx = kx * slabs
    all_rows = row_count * slabs
    all_cols = col_count * modes

    col_waves = jnp.arange(all_freqs, dtype=jnp.int32)
    row_waves = jnp.arange(all_kx, dtype=jnp.int32)
    row_waves = row_waves + jnp.where(2 * row_waves >= all_kx, all_rows - all_kx, 0)
    col_cos, col_sin = tables(all_cols, col_waves, mode_index * col_count, col_count)
    row_cos, row_sin = tables(all_rows, row_waves, slab_index * row_count, row_count)
    col_tab = jnp.stack(
        [col_cos.reshape(-1, modes, freqs), -col_sin.reshape(-1, modes, freqs)], axis=2
    ).reshape(col_count, 2 * all_freqs)
    row_tab = jnp.concatenate([row_cos, row_sin], axis=1)
    col_pair = split_table(col_tab)
    col_back = tuple(part.T for part in col_pair)
    row_back = split_table(row_tab)
    row_pair = tuple(part.T for part in row_back)

    block = LANES // (2 * freqs)
    groups = channels // block
    owners = slabs * modes
    cells = pl.BlockSpec((block, row_count, col_count), lambda c: (c, 0, 0))
    freq_cells = pl.BlockSpec((owners, 1, kx, LANES), lambda c: (0, c, 0, 0))
    per_channel = pl.BlockSpec((block, 1, LANES), lambda c: (c, 0, 0))
    field = jax.ShapeDtypeStruct(source_field.shape, jnp.float32)
    freq_field = jax.ShapeDtypeStruct((owners, groups, kx, LANES), jnp.float32)
    params = pltpu.CompilerParams(
        dimension_semantics=("arbitrary",), vmem_limit_bytes=BIG
    )

    def whole(array):
        return pl.BlockSpec(array.shape, lambda c: (0,) * array.ndim)

    grid = (channels // block,)
    wide = lambda values: jnp.broadcast_to(values[:, None, None], (channels, 1, LANES))
    gain = wide(skip_gain)
    forward = col_pair + row_pair
    back = col_back + row_back

    def spread(partial, ident):
        half = exchange(partial.reshape(modes, -1, LANES), ("mode",), False, ident)
        half = jnp.sum(half, axis=0).reshape(slabs, -1, LANES)
        return jnp.sum(exchange(half, ("slab",), False, ident + 1), axis=0).reshape(
            groups, kx, LANES
        )

    def joined(piece, ident):
        half = exchange(piece, ("slab",), True, ident)
        return exchange(half, ("mode",), True, ident + 1).reshape((owners,) + piece.shape)

    spectra = spread(
        pl.pallas_call(
            spectrum_kernel,
            grid=grid,
            in_specs=[cells] + [whole(t) for t in forward],
            out_specs=freq_cells,
            out_shape=freq_field,
            compiler_params=params,
            name="spectrum",
        )(source_field, *forward),
        0,
    )

    weight = spectral_weight.transpose(0, 2, 3, 4, 1)
    limit = width_limit.reshape(1, outs)
    in_block = block
    w_spec = pl.BlockSpec((in_block, freqs, 2, kx, outs), lambda i: (i, 0, 0, 0, 0))
    s_spec = pl.BlockSpec((1, kx, LANES), lambda i: (i, 0, 0))
    mode_spec = pl.BlockSpec((freqs, 2, kx, outs), lambda i: (0, 0, 0, 0))
    limit_spec = pl.BlockSpec((1, outs), lambda i: (0, 0))
    partial_modes = pl.pallas_call(
        contract_kernel,
        grid=(channels // in_block,),
        in_specs=[w_spec, s_spec, limit_spec],
        out_specs=mode_spec,
        out_shape=jax.ShapeDtypeStruct((freqs, 2, kx, outs), jnp.float32),
        compiler_params=params,
        name="contract",
    )(weight, spectra, limit)
    halves = partial_modes.reshape(freqs, 2, kx, chans, groups, block)
    halves = halves.transpose(3, 4, 2, 5, 1, 0).reshape(chans, groups, kx, LANES)
    summed_modes = jnp.sum(exchange(halves, ("chan",), False, 2), axis=0)

    col_freq = mode_index * freqs + jnp.arange(freqs, dtype=jnp.int32)
    row_freq = slab_index * kx + jnp.arange(kx, dtype=jnp.int32)
    limit_rows = lax.dynamic_slice_in_dim(mode_limit, chan_index * channels, channels, 0)
    weights = mode_weights(limit_rows, col_freq, row_freq, all_kx, all_rows * all_cols)
    weights = jnp.broadcast_to(weights, (channels, kx, 2, freqs))
    weights = weights.reshape(groups, block, kx, 2 * freqs).transpose(0, 2, 1, 3)
    weights = weights.reshape(groups, kx, LANES)
    out_modes = joined(summed_modes * weights, 3)

    output, grad_sum, grad_partial, sums = pl.pallas_call(
        functools.partial(middle_kernel, modes),
        grid=grid,
        in_specs=[cells, cells, freq_cells, per_channel, per_channel]
        + [whole(t) for t in forward + back],
        out_specs=[cells, cells, freq_cells, per_channel],
        out_shape=[
            field,
            field,
            freq_field,
            jax.ShapeDtypeStruct((channels, 1, LANES), jnp.float32),
        ],
        compiler_params=params,
        name="middle",
    )(source_field, cotangent, out_modes, gain, wide(channel_bias), *forward, *back)

    grad_modes = spread(grad_partial, 5) * weights
    all_grads = exchange(grad_modes, ("chan",), True, 7)
    all_grads = all_grads.reshape(chans, groups, kx, block, 2, freqs)
    all_grads = all_grads.transpose(5, 4, 2, 0, 1, 3).reshape(freqs, 2, kx, outs)
    weight_grad, back_modes = pl.pallas_call(
        back_kernel,
        grid=(channels // in_block,),
        in_specs=[w_spec, s_spec, mode_spec, limit_spec],
        out_specs=[w_spec, s_spec],
        out_shape=[
            jax.ShapeDtypeStruct(weight.shape, jnp.float32),
            jax.ShapeDtypeStruct(spectra.shape, jnp.float32),
        ],
        compiler_params=params,
        name="back",
    )(weight, spectra, all_grads, limit)
    spectral_grad = weight_grad.transpose(0, 4, 1, 2, 3)

    sent = back_modes.size // LANES
    row_sums = sums[:, 0, :2].T.reshape(-1)
    extra = -(-row_sums.size // (8 * LANES)) * 8
    row_sums = jnp.pad(row_sums, (0, extra * LANES - row_sums.size)).reshape(extra, LANES)
    packed = jnp.concatenate([back_modes.reshape(sent, LANES), row_sums], axis=0)
    parts = joined(packed, 8)
    field_modes = parts[:, :sent].reshape(owners, groups, kx, LANES)
    totals = jnp.sum(parts[:, sent:], axis=0).reshape(-1)
    gate_grad = totals[:channels]
    bias_grad = totals[channels : 2 * channels]
    field_grad = pl.pallas_call(
        functools.partial(last_kernel, modes),
        grid=grid,
        in_specs=[cells, freq_cells, per_channel] + [whole(t) for t in back],
        out_specs=cells,
        out_shape=field,
        compiler_params=params,
        name="last",
    )(grad_sum, field_modes, gain, *back)
    return (output, field_grad, spectral_grad, gate_grad, bias_grad)


def halves_of(table):
    table = table.astype(np.float32)
    high = table.astype(ml_dtypes.bfloat16)
    low = (table - high.astype(np.float32)).astype(ml_dtypes.bfloat16)
    return high, low


def packed_tables(all_rows, all_cols, slabs, modes, freqs, kx_all):
    cell = np.arange(all_cols)[:, None]
    angle = (cell * np.arange(modes * freqs)[None, :] % all_cols) * (2.0 * np.pi / all_cols)
    parts = np.stack([np.cos(angle), -np.sin(angle)], axis=1).reshape(modes, -1, 2, modes, freqs)
    parts = parts.transpose(0, 1, 3, 2, 4)
    cols = parts.shape[1]
    high, low = halves_of(parts)
    ahead = np.stack([high, low], axis=3).reshape(modes, cols, -1)
    ahead = np.concatenate([ahead, ahead], axis=1)
    flat_high = high.reshape(modes, cols, -1).transpose(0, 2, 1)
    flat_low = low.reshape(modes, cols, -1).transpose(0, 2, 1)
    behind = np.concatenate([flat_high, flat_low, flat_high, flat_low], axis=1)
    wave = np.arange(kx_all)
    wave = wave + np.where(2 * wave >= kx_all, all_rows - kx_all, 0)
    angle = (np.arange(all_rows)[:, None] * wave[None, :] % all_rows) * (2.0 * np.pi / all_rows)
    table = np.concatenate([np.cos(angle), np.sin(angle)], axis=1).reshape(slabs, -1, 2 * kx_all)
    high, low = halves_of(table)
    row_behind = np.concatenate([high, high, low], axis=2)
    high, low = high.transpose(0, 2, 1), low.transpose(0, 2, 1)
    row_ahead = np.concatenate([high, low, high], axis=2)
    return ahead, row_ahead, row_behind, behind


def lane_roll(values, shift):
    shift = shift % values.shape[-1]
    return values if shift == 0 else pltpu.roll(values, shift, values.ndim - 1)


def lanes_of(shape):
    return lax.broadcasted_iota(jnp.int32, shape, len(shape) - 1)


def high_low(values):
    high = values.astype(jnp.bfloat16)
    return high, (values - high.astype(jnp.float32)).astype(jnp.bfloat16)


def quarter_turn(values, span, sign):
    half = span // 2
    first = lanes_of(values.shape) % span < half
    back, ahead = lane_roll(values, -half), lane_roll(values, half)
    return jnp.where(first, -back, ahead) if sign > 0 else jnp.where(first, back, -ahead)


def mix_rows(lines, row_table, rows, span, out_ref, kx):
    block = LANES // span
    mixed = []
    for c in range(0, block, 2):
        pair = jnp.concatenate([lines[c * rows : (c + 1) * rows], lines[(c + 1) * rows : (c + 2) * rows]], axis=1)
        high, low = high_low(pair)
        both = jnp.dot(row_table, jnp.concatenate([high, high, low], axis=0), preferred_element_type=jnp.float32)
        mixed += [both[:, :LANES], both[:, LANES:]]
    lane = lanes_of(mixed[0].shape)
    pairs = []
    for c in range(0, block, 2):
        left = mixed[c] + lane_roll(mixed[c], -span)
        right = mixed[c + 1] + lane_roll(mixed[c + 1], span)
        pairs.append(jnp.where(lane % (2 * span) < span, left, right))
    low_half = lane < LANES // 2
    owners = [
        jnp.where(low_half, pairs[0], lane_roll(pairs[1], LANES // 2)),
        jnp.where(low_half, lane_roll(pairs[0], LANES // 2), pairs[1]),
    ]
    all_kx = owners[0].shape[0] // 2
    slabs = all_kx // kx
    for m, values in enumerate(owners):
        done = values[:all_kx] + quarter_turn(values[all_kx:], span, -1)
        for s in range(slabs):
            out_ref[m * slabs + s, 0] = done[s * kx : (s + 1) * kx]


def spectrum_packed(span, x_ref, ahead_ref, row_ref, out_ref):
    block, rows, cols = x_ref.shape
    high, low = high_low(x_ref[...].reshape(block * rows, cols))
    lines = jnp.dot(jnp.concatenate([high, low], axis=1), ahead_ref[0], preferred_element_type=jnp.float32)
    mix_rows(lines, row_ref[0], rows, span, out_ref, out_ref.shape[2])


def group_lines(modes_ref, row_table, span):
    block = LANES // span
    owners = modes_ref.shape[0]
    half = owners // 2
    stack = []
    for m in range(2):
        stack.append(jnp.concatenate([modes_ref[m * half + s, 0] for s in range(half)], axis=0))
    full = [jnp.concatenate([one, quarter_turn(one, span, 1)], axis=0) for one in stack]
    rolled = [[lane_roll(one, k * span) for k in range(block)] for one in full]
    lane = lanes_of(full[0].shape)
    even = lane % (2 * span) < span
    low_half = lane < LANES // 2
    sides = []
    for c in range(block):
        first = jnp.where(low_half, rolled[0][(0 - c) % block], rolled[0][(2 - c) % block])
        second = jnp.where(low_half, rolled[1][(1 - c) % block], rolled[1][(3 - c) % block])
        sides.append(jnp.where(even, first, second))
    lines = []
    for c in range(0, block, 2):
        high, low = high_low(jnp.concatenate([sides[c], sides[c + 1]], axis=1))
        both = jnp.dot(row_table, jnp.concatenate([high, low, high], axis=0), preferred_element_type=jnp.float32)
        lines += [both[:, :LANES], both[:, LANES:]]
    return lines


def branch_of(lines, behind):
    high, low = high_low(lines)
    return jnp.dot(jnp.concatenate([high, low], axis=1), behind, preferred_element_type=jnp.float32)


def middle_packed(
    span, x_ref, cot_ref, modes_ref, gain_ref, bias_ref, ahead_ref, row_ref, row_back_ref, behind_ref,
    out_ref, grad_ref, spec_ref, sums_ref, split_ref,
):
    block, rows, cols = x_ref.shape
    step = pl.program_id(0)
    scale = math.sqrt(2.0 / math.pi)

    @pl.when(step == 0)
    def _():
        sums_ref[...] = jnp.zeros_like(sums_ref)

    lines = group_lines(modes_ref, row_back_ref[0], span)
    lane = lanes_of(sums_ref.shape)
    line = lax.broadcasted_iota(jnp.int32, sums_ref.shape, 0)
    for c in range(block):
        source = x_ref[c]
        v = branch_of(lines[c], behind_ref[0]) + (gain_ref[step * block + c] * source + bias_ref[step * block + c])
        square = v * v
        inner = v * (scale + (scale * 0.044715) * square)
        up = 0.5 + 0.5 * jnp.tanh(inner)
        out_ref[c] = v * up
        bend = v * (2.0 * scale + (6.0 * scale * 0.044715) * square)
        grad = cot_ref[c] * (up + (up * (1.0 - up)) * bend)
        grad_ref[c] = grad
        high, low = high_low(grad)
        split_ref[c * rows : (c + 1) * rows, :cols] = high
        split_ref[c * rows : (c + 1) * rows, cols:] = low
        gate = jnp.sum(jnp.sum(grad * source, axis=0, keepdims=True), axis=1, keepdims=True)
        bias = jnp.sum(jnp.sum(grad, axis=0, keepdims=True), axis=1, keepdims=True)
        here = (lane == step * block + c) & (line < 2)
        sums_ref[...] = jnp.where(here, jnp.where(line == 0, gate, bias), sums_ref[...])
    made = jnp.dot(split_ref[...], ahead_ref[0], preferred_element_type=jnp.float32)
    mix_rows(made, row_ref[0], rows, span, spec_ref, spec_ref.shape[2])


def last_packed(span, grad_ref, modes_ref, gain_ref, row_back_ref, behind_ref, out_ref):
    block = grad_ref.shape[0]
    step = pl.program_id(0)
    lines = group_lines(modes_ref, row_back_ref[0], span)
    for c in range(block):
        out_ref[c] = branch_of(lines[c], behind_ref[0]) + gain_ref[step * block + c] * grad_ref[c]


def swap_groups(values, kx):
    lane = lanes_of(values.shape) // kx
    line = lax.broadcasted_iota(jnp.int32, values.shape, 1)
    count = values.shape[1]
    hop = 1
    while hop < count:
        up = lane_roll(pltpu.roll(values, count - hop, 1), hop * kx)
        down = lane_roll(pltpu.roll(values, hop, 1), -hop * kx)
        lane_bit, line_bit = lane // hop % 2, line // hop % 2
        values = jnp.where(lane_bit == line_bit, values, jnp.where(lane_bit == 1, up, down))
        hop *= 2
    return values


def to_lanes(packed, out_ref, kx):
    lines = swap_groups(packed.T.reshape(-1, 8, LANES), kx)
    wide = out_ref.shape[0]
    block = lines.shape[0] // wide
    for c in range(block):
        for j in range(wide):
            out_ref[j, pl.ds(c, 8, stride=block)] = lines[c * wide + j]


def to_rows(wide_ref, block, kx):
    wide = wide_ref.shape[0]
    pieces = []
    for c in range(block):
        for j in range(wide):
            pieces.append(wide_ref[j, pl.ds(c, 8, stride=block)][None])
    return swap_groups(jnp.concatenate(pieces, axis=0), kx).reshape(-1, LANES).T


def both_parts(ref, rows):
    half = ref.shape[0] // 2
    parts = [jnp.concatenate([ref[p * half + j, rows] for j in range(half)], axis=1) for p in range(2)]
    return parts[0], parts[1]


def put_part(ref, rows, part, values):
    half = ref.shape[0] // 2
    for j in range(half):
        ref[part * half + j, rows] = values[:, j * LANES : (j + 1) * LANES]


def other(axis, step, size):
    return lax.rem(lax.axis_index(axis) + step, size)


def send(source, target, sends, recvs, axis, peer):
    copy = pltpu.make_async_remote_copy(
        src_ref=source, dst_ref=target, send_sem=sends, recv_sem=recvs,
        device_id={axis: peer}, device_id_type=pl.DeviceIdType.MESH,
    )
    copy.start()
    return copy


def greet(slabs):
    barrier = pltpu.get_barrier_semaphore()
    targets = [("mode", 1, 2), ("chan", 1, 2)] + [("slab", step, slabs) for step in range(1, slabs)]
    for axis, step, size in targets:
        pl.semaphore_signal(
            barrier, inc=1, device_id={axis: other(axis, step, size)}, device_id_type=pl.DeviceIdType.MESH
        )
    pl.semaphore_wait(barrier, len(targets))


def scatter_sum(part_ref, half_ref, give_ref, take_ref, mode_sems, slab_sems, slabs, between):
    me_mode, me_slab = lax.axis_index("mode"), lax.axis_index("slab")
    peer = other("mode", 1, 2)
    order = [slabs // 2] + [step for step in range(1, slabs) if step != slabs // 2] + [0]
    copies = []
    for step in order:
        slab = other("slab", step, slabs)
        copies.append(send(
            part_ref.at[peer * slabs + slab], half_ref.at[step], mode_sems.at[0, step], mode_sems.at[1, step], "mode", peer
        ))
    waits = list(copies)
    out = []
    for step, copy in zip(order, copies):
        copy.wait_recv()
        slab = other("slab", step, slabs)
        total = part_ref[me_mode * slabs + slab] + half_ref[step]
        if step == 0:
            mine = total
        else:
            give_ref[step] = total
            out.append(send(
                give_ref.at[step], take_ref.at[step], slab_sems.at[0, step], slab_sems.at[1, step], "slab", slab
            ))
    between()
    for copy in out:
        copy.wait_recv()
    for step in range(1, slabs):
        mine = mine + take_ref[step]
    return mine, [copy.wait_send for copy in copies + out]


def gather_start(own_ref, out_ref, mode_sems, slab_sems, slabs):
    me = lax.axis_index("mode") * slabs + lax.axis_index("slab")
    copies = []
    for step in [slabs // 2] + [step for step in range(1, slabs) if step != slabs // 2]:
        copies.append(send(
            own_ref, out_ref.at[me], slab_sems.at[0, step], slab_sems.at[1, step], "slab", other("slab", step, slabs)
        ))
    near = send(own_ref, out_ref.at[me], mode_sems.at[0, 0], mode_sems.at[1, 0], "mode", other("mode", 1, 2))
    out_ref[me] = own_ref[...]
    return copies, near


def gather_finish(state, out_ref, mode_sems, slabs, between):
    copies, near = state
    relays = []
    order = [slabs // 2] + [step for step in range(1, slabs) if step != slabs // 2]
    for k in list(range(1, slabs - 1)) + [0]:
        between(k)
        copies[k].wait_recv()
        step = order[k]
        source = lax.axis_index("mode") * slabs + other("slab", slabs - step, slabs)
        relays.append(send(
            out_ref.at[source], out_ref.at[source], mode_sems.at[0, step], mode_sems.at[1, step], "mode", other("mode", 1, 2)
        ))
    near.wait()
    for copy in relays:
        copy.wait()
    for copy in copies:
        copy.wait_send()


def forward_kernel(
    slabs, kx, part_ref, w_ref, limit_ref, weight_ref, out_ref, turned_ref, spec_ref,
    half_ref, give_ref, take_ref, w_buf, t_buf, sum_ref, peer_ref, own_ref,
    mode_a, slab_a, mode_b, slab_b, chan_sems, w_sems, t_sems,
):
    ins, freqs = w_ref.shape[0], w_ref.shape[1]
    outs = w_ref.shape[4]
    mine_outs = outs // 2
    wide = freqs * kx
    for i in range(ins):
        pltpu.make_async_copy(w_ref.at[i], w_buf.at[i], w_sems.at[i]).start()
    greet(slabs)
    first = lax.axis_index("chan") * ins

    def flip():
        def body(i, carry):
            pltpu.make_async_copy(w_ref.at[i], w_buf.at[i], w_sems.at[i]).wait()
            keep = jnp.broadcast_to(limit_ref[:, :1], (outs, wide)) > first + i
            for p in range(2):
                turned = w_buf[i, :, p].reshape(wide, outs).T
                t_buf[i, :, p * wide : (p + 1) * wide] = jnp.where(keep, turned, 0.0)
            pltpu.make_async_copy(t_buf.at[i], turned_ref.at[i], t_sems.at[i]).start()
            return carry
        lax.fori_loop(0, ins, body, 0)

    mine, sent = scatter_sum(part_ref, half_ref, give_ref, take_ref, mode_a, slab_a, slabs, flip)
    to_lanes(mine, spec_ref, kx)

    def contract(i, carry):
        real, imag = carry
        w_real, w_imag = t_buf[i, :, :wide], t_buf[i, :, wide:]
        s_real, s_imag = both_parts(spec_ref, pl.ds(i, 1))
        return real + (s_real * w_real - s_imag * w_imag), imag + (s_real * w_imag + s_imag * w_real)

    zero = jnp.zeros((outs, wide), jnp.float32)
    real, imag = lax.fori_loop(0, ins, contract, (zero, zero))
    put_part(sum_ref, slice(None), 0, real)
    put_part(sum_ref, slice(None), 1, imag)
    theirs = other("chan", 1, 2) * mine_outs
    swap = send(
        sum_ref.at[:, pl.ds(theirs, mine_outs)], peer_ref, chan_sems.at[0], chan_sems.at[1], "chan", other("chan", 1, 2)
    )
    swap.wait_recv()
    for j in range(peer_ref.shape[0]):
        peer_ref[j] = (sum_ref[j, pl.ds(first, mine_outs)] + peer_ref[j]) * weight_ref[j % weight_ref.shape[0]]
    own_ref[...] = to_rows(peer_ref, mine_outs // 8, kx)
    state = gather_start(own_ref, out_ref, mode_b, slab_b, slabs)
    gather_finish(state, out_ref, mode_b, slabs, lambda k: None)
    swap.wait_send()
    for wait in sent:
        wait()

    def settle(i, carry):
        pltpu.make_async_copy(t_buf.at[i], turned_ref.at[i], t_sems.at[i]).wait()
        return carry
    lax.fori_loop(0, ins, settle, 0)


def backward_kernel(
    slabs, kx, part_ref, sums_ref, turned_ref, spec_ref, limit_ref, weight_ref,
    out_ref, wgrad_ref, total_ref,
    half_ref, give_ref, take_ref, g_buf, t_buf, grad_ref, back_ref, own_ref, near_ref, far_ref, pass_ref,
    mode_a, slab_a, mode_b, slab_b, chan_sems, g_sems, t_sems, sum_mode, sum_slab,
):
    ins, freqs = wgrad_ref.shape[0], wgrad_ref.shape[1]
    outs = wgrad_ref.shape[4]
    mine_outs = outs // 2
    wide = freqs * kx
    for i in range(ins):
        pltpu.make_async_copy(turned_ref.at[i], t_buf.at[i], t_sems.at[i]).start()
    greet(slabs)
    first = lax.axis_index("chan") * ins
    near = send(sums_ref, near_ref, sum_mode.at[0], sum_mode.at[1], "mode", other("mode", 1, 2))

    far = []
    def total_up():
        near.wait_recv()
        pass_ref[...] = sums_ref[...] + near_ref[...]
        for step in range(1, slabs):
            far.append(send(
                pass_ref, far_ref.at[step], sum_slab.at[0, step], sum_slab.at[1, step], "slab", other("slab", step, slabs)
            ))

    mine, sent = scatter_sum(part_ref, half_ref, give_ref, take_ref, mode_a, slab_a, slabs, total_up)
    to_lanes(mine, back_ref, kx)
    here = pl.ds(first, mine_outs)
    for j in range(back_ref.shape[0]):
        grad_ref[j, here] = back_ref[j] * weight_ref[j % weight_ref.shape[0]]
    swap = send(
        grad_ref.at[:, here], grad_ref.at[:, here], chan_sems.at[0], chan_sems.at[1], "chan", other("chan", 1, 2)
    )

    def arrive(i, carry):
        pltpu.make_async_copy(turned_ref.at[i], t_buf.at[i], t_sems.at[i]).wait()
        return carry
    lax.fori_loop(0, ins, arrive, 0)
    swap.wait_recv()

    def pull(i, carry):
        w_real, w_imag = t_buf[i, :, :wide], t_buf[i, :, wide:]
        g_real, g_imag = both_parts(grad_ref, slice(None))
        put_part(back_ref, pl.ds(i, 1), 0, jnp.sum(g_real * w_real + g_imag * w_imag, axis=0, keepdims=True))
        put_part(back_ref, pl.ds(i, 1), 1, jnp.sum(g_imag * w_real - g_real * w_imag, axis=0, keepdims=True))
        return carry
    lax.fori_loop(0, ins, pull, 0)
    own_ref[...] = to_rows(back_ref, ins // 8, kx)
    state = gather_start(own_ref, out_ref, mode_b, slab_b, slabs)
    share = ins // (slabs - 1)

    def outer(i, carry):
        keep = jnp.broadcast_to(limit_ref[:, :1], (outs, wide)) > first + i
        g_real, g_imag = both_parts(grad_ref, slice(None))
        s_real, s_imag = both_parts(spec_ref, pl.ds(i, 1))
        real = jnp.where(keep, s_real * g_real + s_imag * g_imag, 0.0)
        imag = jnp.where(keep, s_real * g_imag - s_imag * g_real, 0.0)
        g_buf[i, :, 0] = real.T.reshape(freqs, kx, outs)
        g_buf[i, :, 1] = imag.T.reshape(freqs, kx, outs)
        pltpu.make_async_copy(g_buf.at[i], wgrad_ref.at[i], g_sems.at[i]).start()
        return carry

    done = [0]
    def between(k):
        stop = ins if k == 0 else done[0] + share
        lax.fori_loop(done[0], stop, outer, 0)
        done[0] = stop

    gather_finish(state, out_ref, mode_b, slabs, between)
    total = pass_ref[...]
    for step, copy in zip(range(1, slabs), far):
        copy.wait()
        total = total + far_ref[step]
    total_ref[...] = total
    near.wait_send()
    swap.wait_send()
    for wait in sent:
        wait()

    def settle(i, carry):
        pltpu.make_async_copy(g_buf.at[i], wgrad_ref.at[i], g_sems.at[i]).wait()
        return carry
    lax.fori_loop(0, ins, settle, 0)


def fits(shapes, mesh_sizes):
    channels, rows, cols = shapes[0]
    outs, freqs, kx = shapes[2][1], shapes[2][2], shapes[2][4]
    slabs, modes, chans = mesh_sizes
    return (
        modes == 2 and chans == 2 and slabs > 2 and slabs % 2 == 0
        and 8 * kx == LANES and 8 * freqs == LANES and 2 * freqs * channels == 8 * LANES
        and outs == chans * channels
        and rows % LANES == 0 and cols % LANES == 0
    )


def local(source_field, cotangent, spectral_weight, skip_gain, channel_bias, mode_limit, width_limit):
    slabs, modes, chans = (lax.axis_size(axis) for axis in ("slab", "mode", "chan"))
    args = (source_field, cotangent, spectral_weight, skip_gain, channel_bias, mode_limit, width_limit)
    if not fits([one.shape for one in args], (slabs, modes, chans)):
        return local_plain(*args)
    channels, rows, cols = source_field.shape
    outs, freqs, kx = spectral_weight.shape[1], spectral_weight.shape[2], spectral_weight.shape[4]
    span = 2 * freqs
    block = LANES // span
    groups = channels // block
    owners = slabs * modes
    all_kx, all_rows, all_cols = kx * slabs, rows * slabs, cols * modes
    wide = freqs * kx
    ahead, row_ahead, row_behind, behind = (
        jnp.asarray(t) for t in packed_tables(all_rows, all_cols, slabs, modes, freqs, all_kx)
    )
    slab_index, mode_index, chan_index = (lax.axis_index(axis) for axis in ("slab", "mode", "chan"))

    def pick(table, axis):
        return pl.BlockSpec((1,) + table.shape[1:], lambda g: (lax.axis_index(axis), 0, 0))

    cells = pl.BlockSpec((block, rows, cols), lambda g: (g, 0, 0))
    freq_cells = pl.BlockSpec((owners, 1, kx, LANES), lambda g: (0, g, 0, 0))
    scalars = pl.BlockSpec(memory_space=pltpu.SMEM)
    small = pl.BlockSpec((8, LANES), lambda g: (0, 0))
    field = jax.ShapeDtypeStruct(source_field.shape, jnp.float32)
    freq_field = jax.ShapeDtypeStruct((owners, groups, kx, LANES), jnp.float32)
    params = pltpu.CompilerParams(dimension_semantics=("arbitrary",), vmem_limit_bytes=BIG)
    f32 = jnp.float32

    partial = pl.pallas_call(
        functools.partial(spectrum_packed, span),
        grid=(groups,),
        in_specs=[cells, pick(ahead, "mode"), pick(row_ahead, "slab")],
        out_specs=freq_cells,
        out_shape=freq_field,
        compiler_params=params,
        name="spectrum",
    )(source_field, ahead, row_ahead)

    weight = spectral_weight.transpose(0, 2, 3, 4, 1)
    col_freq = mode_index * freqs + jnp.arange(freqs, dtype=jnp.int32)
    row_freq = slab_index * kx + jnp.arange(kx, dtype=jnp.int32)
    limit_rows = lax.dynamic_slice_in_dim(mode_limit, chan_index * channels, channels, 0)
    flat_cols, flat_rows = jnp.repeat(col_freq, kx)[None, :], jnp.tile(row_freq, freqs)[None, :]
    kept = (flat_cols < limit_rows[:, 0:1]) & (
        (flat_rows < limit_rows[:, 1:2]) | (all_kx - flat_rows < limit_rows[:, 1:2])
    )
    scales = jnp.where(flat_cols == 0, 1.0, 2.0).astype(jnp.float32) / (all_rows * all_cols)
    weights = jnp.where(kept, scales, 0.0).reshape(channels, -1, LANES).transpose(1, 0, 2)
    limit = jnp.broadcast_to(width_limit[:, None], (outs, LANES))

    dma, vmem = pltpu.SemaphoreType.DMA, pltpu.VMEM
    in_vmem, anywhere = pl.BlockSpec(memory_space=pltpu.VMEM), pl.BlockSpec(memory_space=pl.ANY)
    piece = (groups * kx, LANES)
    common = [vmem((slabs,) + piece, f32), vmem((slabs,) + piece, f32), vmem((slabs,) + piece, f32)]
    pair = [dma((2, slabs))] * 4
    comm = lambda ident: pltpu.CompilerParams(collective_id=ident, has_side_effects=True, vmem_limit_bytes=BIG)
    gathered = jax.ShapeDtypeStruct((owners,) + piece, f32)
    flat = lambda lines: (2 * wide // LANES, lines, LANES)
    turned_shape = jax.ShapeDtypeStruct((channels, outs, 2 * wide), f32)

    out_modes, turned, spec = pl.pallas_call(
        functools.partial(forward_kernel, slabs, kx),
        in_specs=[in_vmem, anywhere, in_vmem, in_vmem],
        out_specs=[in_vmem, anywhere, in_vmem],
        out_shape=[gathered, turned_shape, jax.ShapeDtypeStruct(flat(channels), f32)],
        scratch_shapes=common + [
            vmem(weight.shape, f32), vmem(turned_shape.shape, f32), vmem(flat(outs), f32),
            vmem(flat(outs // 2), f32), vmem(piece, f32),
        ] + pair + [dma((2,)), dma((channels,)), dma((channels,))],
        compiler_params=comm(20),
        name="forward_modes",
    )(partial.reshape((owners,) + piece), weight, limit, weights)

    output, grad_sum, grad_partial, sums = pl.pallas_call(
        functools.partial(middle_packed, span),
        grid=(groups,),
        in_specs=[
            cells, cells, freq_cells, scalars, scalars, pick(ahead, "mode"), pick(row_ahead, "slab"),
            pick(row_behind, "slab"), pick(behind, "mode"),
        ],
        out_specs=[cells, cells, freq_cells, small],
        out_shape=[field, field, freq_field, jax.ShapeDtypeStruct((8, LANES), f32)],
        scratch_shapes=[vmem((block * rows, 2 * cols), jnp.bfloat16)],
        compiler_params=params,
        name="middle",
    )(
        source_field, cotangent, out_modes.reshape(freq_field.shape), skip_gain, channel_bias,
        ahead, row_ahead, row_behind, behind,
    )

    back_modes, weight_grad, totals = pl.pallas_call(
        functools.partial(backward_kernel, slabs, kx),
        in_specs=[in_vmem, in_vmem, anywhere, in_vmem, in_vmem, in_vmem],
        out_specs=[in_vmem, anywhere, in_vmem],
        out_shape=[gathered, jax.ShapeDtypeStruct(weight.shape, f32), jax.ShapeDtypeStruct((8, LANES), f32)],
        scratch_shapes=common + [
            vmem(weight.shape, f32), vmem(turned_shape.shape, f32), vmem(flat(outs), f32),
            vmem(flat(channels), f32), vmem(piece, f32), vmem((8, LANES), f32),
            vmem((slabs, 8, LANES), f32), vmem((8, LANES), f32),
        ] + pair + [dma((2,)), dma((channels,)), dma((channels,)), dma((2,)), dma((2, slabs))],
        compiler_params=comm(21),
        name="backward_modes",
    )(grad_partial.reshape((owners,) + piece), sums, turned, spec, limit, weights)
    spectral_grad = weight_grad.transpose(0, 4, 1, 2, 3)

    field_grad = pl.pallas_call(
        functools.partial(last_packed, span),
        grid=(groups,),
        in_specs=[cells, freq_cells, scalars, pick(row_behind, "slab"), pick(behind, "mode")],
        out_specs=cells,
        out_shape=field,
        compiler_params=params,
        name="last",
    )(grad_sum, back_modes.reshape(freq_field.shape), skip_gain, row_behind, behind)
    return (output, field_grad, spectral_grad, totals[0, :channels], totals[1, :channels])


def solution(mesh):
    in_specs = (
        P(("member", "chan"), "slab", "mode"),
        P(("member", "chan"), "slab", "mode"),
        P(("member", "chan"), None, "mode", None, "slab"),
        P(("member", "chan")),
        P(("member", "chan")),
        P("member", None),
        P("member"),
    )
    out_specs = (
        P(("member", "chan"), "slab", "mode"),
        P(("member", "chan"), "slab", "mode"),
        P(("member", "chan"), None, "mode", None, "slab"),
        P(("member", "chan")),
        P(("member", "chan")),
    )
    return jax.shard_map(local, mesh=mesh, in_specs=in_specs, out_specs=out_specs, check_vma=False)
```

```python
import functools
import math

import jax
import jax.numpy as jnp
import ml_dtypes
import numpy as np
from jax import lax
from jax.experimental import pallas as pl
from jax.experimental.pallas import tpu as pltpu
from jax.sharding import PartitionSpec as P

LANES = 128
BIG = 60 * 1024 * 1024
MIB = 1024 * 1024


def split_table(table):
    high = lax.reduce_precision(table, 8, 7)
    return high.astype(jnp.bfloat16), (table - high).astype(jnp.bfloat16)


def split_block(values):
    high = values.astype(jnp.bfloat16)
    return high, (values - high.astype(jnp.float32)).astype(jnp.bfloat16)


def dot_pair(left, right):
    left_high, left_low = left
    right_high, right_low = right
    mul = functools.partial(jnp.dot, preferred_element_type=jnp.float32)
    return mul(left_high, right_high) + mul(left_low, right_high) + mul(left_high, right_low)


def tables(extent, waves, first_cell, cell_count):
    cell_index = first_cell + jnp.arange(cell_count, dtype=jnp.int32)
    products = (cell_index[:, None] * waves[None, :] % extent).astype(jnp.float32)
    angles = products * (2.0 * math.pi / extent)
    return jnp.cos(angles), jnp.sin(angles)


def store_spectrum(values, col_pair, row_pair, out_ref):
    block, rows, cols = values.shape
    lines = dot_pair(split_block(values.reshape(block * rows, cols)), col_pair)
    all_kx = row_pair[0].shape[0] // 2
    kx, lanes = out_ref.shape[2:]
    span = lanes // block
    mode_count = lines.shape[1] // span
    slabs = out_ref.shape[0] // mode_count
    done = []
    for c in range(block):
        mixed = dot_pair(row_pair, split_block(lines[c * rows : (c + 1) * rows]))
        done.append(mixed[:all_kx] - turn(mixed[all_kx:], span))
    for m in range(mode_count):
        packed = jnp.concatenate([one[:, m * span : (m + 1) * span] for one in done], axis=1)
        for s in range(slabs):
            out_ref[m * slabs + s, 0] = packed[s * kx : (s + 1) * kx]


def turn(values, span):
    half = span // 2
    pieces = []
    for first in range(0, values.shape[1], span):
        pieces.append(-values[:, first + half : first + span])
        pieces.append(values[:, first : first + half])
    return jnp.concatenate(pieces, axis=1)


def all_modes(modes_ref, mode_count, c, block):
    span = modes_ref.shape[3] // block
    slabs = modes_ref.shape[0] // mode_count
    columns = []
    for m in range(mode_count):
        stack = [modes_ref[m * slabs + s, 0] for s in range(slabs)]
        columns.append(jnp.concatenate(stack, axis=0)[:, c * span : (c + 1) * span])
    return jnp.concatenate(columns, axis=1), span


def synth(modes_and_span, row_pair, col_pair):
    modes, span = modes_and_span
    stacked = jnp.concatenate([modes, turn(modes, span)], axis=0)
    lines = dot_pair(row_pair, split_block(stacked))
    return dot_pair(split_block(lines), col_pair)


def spectrum_kernel(x_ref, ch_ref, cl_ref, rh_ref, rl_ref, out_ref):
    store_spectrum(x_ref[...], (ch_ref[...], cl_ref[...]), (rh_ref[...], rl_ref[...]), out_ref)


def middle_kernel(
    mode_count, x_ref, cot_ref, modes_ref, gain_ref, bias_ref, ch_ref, cl_ref, rh_ref, rl_ref,
    cth_ref, ctl_ref, ih_ref, il_ref, out_ref, grad_ref, spec_ref, sums_ref,
):
    block = x_ref.shape[0]
    row_back = (ih_ref[...], il_ref[...])
    col_back = (cth_ref[...], ctl_ref[...])
    scale = math.sqrt(2.0 / math.pi)
    for c in range(block):
        source = x_ref[c]
        gain = gain_ref[c]
        v = synth(all_modes(modes_ref, mode_count, c, block), row_back, col_back) + gain[:, :1] * source + bias_ref[c][:, :1]
        square = v * v
        t = jnp.tanh(scale * v * (1.0 + 0.044715 * square))
        half_up = 0.5 * (1.0 + t)
        out_ref[c] = v * half_up
        slope = half_up + 0.5 * v * (1.0 - t * t) * (scale * (1.0 + 3.0 * 0.044715 * square))
        grad = cot_ref[c] * slope
        grad_ref[c] = grad
        gate = jnp.sum(jnp.sum(grad * source, axis=0, keepdims=True), axis=1, keepdims=True)
        bias = jnp.sum(jnp.sum(grad, axis=0, keepdims=True), axis=1, keepdims=True)
        lane = lax.broadcasted_iota(jnp.int32, (1, LANES), 1)
        sums_ref[c] = jnp.where(lane == 0, gate, bias)
    store_spectrum(
        grad_ref[...], (ch_ref[...], cl_ref[...]), (rh_ref[...], rl_ref[...]), spec_ref
    )


def last_kernel(mode_count, grad_ref, modes_ref, gain_ref, cth_ref, ctl_ref, ih_ref, il_ref, out_ref):
    block = grad_ref.shape[0]
    for c in range(block):
        modes = all_modes(modes_ref, mode_count, c, block)
        branch = synth(modes, (ih_ref[...], il_ref[...]), (cth_ref[...], ctl_ref[...]))
        out_ref[c] = branch + gain_ref[c][:, :1] * grad_ref[c]


def contract_kernel(w_ref, spec_ref, limit_ref, out_ref):
    block, freqs, _, kx, outs = w_ref.shape
    first = lax.axis_index("chan") * (block * pl.num_programs(0)) + pl.program_id(0) * block

    @pl.when(pl.program_id(0) == 0)
    def _():
        out_ref[...] = jnp.zeros_like(out_ref)

    limit = limit_ref[...]
    for y in range(freqs):
        real = out_ref[y, 0]
        imag = out_ref[y, 1]
        for i in range(block):
            keep = first + i < limit
            spec = spec_ref[0]
            at = 2 * freqs * i + y
            s_real = jnp.where(keep, spec[:, at : at + 1], 0.0)
            s_imag = jnp.where(keep, spec[:, freqs + at : freqs + at + 1], 0.0)
            w_real = w_ref[i, y, 0]
            w_imag = w_ref[i, y, 1]
            real = real + (s_real * w_real - s_imag * w_imag)
            imag = imag + (s_real * w_imag + s_imag * w_real)
        out_ref[y, 0] = real
        out_ref[y, 1] = imag


def back_kernel(w_ref, spec_ref, grads_ref, limit_ref, wgrad_ref, out_ref):
    block, freqs, _, kx, outs = w_ref.shape
    first = lax.axis_index("chan") * (block * pl.num_programs(0)) + pl.program_id(0) * block
    limit = limit_ref[...]
    lane = lax.broadcasted_iota(jnp.int32, out_ref.shape[1:], 1)
    spec = spec_ref[0]
    back = jnp.zeros(out_ref.shape[1:], jnp.float32)
    for i in range(block):
        keep = first + i < limit
        for y in range(freqs):
            at = 2 * freqs * i + y
            g_real = jnp.where(keep, grads_ref[y, 0], 0.0)
            g_imag = jnp.where(keep, grads_ref[y, 1], 0.0)
            s_real = spec[:, at : at + 1]
            s_imag = spec[:, freqs + at : freqs + at + 1]
            wgrad_ref[i, y, 0] = s_real * g_real + s_imag * g_imag
            wgrad_ref[i, y, 1] = s_real * g_imag - s_imag * g_real
            w_real = w_ref[i, y, 0]
            w_imag = w_ref[i, y, 1]
            b_real = jnp.sum(g_real * w_real + g_imag * w_imag, axis=1, keepdims=True)
            b_imag = jnp.sum(g_imag * w_real - g_real * w_imag, axis=1, keepdims=True)
            back = jnp.where(lane == at, b_real, back)
            back = jnp.where(lane == freqs + at, b_imag, back)
    out_ref[0] = back


def exchange_kernel(axes, sizes, gather, x_ref, out_ref, send_sem, recv_sem, own_sem):
    total = math.prod(sizes)
    me = lax.axis_index(axes[0])
    for axis, size in zip(axes[1:], sizes[1:]):
        me = me * size + lax.axis_index(axis)

    def place(index):
        coords = {}
        for axis, size in reversed(list(zip(axes, sizes))):
            coords[axis] = lax.rem(index, size)
            index = lax.div(index, size)
        return coords

    barrier = pltpu.get_barrier_semaphore()
    for step in range(1, total):
        pl.semaphore_signal(
            barrier, inc=1, device_id=place(lax.rem(me + step, total)),
            device_id_type=pl.DeviceIdType.MESH,
        )
    pl.semaphore_wait(barrier, total - 1)
    copies = []
    for step in range(1, total):
        peer = lax.rem(me + step, total)
        copy = pltpu.make_async_remote_copy(
            src_ref=x_ref if gather else x_ref.at[peer],
            dst_ref=out_ref.at[me],
            send_sem=send_sem.at[step],
            recv_sem=recv_sem.at[step],
            device_id=place(peer),
            device_id_type=pl.DeviceIdType.MESH,
        )
        copy.start()
        copies.append(copy)
    own = pltpu.make_async_copy(x_ref if gather else x_ref.at[me], out_ref.at[me], own_sem)
    own.start()
    own.wait()
    for copy in copies:
        copy.wait()


def exchange(values, axes, gather, ident):
    sizes = tuple(lax.axis_size(axis) for axis in axes)
    total = math.prod(sizes)
    piece = values.shape if gather else values.shape[1:]
    flat = values.reshape((-1, LANES) if gather else (total, -1, LANES))
    out = pl.pallas_call(
        functools.partial(exchange_kernel, axes, sizes, gather),
        out_shape=jax.ShapeDtypeStruct((total,) + flat.shape[-2:], jnp.float32),
        in_specs=[pl.BlockSpec(memory_space=pltpu.VMEM)],
        out_specs=pl.BlockSpec(memory_space=pltpu.VMEM),
        scratch_shapes=[
            pltpu.SemaphoreType.DMA((total,)),
            pltpu.SemaphoreType.DMA((total,)),
            pltpu.SemaphoreType.DMA,
        ],
        compiler_params=pltpu.CompilerParams(collective_id=ident, has_side_effects=True),
        name="exchange" + str(ident),
    )(flat)
    return out.reshape((total,) + piece)


def mode_weights(limit_rows, col_freq, row_freq, kx_count, cells_total):
    keep_cols = col_freq[None, :] < limit_rows[:, 0:1]
    keep_rows = (row_freq[None, :] < limit_rows[:, 1:2]) | (
        (kx_count - row_freq)[None, :] < limit_rows[:, 1:2]
    )
    scales = jnp.where(col_freq == 0, 1.0, 2.0).astype(jnp.float32) / cells_total
    joined = keep_rows[:, :, None] & keep_cols[:, None, :]
    return (joined.astype(jnp.float32) * scales[None, None, :])[:, :, None, :]


def local_plain(
    source_field, cotangent, spectral_weight, skip_gain, channel_bias, mode_limit, width_limit
):
    channels, row_count, col_count = source_field.shape
    slabs = lax.axis_size("slab")
    modes = lax.axis_size("mode")
    chans = lax.axis_size("chan")
    slab_index = lax.axis_index("slab")
    mode_index = lax.axis_index("mode")
    chan_index = lax.axis_index("chan")
    outs = spectral_weight.shape[1]
    freqs = spectral_weight.shape[2]
    kx = spectral_weight.shape[4]
    all_freqs = freqs * modes
    all_kx = kx * slabs
    all_rows = row_count * slabs
    all_cols = col_count * modes

    col_waves = jnp.arange(all_freqs, dtype=jnp.int32)
    row_waves = jnp.arange(all_kx, dtype=jnp.int32)
    row_waves = row_waves + jnp.where(2 * row_waves >= all_kx, all_rows - all_kx, 0)
    col_cos, col_sin = tables(all_cols, col_waves, mode_index * col_count, col_count)
    row_cos, row_sin = tables(all_rows, row_waves, slab_index * row_count, row_count)
    col_tab = jnp.stack(
        [col_cos.reshape(-1, modes, freqs), -col_sin.reshape(-1, modes, freqs)], axis=2
    ).reshape(col_count, 2 * all_freqs)
    row_tab = jnp.concatenate([row_cos, row_sin], axis=1)
    col_pair = split_table(col_tab)
    col_back = tuple(part.T for part in col_pair)
    row_back = split_table(row_tab)
    row_pair = tuple(part.T for part in row_back)

    block = LANES // (2 * freqs)
    groups = channels // block
    owners = slabs * modes
    cells = pl.BlockSpec((block, row_count, col_count), lambda c: (c, 0, 0))
    freq_cells = pl.BlockSpec((owners, 1, kx, LANES), lambda c: (0, c, 0, 0))
    per_channel = pl.BlockSpec((block, 1, LANES), lambda c: (c, 0, 0))
    field = jax.ShapeDtypeStruct(source_field.shape, jnp.float32)
    freq_field = jax.ShapeDtypeStruct((owners, groups, kx, LANES), jnp.float32)
    params = pltpu.CompilerParams(
        dimension_semantics=("arbitrary",), vmem_limit_bytes=BIG
    )

    def whole(array):
        return pl.BlockSpec(array.shape, lambda c: (0,) * array.ndim)

    grid = (channels // block,)
    wide = lambda values: jnp.broadcast_to(values[:, None, None], (channels, 1, LANES))
    gain = wide(skip_gain)
    forward = col_pair + row_pair
    back = col_back + row_back

    def spread(partial, ident):
        half = exchange(partial.reshape(modes, -1, LANES), ("mode",), False, ident)
        half = jnp.sum(half, axis=0).reshape(slabs, -1, LANES)
        return jnp.sum(exchange(half, ("slab",), False, ident + 1), axis=0).reshape(
            groups, kx, LANES
        )

    def joined(piece, ident):
        half = exchange(piece, ("slab",), True, ident)
        return exchange(half, ("mode",), True, ident + 1).reshape((owners,) + piece.shape)

    spectra = spread(
        pl.pallas_call(
            spectrum_kernel,
            grid=grid,
            in_specs=[cells] + [whole(t) for t in forward],
            out_specs=freq_cells,
            out_shape=freq_field,
            compiler_params=params,
            name="spectrum",
        )(source_field, *forward),
        0,
    )

    weight = spectral_weight.transpose(0, 2, 3, 4, 1)
    limit = width_limit.reshape(1, outs)
    in_block = block
    w_spec = pl.BlockSpec((in_block, freqs, 2, kx, outs), lambda i: (i, 0, 0, 0, 0))
    s_spec = pl.BlockSpec((1, kx, LANES), lambda i: (i, 0, 0))
    mode_spec = pl.BlockSpec((freqs, 2, kx, outs), lambda i: (0, 0, 0, 0))
    limit_spec = pl.BlockSpec((1, outs), lambda i: (0, 0))
    partial_modes = pl.pallas_call(
        contract_kernel,
        grid=(channels // in_block,),
        in_specs=[w_spec, s_spec, limit_spec],
        out_specs=mode_spec,
        out_shape=jax.ShapeDtypeStruct((freqs, 2, kx, outs), jnp.float32),
        compiler_params=params,
        name="contract",
    )(weight, spectra, limit)
    halves = partial_modes.reshape(freqs, 2, kx, chans, groups, block)
    halves = halves.transpose(3, 4, 2, 5, 1, 0).reshape(chans, groups, kx, LANES)
    summed_modes = jnp.sum(exchange(halves, ("chan",), False, 2), axis=0)

    col_freq = mode_index * freqs + jnp.arange(freqs, dtype=jnp.int32)
    row_freq = slab_index * kx + jnp.arange(kx, dtype=jnp.int32)
    limit_rows = lax.dynamic_slice_in_dim(mode_limit, chan_index * channels, channels, 0)
    weights = mode_weights(limit_rows, col_freq, row_freq, all_kx, all_rows * all_cols)
    weights = jnp.broadcast_to(weights, (channels, kx, 2, freqs))
    weights = weights.reshape(groups, block, kx, 2 * freqs).transpose(0, 2, 1, 3)
    weights = weights.reshape(groups, kx, LANES)
    out_modes = joined(summed_modes * weights, 3)

    output, grad_sum, grad_partial, sums = pl.pallas_call(
        functools.partial(middle_kernel, modes),
        grid=grid,
        in_specs=[cells, cells, freq_cells, per_channel, per_channel]
        + [whole(t) for t in forward + back],
        out_specs=[cells, cells, freq_cells, per_channel],
        out_shape=[
            field,
            field,
            freq_field,
            jax.ShapeDtypeStruct((channels, 1, LANES), jnp.float32),
        ],
        compiler_params=params,
        name="middle",
    )(source_field, cotangent, out_modes, gain, wide(channel_bias), *forward, *back)

    grad_modes = spread(grad_partial, 5) * weights
    all_grads = exchange(grad_modes, ("chan",), True, 7)
    all_grads = all_grads.reshape(chans, groups, kx, block, 2, freqs)
    all_grads = all_grads.transpose(5, 4, 2, 0, 1, 3).reshape(freqs, 2, kx, outs)
    weight_grad, back_modes = pl.pallas_call(
        back_kernel,
        grid=(channels // in_block,),
        in_specs=[w_spec, s_spec, mode_spec, limit_spec],
        out_specs=[w_spec, s_spec],
        out_shape=[
            jax.ShapeDtypeStruct(weight.shape, jnp.float32),
            jax.ShapeDtypeStruct(spectra.shape, jnp.float32),
        ],
        compiler_params=params,
        name="back",
    )(weight, spectra, all_grads, limit)
    spectral_grad = weight_grad.transpose(0, 4, 1, 2, 3)

    sent = back_modes.size // LANES
    row_sums = sums[:, 0, :2].T.reshape(-1)
    extra = -(-row_sums.size // (8 * LANES)) * 8
    row_sums = jnp.pad(row_sums, (0, extra * LANES - row_sums.size)).reshape(extra, LANES)
    packed = jnp.concatenate([back_modes.reshape(sent, LANES), row_sums], axis=0)
    parts = joined(packed, 8)
    field_modes = parts[:, :sent].reshape(owners, groups, kx, LANES)
    totals = jnp.sum(parts[:, sent:], axis=0).reshape(-1)
    gate_grad = totals[:channels]
    bias_grad = totals[channels : 2 * channels]
    field_grad = pl.pallas_call(
        functools.partial(last_kernel, modes),
        grid=grid,
        in_specs=[cells, freq_cells, per_channel] + [whole(t) for t in back],
        out_specs=cells,
        out_shape=field,
        compiler_params=params,
        name="last",
    )(grad_sum, field_modes, gain, *back)
    return (output, field_grad, spectral_grad, gate_grad, bias_grad)


def halves_of(table):
    table = table.astype(np.float32)
    high = table.astype(ml_dtypes.bfloat16)
    low = (table - high.astype(np.float32)).astype(ml_dtypes.bfloat16)
    return high, low


def packed_tables(all_rows, all_cols, slabs, modes, freqs, kx_all):
    cell = np.arange(all_cols)[:, None]
    angle = (cell * np.arange(modes * freqs)[None, :] % all_cols) * (2.0 * np.pi / all_cols)
    parts = np.stack([np.cos(angle), -np.sin(angle)], axis=1).reshape(modes, -1, 2, modes, freqs)
    parts = parts.transpose(0, 1, 3, 2, 4)
    cols = parts.shape[1]
    high, low = halves_of(parts)
    ahead = np.stack([high, low], axis=3).reshape(modes, cols, -1)
    ahead = np.concatenate([ahead, ahead], axis=1)
    flat_high = high.reshape(modes, cols, -1).transpose(0, 2, 1)
    flat_low = low.reshape(modes, cols, -1).transpose(0, 2, 1)
    behind = np.concatenate([flat_high, flat_low, flat_high, flat_low], axis=1)
    wave = np.arange(kx_all)
    wave = wave + np.where(2 * wave >= kx_all, all_rows - kx_all, 0)
    angle = (np.arange(all_rows)[:, None] * wave[None, :] % all_rows) * (2.0 * np.pi / all_rows)
    table = np.concatenate([np.cos(angle), np.sin(angle)], axis=1).reshape(slabs, -1, 2 * kx_all)
    high, low = halves_of(table)
    row_behind = np.concatenate([high, high, low], axis=2)
    high, low = high.transpose(0, 2, 1), low.transpose(0, 2, 1)
    row_ahead = np.concatenate([high, low, high], axis=2)
    return ahead, row_ahead, row_behind, behind


def lane_roll(values, shift):
    shift = shift % values.shape[-1]
    return values if shift == 0 else pltpu.roll(values, shift, values.ndim - 1)


def lanes_of(shape):
    return lax.broadcasted_iota(jnp.int32, shape, len(shape) - 1)


def high_low(values):
    high = values.astype(jnp.bfloat16)
    return high, (values - high.astype(jnp.float32)).astype(jnp.bfloat16)


def quarter_turn(values, span, sign):
    half = span // 2
    first = lanes_of(values.shape) % span < half
    back, ahead = lane_roll(values, -half), lane_roll(values, half)
    return jnp.where(first, -back, ahead) if sign > 0 else jnp.where(first, back, -ahead)


def mix_rows(lines, row_table, rows, span, out_ref, kx):
    block = LANES // span
    mixed = []
    for c in range(0, block, 2):
        pair = jnp.concatenate([lines[c * rows : (c + 1) * rows], lines[(c + 1) * rows : (c + 2) * rows]], axis=1)
        high, low = high_low(pair)
        both = jnp.dot(row_table, jnp.concatenate([high, high, low], axis=0), preferred_element_type=jnp.float32)
        mixed += [both[:, :LANES], both[:, LANES:]]
    lane = lanes_of(mixed[0].shape)
    pairs = []
    for c in range(0, block, 2):
        left = mixed[c] + lane_roll(mixed[c], -span)
        right = mixed[c + 1] + lane_roll(mixed[c + 1], span)
        pairs.append(jnp.where(lane % (2 * span) < span, left, right))
    low_half = lane < LANES // 2
    owners = [
        jnp.where(low_half, pairs[0], lane_roll(pairs[1], LANES // 2)),
        jnp.where(low_half, lane_roll(pairs[0], LANES // 2), pairs[1]),
    ]
    all_kx = owners[0].shape[0] // 2
    slabs = all_kx // kx
    for m, values in enumerate(owners):
        done = values[:all_kx] + quarter_turn(values[all_kx:], span, -1)
        for s in range(slabs):
            out_ref[m * slabs + s, 0] = done[s * kx : (s + 1) * kx]


def spectrum_packed(span, x_ref, ahead_ref, row_ref, out_ref):
    block, rows, cols = x_ref.shape
    high, low = high_low(x_ref[...].reshape(block * rows, cols))
    lines = jnp.dot(jnp.concatenate([high, low], axis=1), ahead_ref[0], preferred_element_type=jnp.float32)
    mix_rows(lines, row_ref[0], rows, span, out_ref, out_ref.shape[2])


def group_lines(modes_ref, row_table, span):
    block = LANES // span
    owners = modes_ref.shape[0]
    half = owners // 2
    stack = []
    for m in range(2):
        stack.append(jnp.concatenate([modes_ref[m * half + s, 0] for s in range(half)], axis=0))
    full = [jnp.concatenate([one, quarter_turn(one, span, 1)], axis=0) for one in stack]
    rolled = [[lane_roll(one, k * span) for k in range(block)] for one in full]
    lane = lanes_of(full[0].shape)
    even = lane % (2 * span) < span
    low_half = lane < LANES // 2
    sides = []
    for c in range(block):
        first = jnp.where(low_half, rolled[0][(0 - c) % block], rolled[0][(2 - c) % block])
        second = jnp.where(low_half, rolled[1][(1 - c) % block], rolled[1][(3 - c) % block])
        sides.append(jnp.where(even, first, second))
    lines = []
    for c in range(0, block, 2):
        high, low = high_low(jnp.concatenate([sides[c], sides[c + 1]], axis=1))
        both = jnp.dot(row_table, jnp.concatenate([high, low, high], axis=0), preferred_element_type=jnp.float32)
        lines += [both[:, :LANES], both[:, LANES:]]
    return lines


def branch_of(lines, behind):
    high, low = high_low(lines)
    return jnp.dot(jnp.concatenate([high, low], axis=1), behind, preferred_element_type=jnp.float32)


def middle_packed(
    span, x_ref, cot_ref, modes_ref, gain_ref, bias_ref, ahead_ref, row_ref, row_back_ref, behind_ref,
    out_ref, grad_ref, spec_ref, sums_ref, split_ref,
):
    block, rows, cols = x_ref.shape
    step = pl.program_id(0)
    scale = math.sqrt(2.0 / math.pi)

    @pl.when(step == 0)
    def _():
        sums_ref[...] = jnp.zeros_like(sums_ref)

    lines = group_lines(modes_ref, row_back_ref[0], span)
    lane = lanes_of(sums_ref.shape)
    line = lax.broadcasted_iota(jnp.int32, sums_ref.shape, 0)
    for c in range(block):
        source = x_ref[c]
        v = branch_of(lines[c], behind_ref[0]) + (gain_ref[step * block + c] * source + bias_ref[step * block + c])
        square = v * v
        inner = v * (scale + (scale * 0.044715) * square)
        up = 0.5 + 0.5 * jnp.tanh(inner)
        out_ref[c] = v * up
        bend = v * (2.0 * scale + (6.0 * scale * 0.044715) * square)
        grad = cot_ref[c] * (up + (up * (1.0 - up)) * bend)
        grad_ref[step * block + c] = grad
        high, low = high_low(grad)
        split_ref[c * rows : (c + 1) * rows, :cols] = high
        split_ref[c * rows : (c + 1) * rows, cols:] = low
        gate = jnp.sum(jnp.sum(grad * source, axis=0, keepdims=True), axis=1, keepdims=True)
        bias = jnp.sum(jnp.sum(grad, axis=0, keepdims=True), axis=1, keepdims=True)
        here = (lane == step * block + c) & (line < 2)
        sums_ref[...] = jnp.where(here, jnp.where(line == 0, gate, bias), sums_ref[...])
    made = jnp.dot(split_ref[...], ahead_ref[0], preferred_element_type=jnp.float32)
    mix_rows(made, row_ref[0], rows, span, spec_ref, spec_ref.shape[2])


def last_packed(
    span, kx, grad_ref, modes_ref, gain_ref, row_back_ref, behind_ref, grads_ref, spec_ref, limit_ref, out_ref, wgrad_ref
):
    block = out_ref.shape[0]
    step = pl.program_id(0)
    lines = group_lines(modes_ref, row_back_ref[0], span)
    count, freqs, outs = wgrad_ref.shape[0], wgrad_ref.shape[1], wgrad_ref.shape[4]
    wide = freqs * kx
    first = lax.axis_index("chan") * (count * pl.num_programs(0)) + step * count
    g_real, g_imag = both_parts(grads_ref, slice(None))
    for i in range(count):
        keep = jnp.broadcast_to(limit_ref[:, :1], (outs, wide)) > first + i
        s_real, s_imag = both_parts(spec_ref, pl.ds(step * count + i, 1))
        real = jnp.where(keep, s_real * g_real + s_imag * g_imag, 0.0)
        imag = jnp.where(keep, s_real * g_imag - s_imag * g_real, 0.0)
        wgrad_ref[i, :, 0] = real.T.reshape(freqs, kx, outs)
        wgrad_ref[i, :, 1] = imag.T.reshape(freqs, kx, outs)
    for c in range(block):
        out_ref[c] = branch_of(lines[c], behind_ref[0]) + gain_ref[step * block + c] * grad_ref[step * block + c]


def swap_groups(values, kx):
    lane = lanes_of(values.shape) // kx
    line = lax.broadcasted_iota(jnp.int32, values.shape, 1)
    count = values.shape[1]
    hop = 1
    while hop < count:
        up = lane_roll(pltpu.roll(values, count - hop, 1), hop * kx)
        down = lane_roll(pltpu.roll(values, hop, 1), -hop * kx)
        lane_bit, line_bit = lane // hop % 2, line // hop % 2
        values = jnp.where(lane_bit == line_bit, values, jnp.where(lane_bit == 1, up, down))
        hop *= 2
    return values


def to_lanes(packed, out_ref, kx):
    lines = swap_groups(packed.T.reshape(-1, 8, LANES), kx)
    wide = out_ref.shape[0]
    block = lines.shape[0] // wide
    for c in range(block):
        for j in range(wide):
            out_ref[j, pl.ds(c, 8, stride=block)] = lines[c * wide + j]


def to_rows(wide_ref, block, kx):
    wide = wide_ref.shape[0]
    pieces = []
    for c in range(block):
        for j in range(wide):
            pieces.append(wide_ref[j, pl.ds(c, 8, stride=block)][None])
    return swap_groups(jnp.concatenate(pieces, axis=0), kx).reshape(-1, LANES).T


def both_parts(ref, rows):
    half = ref.shape[0] // 2
    parts = [jnp.concatenate([ref[p * half + j, rows] for j in range(half)], axis=1) for p in range(2)]
    return parts[0], parts[1]


def put_part(ref, rows, part, values):
    half = ref.shape[0] // 2
    for j in range(half):
        ref[part * half + j, rows] = values[:, j * LANES : (j + 1) * LANES]


def other(axis, step, size):
    return lax.rem(lax.axis_index(axis) + step, size)


def send(source, target, sends, recvs, axis, peer):
    copy = pltpu.make_async_remote_copy(
        src_ref=source, dst_ref=target, send_sem=sends, recv_sem=recvs,
        device_id={axis: peer}, device_id_type=pl.DeviceIdType.MESH,
    )
    copy.start()
    return copy


def greet(slabs):
    barrier = pltpu.get_barrier_semaphore()
    targets = [("mode", 1, 2), ("chan", 1, 2)] + [("slab", step, slabs) for step in range(1, slabs)]
    for axis, step, size in targets:
        pl.semaphore_signal(
            barrier, inc=1, device_id={axis: other(axis, step, size)}, device_id_type=pl.DeviceIdType.MESH
        )
    pl.semaphore_wait(barrier, len(targets))


def scatter_sum(part_ref, half_ref, give_ref, take_ref, mode_sems, slab_sems, slabs, between):
    me_mode, me_slab = lax.axis_index("mode"), lax.axis_index("slab")
    peer = other("mode", 1, 2)
    order = [slabs // 2] + [step for step in range(1, slabs) if step != slabs // 2] + [0]
    copies = []
    for step in order:
        slab = other("slab", step, slabs)
        copies.append(send(
            part_ref.at[peer * slabs + slab], half_ref.at[step], mode_sems.at[0, step], mode_sems.at[1, step], "mode", peer
        ))
    waits = list(copies)
    out = []
    for step, copy in zip(order, copies):
        copy.wait_recv()
        slab = other("slab", step, slabs)
        total = part_ref[me_mode * slabs + slab] + half_ref[step]
        if step == 0:
            mine = total
        else:
            give_ref[step] = total
            out.append(send(
                give_ref.at[step], take_ref.at[step], slab_sems.at[0, step], slab_sems.at[1, step], "slab", slab
            ))
    between()
    for copy in out:
        copy.wait_recv()
    for step in range(1, slabs):
        mine = mine + take_ref[step]
    return mine, [copy.wait_send for copy in copies + out]


def gather_start(own_ref, out_ref, mode_sems, slab_sems, slabs):
    me = lax.axis_index("mode") * slabs + lax.axis_index("slab")
    copies = []
    for step in [slabs // 2] + [step for step in range(1, slabs) if step != slabs // 2]:
        copies.append(send(
            own_ref, out_ref.at[me], slab_sems.at[0, step], slab_sems.at[1, step], "slab", other("slab", step, slabs)
        ))
    near = send(own_ref, out_ref.at[me], mode_sems.at[0, 0], mode_sems.at[1, 0], "mode", other("mode", 1, 2))
    out_ref[me] = own_ref[...]
    return copies, near


def gather_finish(state, out_ref, mode_sems, slabs, between):
    copies, near = state
    relays = []
    order = [slabs // 2] + [step for step in range(1, slabs) if step != slabs // 2]
    for k in list(range(1, slabs - 1)) + [0]:
        between(k)
        copies[k].wait_recv()
        step = order[k]
        source = lax.axis_index("mode") * slabs + other("slab", slabs - step, slabs)
        relays.append(send(
            out_ref.at[source], out_ref.at[source], mode_sems.at[0, step], mode_sems.at[1, step], "mode", other("mode", 1, 2)
        ))
    near.wait()
    for copy in relays:
        copy.wait()
    for copy in copies:
        copy.wait_send()


def forward_kernel(
    slabs, kx, part_ref, w_ref, limit_ref, weight_ref, out_ref, turned_ref, spec_ref,
    half_ref, give_ref, take_ref, w_buf, t_buf, sum_ref, peer_ref, own_ref,
    mode_a, slab_a, mode_b, slab_b, chan_sems, w_sems, t_sems,
):
    ins, freqs = w_ref.shape[0], w_ref.shape[1]
    outs = w_ref.shape[4]
    mine_outs = outs // 2
    wide = freqs * kx
    for i in range(ins):
        pltpu.make_async_copy(w_ref.at[i], w_buf.at[i], w_sems.at[i]).start()
    greet(slabs)
    first = lax.axis_index("chan") * ins

    def flip():
        def body(i, carry):
            pltpu.make_async_copy(w_ref.at[i], w_buf.at[i], w_sems.at[i]).wait()
            keep = jnp.broadcast_to(limit_ref[:, :1], (outs, wide)) > first + i
            for p in range(2):
                turned = w_buf[i, :, p].reshape(wide, outs).T
                t_buf[i, :, p * wide : (p + 1) * wide] = jnp.where(keep, turned, 0.0)
            pltpu.make_async_copy(t_buf.at[i], turned_ref.at[i], t_sems.at[i]).start()
            return carry
        lax.fori_loop(0, ins, body, 0)

    mine, sent = scatter_sum(part_ref, half_ref, give_ref, take_ref, mode_a, slab_a, slabs, flip)
    to_lanes(mine, spec_ref, kx)

    def contract(i, carry):
        real, imag = carry
        w_real, w_imag = t_buf[i, :, :wide], t_buf[i, :, wide:]
        s_real, s_imag = both_parts(spec_ref, pl.ds(i, 1))
        return real + (s_real * w_real - s_imag * w_imag), imag + (s_real * w_imag + s_imag * w_real)

    zero = jnp.zeros((outs, wide), jnp.float32)
    real, imag = lax.fori_loop(0, ins, contract, (zero, zero))
    put_part(sum_ref, slice(None), 0, real)
    put_part(sum_ref, slice(None), 1, imag)
    theirs = other("chan", 1, 2) * mine_outs
    swap = send(
        sum_ref.at[:, pl.ds(theirs, mine_outs)], peer_ref, chan_sems.at[0], chan_sems.at[1], "chan", other("chan", 1, 2)
    )
    swap.wait_recv()
    for j in range(peer_ref.shape[0]):
        peer_ref[j] = (sum_ref[j, pl.ds(first, mine_outs)] + peer_ref[j]) * weight_ref[j % weight_ref.shape[0]]
    own_ref[...] = to_rows(peer_ref, mine_outs // 8, kx)
    state = gather_start(own_ref, out_ref, mode_b, slab_b, slabs)
    gather_finish(state, out_ref, mode_b, slabs, lambda k: None)
    swap.wait_send()
    for wait in sent:
        wait()

    def settle(i, carry):
        pltpu.make_async_copy(t_buf.at[i], turned_ref.at[i], t_sems.at[i]).wait()
        return carry
    lax.fori_loop(0, ins, settle, 0)


def backward_kernel(
    slabs, kx, part_ref, sums_ref, turned_ref, weight_ref, out_ref, grad_ref, total_ref,
    half_ref, give_ref, take_ref, t_buf, back_ref, own_ref, near_ref, far_ref, pass_ref,
    mode_a, slab_a, mode_b, slab_b, chan_sems, t_sems, sum_mode, sum_slab,
):
    ins, outs, wide = turned_ref.shape[0], turned_ref.shape[1], turned_ref.shape[2] // 2
    mine_outs = outs // 2
    for i in range(ins):
        pltpu.make_async_copy(turned_ref.at[i], t_buf.at[i], t_sems.at[i]).start()
    greet(slabs)
    first = lax.axis_index("chan") * ins
    near = send(sums_ref, near_ref, sum_mode.at[0], sum_mode.at[1], "mode", other("mode", 1, 2))

    far = []
    def total_up():
        near.wait_recv()
        pass_ref[...] = sums_ref[...] + near_ref[...]
        for step in range(1, slabs):
            far.append(send(
                pass_ref, far_ref.at[step], sum_slab.at[0, step], sum_slab.at[1, step], "slab", other("slab", step, slabs)
            ))

    mine, sent = scatter_sum(part_ref, half_ref, give_ref, take_ref, mode_a, slab_a, slabs, total_up)
    to_lanes(mine, back_ref, kx)
    here = pl.ds(first, mine_outs)
    for j in range(back_ref.shape[0]):
        grad_ref[j, here] = back_ref[j] * weight_ref[j % weight_ref.shape[0]]
    swap = send(
        grad_ref.at[:, here], grad_ref.at[:, here], chan_sems.at[0], chan_sems.at[1], "chan", other("chan", 1, 2)
    )

    def arrive(i, carry):
        pltpu.make_async_copy(turned_ref.at[i], t_buf.at[i], t_sems.at[i]).wait()
        return carry
    lax.fori_loop(0, ins, arrive, 0)
    swap.wait_recv()

    def pull(i, carry):
        w_real, w_imag = t_buf[i, :, :wide], t_buf[i, :, wide:]
        g_real, g_imag = both_parts(grad_ref, slice(None))
        put_part(back_ref, pl.ds(i, 1), 0, jnp.sum(g_real * w_real + g_imag * w_imag, axis=0, keepdims=True))
        put_part(back_ref, pl.ds(i, 1), 1, jnp.sum(g_imag * w_real - g_real * w_imag, axis=0, keepdims=True))
        return carry
    lax.fori_loop(0, ins, pull, 0)
    own_ref[...] = to_rows(back_ref, ins // 8, kx)
    state = gather_start(own_ref, out_ref, mode_b, slab_b, slabs)
    gather_finish(state, out_ref, mode_b, slabs, lambda k: None)
    total = pass_ref[...]
    for step, copy in zip(range(1, slabs), far):
        copy.wait()
        total = total + far_ref[step]
    total_ref[...] = total
    near.wait_send()
    swap.wait_send()
    for wait in sent:
        wait()


def fits(shapes, mesh_sizes):
    channels, rows, cols = shapes[0]
    outs, freqs, kx = shapes[2][1], shapes[2][2], shapes[2][4]
    slabs, modes, chans = mesh_sizes
    return (
        modes == 2 and chans == 2 and slabs > 2 and slabs % 2 == 0
        and 8 * kx == LANES and 8 * freqs == LANES and 2 * freqs * channels == 8 * LANES
        and outs == chans * channels
        and rows % LANES == 0 and cols % LANES == 0
    )


def local(source_field, cotangent, spectral_weight, skip_gain, channel_bias, mode_limit, width_limit):
    slabs, modes, chans = (lax.axis_size(axis) for axis in ("slab", "mode", "chan"))
    args = (source_field, cotangent, spectral_weight, skip_gain, channel_bias, mode_limit, width_limit)
    if not fits([one.shape for one in args], (slabs, modes, chans)):
        return local_plain(*args)
    channels, rows, cols = source_field.shape
    outs, freqs, kx = spectral_weight.shape[1], spectral_weight.shape[2], spectral_weight.shape[4]
    span = 2 * freqs
    block = LANES // span
    groups = channels // block
    owners = slabs * modes
    all_kx, all_rows, all_cols = kx * slabs, rows * slabs, cols * modes
    wide = freqs * kx
    ahead, row_ahead, row_behind, behind = (
        jnp.asarray(t) for t in packed_tables(all_rows, all_cols, slabs, modes, freqs, all_kx)
    )
    slab_index, mode_index, chan_index = (lax.axis_index(axis) for axis in ("slab", "mode", "chan"))

    def pick(table, axis):
        return pl.BlockSpec((1,) + table.shape[1:], lambda g: (lax.axis_index(axis), 0, 0))

    cells = pl.BlockSpec((block, rows, cols), lambda g: (g, 0, 0))
    freq_cells = pl.BlockSpec((owners, 1, kx, LANES), lambda g: (0, g, 0, 0))
    scalars = pl.BlockSpec(memory_space=pltpu.SMEM)
    small = pl.BlockSpec((8, LANES), lambda g: (0, 0))
    field = jax.ShapeDtypeStruct(source_field.shape, jnp.float32)
    freq_field = jax.ShapeDtypeStruct((owners, groups, kx, LANES), jnp.float32)
    params = pltpu.CompilerParams(dimension_semantics=("arbitrary",), vmem_limit_bytes=40 * 1024 * 1024)
    f32 = jnp.float32

    partial = pl.pallas_call(
        functools.partial(spectrum_packed, span),
        grid=(groups,),
        in_specs=[cells, pick(ahead, "mode"), pick(row_ahead, "slab")],
        out_specs=freq_cells,
        out_shape=freq_field,
        compiler_params=params,
        name="spectrum",
    )(source_field, ahead, row_ahead)

    weight = spectral_weight.transpose(0, 2, 3, 4, 1)
    col_freq = mode_index * freqs + jnp.arange(freqs, dtype=jnp.int32)
    row_freq = slab_index * kx + jnp.arange(kx, dtype=jnp.int32)
    limit_rows = lax.dynamic_slice_in_dim(mode_limit, chan_index * channels, channels, 0)
    flat_cols, flat_rows = jnp.repeat(col_freq, kx)[None, :], jnp.tile(row_freq, freqs)[None, :]
    kept = (flat_cols < limit_rows[:, 0:1]) & (
        (flat_rows < limit_rows[:, 1:2]) | (all_kx - flat_rows < limit_rows[:, 1:2])
    )
    scales = jnp.where(flat_cols == 0, 1.0, 2.0).astype(jnp.float32) / (all_rows * all_cols)
    weights = jnp.where(kept, scales, 0.0).reshape(channels, -1, LANES).transpose(1, 0, 2)
    limit = jnp.broadcast_to(width_limit[:, None], (outs, LANES))

    dma, vmem = pltpu.SemaphoreType.DMA, pltpu.VMEM
    in_vmem, anywhere = pl.BlockSpec(memory_space=pltpu.VMEM), pl.BlockSpec(memory_space=pl.ANY)
    piece = (groups * kx, LANES)
    common = [vmem((slabs,) + piece, f32), vmem((slabs,) + piece, f32), vmem((slabs,) + piece, f32)]
    pair = [dma((2, slabs))] * 4
    comm = lambda ident, room: pltpu.CompilerParams(
        collective_id=ident, has_side_effects=True, vmem_limit_bytes=room * MIB
    )
    gathered = jax.ShapeDtypeStruct((owners,) + piece, f32)
    flat = lambda lines: (2 * wide // LANES, lines, LANES)
    turned_shape = jax.ShapeDtypeStruct((channels, outs, 2 * wide), f32)

    out_modes, turned, spec = pl.pallas_call(
        functools.partial(forward_kernel, slabs, kx),
        in_specs=[in_vmem, anywhere, in_vmem, in_vmem],
        out_specs=[in_vmem, anywhere, in_vmem],
        out_shape=[gathered, turned_shape, jax.ShapeDtypeStruct(flat(channels), f32)],
        scratch_shapes=common + [
            vmem(weight.shape, f32), vmem(turned_shape.shape, f32), vmem(flat(outs), f32),
            vmem(flat(outs // 2), f32), vmem(piece, f32),
        ] + pair + [dma((2,)), dma((channels,)), dma((channels,))],
        compiler_params=comm(20, 30),
        name="forward_modes",
    )(partial.reshape((owners,) + piece), weight, limit, weights)

    output, grad_sum, grad_partial, sums = pl.pallas_call(
        functools.partial(middle_packed, span),
        grid=(groups,),
        in_specs=[
            cells, cells, freq_cells, scalars, scalars, pick(ahead, "mode"), pick(row_ahead, "slab"),
            pick(row_behind, "slab"), pick(behind, "mode"),
        ],
        out_specs=[cells, in_vmem, freq_cells, small],
        out_shape=[field, pltpu.VMEM(field.shape, f32), freq_field, jax.ShapeDtypeStruct((8, LANES), f32)],
        scratch_shapes=[vmem((block * rows, 2 * cols), jnp.bfloat16)],
        compiler_params=params,
        name="middle",
    )(
        source_field, cotangent, out_modes.reshape(freq_field.shape), skip_gain, channel_bias,
        ahead, row_ahead, row_behind, behind,
    )

    back_modes, all_grads, totals = pl.pallas_call(
        functools.partial(backward_kernel, slabs, kx),
        in_specs=[in_vmem, in_vmem, anywhere, in_vmem],
        out_specs=[in_vmem, in_vmem, in_vmem],
        out_shape=[gathered, jax.ShapeDtypeStruct(flat(outs), f32), jax.ShapeDtypeStruct((8, LANES), f32)],
        scratch_shapes=common + [
            vmem(turned_shape.shape, f32), vmem(flat(channels), f32), vmem(piece, f32), vmem((8, LANES), f32),
            vmem((slabs, 8, LANES), f32), vmem((8, LANES), f32),
        ] + pair + [dma((2,)), dma((channels,)), dma((2,)), dma((2, slabs))],
        compiler_params=comm(21, 16),
        name="backward_modes",
    )(grad_partial.reshape((owners,) + piece), sums, turned, weights)

    count = channels // groups
    whole = lambda array: pl.BlockSpec(array.shape, lambda g: (0,) * array.ndim)
    field_grad, weight_grad = pl.pallas_call(
        functools.partial(last_packed, span, kx),
        grid=(groups,),
        in_specs=[
            in_vmem, freq_cells, scalars, pick(row_behind, "slab"), pick(behind, "mode"),
            whole(all_grads), whole(spec), whole(limit),
        ],
        out_specs=[cells, pl.BlockSpec((count,) + weight.shape[1:], lambda g: (g, 0, 0, 0, 0))],
        out_shape=[field, jax.ShapeDtypeStruct(weight.shape, f32)],
        compiler_params=params,
        name="last",
    )(
        pltpu.with_memory_space_constraint(grad_sum, pltpu.VMEM), back_modes.reshape(freq_field.shape), skip_gain,
        row_behind, behind, all_grads, spec, limit,
    )
    spectral_grad = weight_grad.transpose(0, 4, 1, 2, 3)
    return (output, field_grad, spectral_grad, totals[0, :channels], totals[1, :channels])


def solution(mesh):
    in_specs = (
        P(("member", "chan"), "slab", "mode"),
        P(("member", "chan"), "slab", "mode"),
        P(("member", "chan"), None, "mode", None, "slab"),
        P(("member", "chan")),
        P(("member", "chan")),
        P("member", None),
        P("member"),
    )
    out_specs = (
        P(("member", "chan"), "slab", "mode"),
        P(("member", "chan"), "slab", "mode"),
        P(("member", "chan"), None, "mode", None, "slab"),
        P(("member", "chan")),
        P(("member", "chan")),
    )
    return jax.shard_map(local, mesh=mesh, in_specs=in_specs, out_specs=out_specs, check_vma=False)
```

```python
import functools
import math

import jax
import jax.numpy as jnp
import ml_dtypes
import numpy as np
from jax import lax
from jax.experimental import pallas as pl
from jax.experimental.pallas import tpu as pltpu
from jax.sharding import PartitionSpec as P

LANES = 128
BIG = 60 * 1024 * 1024
MIB = 1024 * 1024
FORWARD, MIDDLE, LAST = 40, 40, 40


def split_table(table):
    high = lax.reduce_precision(table, 8, 7)
    return high.astype(jnp.bfloat16), (table - high).astype(jnp.bfloat16)


def split_block(values):
    high = values.astype(jnp.bfloat16)
    return high, (values - high.astype(jnp.float32)).astype(jnp.bfloat16)


def dot_pair(left, right):
    left_high, left_low = left
    right_high, right_low = right
    mul = functools.partial(jnp.dot, preferred_element_type=jnp.float32)
    return mul(left_high, right_high) + mul(left_low, right_high) + mul(left_high, right_low)


def tables(extent, waves, first_cell, cell_count):
    cell_index = first_cell + jnp.arange(cell_count, dtype=jnp.int32)
    products = (cell_index[:, None] * waves[None, :] % extent).astype(jnp.float32)
    angles = products * (2.0 * math.pi / extent)
    return jnp.cos(angles), jnp.sin(angles)


def store_spectrum(values, col_pair, row_pair, out_ref):
    block, rows, cols = values.shape
    lines = dot_pair(split_block(values.reshape(block * rows, cols)), col_pair)
    all_kx = row_pair[0].shape[0] // 2
    kx, lanes = out_ref.shape[2:]
    span = lanes // block
    mode_count = lines.shape[1] // span
    slabs = out_ref.shape[0] // mode_count
    done = []
    for c in range(block):
        mixed = dot_pair(row_pair, split_block(lines[c * rows : (c + 1) * rows]))
        done.append(mixed[:all_kx] - turn(mixed[all_kx:], span))
    for m in range(mode_count):
        packed = jnp.concatenate([one[:, m * span : (m + 1) * span] for one in done], axis=1)
        for s in range(slabs):
            out_ref[m * slabs + s, 0] = packed[s * kx : (s + 1) * kx]


def turn(values, span):
    half = span // 2
    pieces = []
    for first in range(0, values.shape[1], span):
        pieces.append(-values[:, first + half : first + span])
        pieces.append(values[:, first : first + half])
    return jnp.concatenate(pieces, axis=1)


def all_modes(modes_ref, mode_count, c, block):
    span = modes_ref.shape[3] // block
    slabs = modes_ref.shape[0] // mode_count
    columns = []
    for m in range(mode_count):
        stack = [modes_ref[m * slabs + s, 0] for s in range(slabs)]
        columns.append(jnp.concatenate(stack, axis=0)[:, c * span : (c + 1) * span])
    return jnp.concatenate(columns, axis=1), span


def synth(modes_and_span, row_pair, col_pair):
    modes, span = modes_and_span
    stacked = jnp.concatenate([modes, turn(modes, span)], axis=0)
    lines = dot_pair(row_pair, split_block(stacked))
    return dot_pair(split_block(lines), col_pair)


def spectrum_kernel(x_ref, ch_ref, cl_ref, rh_ref, rl_ref, out_ref):
    store_spectrum(x_ref[...], (ch_ref[...], cl_ref[...]), (rh_ref[...], rl_ref[...]), out_ref)


def middle_kernel(
    mode_count, x_ref, cot_ref, modes_ref, gain_ref, bias_ref, ch_ref, cl_ref, rh_ref, rl_ref,
    cth_ref, ctl_ref, ih_ref, il_ref, out_ref, grad_ref, spec_ref, sums_ref,
):
    block = x_ref.shape[0]
    row_back = (ih_ref[...], il_ref[...])
    col_back = (cth_ref[...], ctl_ref[...])
    scale = math.sqrt(2.0 / math.pi)
    for c in range(block):
        source = x_ref[c]
        gain = gain_ref[c]
        v = synth(all_modes(modes_ref, mode_count, c, block), row_back, col_back) + gain[:, :1] * source + bias_ref[c][:, :1]
        square = v * v
        t = jnp.tanh(scale * v * (1.0 + 0.044715 * square))
        half_up = 0.5 * (1.0 + t)
        out_ref[c] = v * half_up
        slope = half_up + 0.5 * v * (1.0 - t * t) * (scale * (1.0 + 3.0 * 0.044715 * square))
        grad = cot_ref[c] * slope
        grad_ref[c] = grad
        gate = jnp.sum(jnp.sum(grad * source, axis=0, keepdims=True), axis=1, keepdims=True)
        bias = jnp.sum(jnp.sum(grad, axis=0, keepdims=True), axis=1, keepdims=True)
        lane = lax.broadcasted_iota(jnp.int32, (1, LANES), 1)
        sums_ref[c] = jnp.where(lane == 0, gate, bias)
    store_spectrum(
        grad_ref[...], (ch_ref[...], cl_ref[...]), (rh_ref[...], rl_ref[...]), spec_ref
    )


def last_kernel(mode_count, grad_ref, modes_ref, gain_ref, cth_ref, ctl_ref, ih_ref, il_ref, out_ref):
    block = grad_ref.shape[0]
    for c in range(block):
        modes = all_modes(modes_ref, mode_count, c, block)
        branch = synth(modes, (ih_ref[...], il_ref[...]), (cth_ref[...], ctl_ref[...]))
        out_ref[c] = branch + gain_ref[c][:, :1] * grad_ref[c]


def contract_kernel(w_ref, spec_ref, limit_ref, out_ref):
    block, freqs, _, kx, outs = w_ref.shape
    first = lax.axis_index("chan") * (block * pl.num_programs(0)) + pl.program_id(0) * block

    @pl.when(pl.program_id(0) == 0)
    def _():
        out_ref[...] = jnp.zeros_like(out_ref)

    limit = limit_ref[...]
    for y in range(freqs):
        real = out_ref[y, 0]
        imag = out_ref[y, 1]
        for i in range(block):
            keep = first + i < limit
            spec = spec_ref[0]
            at = 2 * freqs * i + y
            s_real = jnp.where(keep, spec[:, at : at + 1], 0.0)
            s_imag = jnp.where(keep, spec[:, freqs + at : freqs + at + 1], 0.0)
            w_real = w_ref[i, y, 0]
            w_imag = w_ref[i, y, 1]
            real = real + (s_real * w_real - s_imag * w_imag)
            imag = imag + (s_real * w_imag + s_imag * w_real)
        out_ref[y, 0] = real
        out_ref[y, 1] = imag


def back_kernel(w_ref, spec_ref, grads_ref, limit_ref, wgrad_ref, out_ref):
    block, freqs, _, kx, outs = w_ref.shape
    first = lax.axis_index("chan") * (block * pl.num_programs(0)) + pl.program_id(0) * block
    limit = limit_ref[...]
    lane = lax.broadcasted_iota(jnp.int32, out_ref.shape[1:], 1)
    spec = spec_ref[0]
    back = jnp.zeros(out_ref.shape[1:], jnp.float32)
    for i in range(block):
        keep = first + i < limit
        for y in range(freqs):
            at = 2 * freqs * i + y
            g_real = jnp.where(keep, grads_ref[y, 0], 0.0)
            g_imag = jnp.where(keep, grads_ref[y, 1], 0.0)
            s_real = spec[:, at : at + 1]
            s_imag = spec[:, freqs + at : freqs + at + 1]
            wgrad_ref[i, y, 0] = s_real * g_real + s_imag * g_imag
            wgrad_ref[i, y, 1] = s_real * g_imag - s_imag * g_real
            w_real = w_ref[i, y, 0]
            w_imag = w_ref[i, y, 1]
            b_real = jnp.sum(g_real * w_real + g_imag * w_imag, axis=1, keepdims=True)
            b_imag = jnp.sum(g_imag * w_real - g_real * w_imag, axis=1, keepdims=True)
            back = jnp.where(lane == at, b_real, back)
            back = jnp.where(lane == freqs + at, b_imag, back)
    out_ref[0] = back


def exchange_kernel(axes, sizes, gather, x_ref, out_ref, send_sem, recv_sem, own_sem):
    total = math.prod(sizes)
    me = lax.axis_index(axes[0])
    for axis, size in zip(axes[1:], sizes[1:]):
        me = me * size + lax.axis_index(axis)

    def place(index):
        coords = {}
        for axis, size in reversed(list(zip(axes, sizes))):
            coords[axis] = lax.rem(index, size)
            index = lax.div(index, size)
        return coords

    barrier = pltpu.get_barrier_semaphore()
    for step in range(1, total):
        pl.semaphore_signal(
            barrier, inc=1, device_id=place(lax.rem(me + step, total)),
            device_id_type=pl.DeviceIdType.MESH,
        )
    pl.semaphore_wait(barrier, total - 1)
    copies = []
    for step in range(1, total):
        peer = lax.rem(me + step, total)
        copy = pltpu.make_async_remote_copy(
            src_ref=x_ref if gather else x_ref.at[peer],
            dst_ref=out_ref.at[me],
            send_sem=send_sem.at[step],
            recv_sem=recv_sem.at[step],
            device_id=place(peer),
            device_id_type=pl.DeviceIdType.MESH,
        )
        copy.start()
        copies.append(copy)
    own = pltpu.make_async_copy(x_ref if gather else x_ref.at[me], out_ref.at[me], own_sem)
    own.start()
    own.wait()
    for copy in copies:
        copy.wait()


def exchange(values, axes, gather, ident):
    sizes = tuple(lax.axis_size(axis) for axis in axes)
    total = math.prod(sizes)
    piece = values.shape if gather else values.shape[1:]
    flat = values.reshape((-1, LANES) if gather else (total, -1, LANES))
    out = pl.pallas_call(
        functools.partial(exchange_kernel, axes, sizes, gather),
        out_shape=jax.ShapeDtypeStruct((total,) + flat.shape[-2:], jnp.float32),
        in_specs=[pl.BlockSpec(memory_space=pltpu.VMEM)],
        out_specs=pl.BlockSpec(memory_space=pltpu.VMEM),
        scratch_shapes=[
            pltpu.SemaphoreType.DMA((total,)),
            pltpu.SemaphoreType.DMA((total,)),
            pltpu.SemaphoreType.DMA,
        ],
        compiler_params=pltpu.CompilerParams(collective_id=ident, has_side_effects=True),
        name="exchange" + str(ident),
    )(flat)
    return out.reshape((total,) + piece)


def mode_weights(limit_rows, col_freq, row_freq, kx_count, cells_total):
    keep_cols = col_freq[None, :] < limit_rows[:, 0:1]
    keep_rows = (row_freq[None, :] < limit_rows[:, 1:2]) | (
        (kx_count - row_freq)[None, :] < limit_rows[:, 1:2]
    )
    scales = jnp.where(col_freq == 0, 1.0, 2.0).astype(jnp.float32) / cells_total
    joined = keep_rows[:, :, None] & keep_cols[:, None, :]
    return (joined.astype(jnp.float32) * scales[None, None, :])[:, :, None, :]


def local_plain(
    source_field, cotangent, spectral_weight, skip_gain, channel_bias, mode_limit, width_limit
):
    channels, row_count, col_count = source_field.shape
    slabs = lax.axis_size("slab")
    modes = lax.axis_size("mode")
    chans = lax.axis_size("chan")
    slab_index = lax.axis_index("slab")
    mode_index = lax.axis_index("mode")
    chan_index = lax.axis_index("chan")
    outs = spectral_weight.shape[1]
    freqs = spectral_weight.shape[2]
    kx = spectral_weight.shape[4]
    all_freqs = freqs * modes
    all_kx = kx * slabs
    all_rows = row_count * slabs
    all_cols = col_count * modes

    col_waves = jnp.arange(all_freqs, dtype=jnp.int32)
    row_waves = jnp.arange(all_kx, dtype=jnp.int32)
    row_waves = row_waves + jnp.where(2 * row_waves >= all_kx, all_rows - all_kx, 0)
    col_cos, col_sin = tables(all_cols, col_waves, mode_index * col_count, col_count)
    row_cos, row_sin = tables(all_rows, row_waves, slab_index * row_count, row_count)
    col_tab = jnp.stack(
        [col_cos.reshape(-1, modes, freqs), -col_sin.reshape(-1, modes, freqs)], axis=2
    ).reshape(col_count, 2 * all_freqs)
    row_tab = jnp.concatenate([row_cos, row_sin], axis=1)
    col_pair = split_table(col_tab)
    col_back = tuple(part.T for part in col_pair)
    row_back = split_table(row_tab)
    row_pair = tuple(part.T for part in row_back)

    block = LANES // (2 * freqs)
    groups = channels // block
    owners = slabs * modes
    cells = pl.BlockSpec((block, row_count, col_count), lambda c: (c, 0, 0))
    freq_cells = pl.BlockSpec((owners, 1, kx, LANES), lambda c: (0, c, 0, 0))
    per_channel = pl.BlockSpec((block, 1, LANES), lambda c: (c, 0, 0))
    field = jax.ShapeDtypeStruct(source_field.shape, jnp.float32)
    freq_field = jax.ShapeDtypeStruct((owners, groups, kx, LANES), jnp.float32)
    params = pltpu.CompilerParams(
        dimension_semantics=("arbitrary",), vmem_limit_bytes=BIG
    )

    def whole(array):
        return pl.BlockSpec(array.shape, lambda c: (0,) * array.ndim)

    grid = (channels // block,)
    wide = lambda values: jnp.broadcast_to(values[:, None, None], (channels, 1, LANES))
    gain = wide(skip_gain)
    forward = col_pair + row_pair
    back = col_back + row_back

    def spread(partial, ident):
        half = exchange(partial.reshape(modes, -1, LANES), ("mode",), False, ident)
        half = jnp.sum(half, axis=0).reshape(slabs, -1, LANES)
        return jnp.sum(exchange(half, ("slab",), False, ident + 1), axis=0).reshape(
            groups, kx, LANES
        )

    def joined(piece, ident):
        half = exchange(piece, ("slab",), True, ident)
        return exchange(half, ("mode",), True, ident + 1).reshape((owners,) + piece.shape)

    spectra = spread(
        pl.pallas_call(
            spectrum_kernel,
            grid=grid,
            in_specs=[cells] + [whole(t) for t in forward],
            out_specs=freq_cells,
            out_shape=freq_field,
            compiler_params=params,
            name="spectrum",
        )(source_field, *forward),
        0,
    )

    weight = spectral_weight.transpose(0, 2, 3, 4, 1)
    limit = width_limit.reshape(1, outs)
    in_block = block
    w_spec = pl.BlockSpec((in_block, freqs, 2, kx, outs), lambda i: (i, 0, 0, 0, 0))
    s_spec = pl.BlockSpec((1, kx, LANES), lambda i: (i, 0, 0))
    mode_spec = pl.BlockSpec((freqs, 2, kx, outs), lambda i: (0, 0, 0, 0))
    limit_spec = pl.BlockSpec((1, outs), lambda i: (0, 0))
    partial_modes = pl.pallas_call(
        contract_kernel,
        grid=(channels // in_block,),
        in_specs=[w_spec, s_spec, limit_spec],
        out_specs=mode_spec,
        out_shape=jax.ShapeDtypeStruct((freqs, 2, kx, outs), jnp.float32),
        compiler_params=params,
        name="contract",
    )(weight, spectra, limit)
    halves = partial_modes.reshape(freqs, 2, kx, chans, groups, block)
    halves = halves.transpose(3, 4, 2, 5, 1, 0).reshape(chans, groups, kx, LANES)
    summed_modes = jnp.sum(exchange(halves, ("chan",), False, 2), axis=0)

    col_freq = mode_index * freqs + jnp.arange(freqs, dtype=jnp.int32)
    row_freq = slab_index * kx + jnp.arange(kx, dtype=jnp.int32)
    limit_rows = lax.dynamic_slice_in_dim(mode_limit, chan_index * channels, channels, 0)
    weights = mode_weights(limit_rows, col_freq, row_freq, all_kx, all_rows * all_cols)
    weights = jnp.broadcast_to(weights, (channels, kx, 2, freqs))
    weights = weights.reshape(groups, block, kx, 2 * freqs).transpose(0, 2, 1, 3)
    weights = weights.reshape(groups, kx, LANES)
    out_modes = joined(summed_modes * weights, 3)

    output, grad_sum, grad_partial, sums = pl.pallas_call(
        functools.partial(middle_kernel, modes),
        grid=grid,
        in_specs=[cells, cells, freq_cells, per_channel, per_channel]
        + [whole(t) for t in forward + back],
        out_specs=[cells, cells, freq_cells, per_channel],
        out_shape=[
            field,
            field,
            freq_field,
            jax.ShapeDtypeStruct((channels, 1, LANES), jnp.float32),
        ],
        compiler_params=params,
        name="middle",
    )(source_field, cotangent, out_modes, gain, wide(channel_bias), *forward, *back)

    grad_modes = spread(grad_partial, 5) * weights
    all_grads = exchange(grad_modes, ("chan",), True, 7)
    all_grads = all_grads.reshape(chans, groups, kx, block, 2, freqs)
    all_grads = all_grads.transpose(5, 4, 2, 0, 1, 3).reshape(freqs, 2, kx, outs)
    weight_grad, back_modes = pl.pallas_call(
        back_kernel,
        grid=(channels // in_block,),
        in_specs=[w_spec, s_spec, mode_spec, limit_spec],
        out_specs=[w_spec, s_spec],
        out_shape=[
            jax.ShapeDtypeStruct(weight.shape, jnp.float32),
            jax.ShapeDtypeStruct(spectra.shape, jnp.float32),
        ],
        compiler_params=params,
        name="back",
    )(weight, spectra, all_grads, limit)
    spectral_grad = weight_grad.transpose(0, 4, 1, 2, 3)

    sent = back_modes.size // LANES
    row_sums = sums[:, 0, :2].T.reshape(-1)
    extra = -(-row_sums.size // (8 * LANES)) * 8
    row_sums = jnp.pad(row_sums, (0, extra * LANES - row_sums.size)).reshape(extra, LANES)
    packed = jnp.concatenate([back_modes.reshape(sent, LANES), row_sums], axis=0)
    parts = joined(packed, 8)
    field_modes = parts[:, :sent].reshape(owners, groups, kx, LANES)
    totals = jnp.sum(parts[:, sent:], axis=0).reshape(-1)
    gate_grad = totals[:channels]
    bias_grad = totals[channels : 2 * channels]
    field_grad = pl.pallas_call(
        functools.partial(last_kernel, modes),
        grid=grid,
        in_specs=[cells, freq_cells, per_channel] + [whole(t) for t in back],
        out_specs=cells,
        out_shape=field,
        compiler_params=params,
        name="last",
    )(grad_sum, field_modes, gain, *back)
    return (output, field_grad, spectral_grad, gate_grad, bias_grad)


def halves_of(table):
    table = table.astype(np.float32)
    high = table.astype(ml_dtypes.bfloat16)
    low = (table - high.astype(np.float32)).astype(ml_dtypes.bfloat16)
    return high, low


def packed_tables(all_rows, all_cols, slabs, modes, freqs, kx_all):
    cell = np.arange(all_cols)[:, None]
    angle = (cell * np.arange(modes * freqs)[None, :] % all_cols) * (2.0 * np.pi / all_cols)
    parts = np.stack([np.cos(angle), -np.sin(angle)], axis=1).reshape(modes, -1, 2, modes, freqs)
    parts = parts.transpose(0, 1, 3, 2, 4)
    cols = parts.shape[1]
    high, low = halves_of(parts)
    ahead = np.stack([high, low], axis=3).reshape(modes, cols, -1)
    flat_high = high.reshape(modes, cols, -1).transpose(0, 2, 1)
    flat_low = low.reshape(modes, cols, -1).transpose(0, 2, 1)
    behind = np.concatenate([flat_high, flat_low], axis=1)
    wave = np.arange(kx_all)
    wave = wave + np.where(2 * wave >= kx_all, all_rows - kx_all, 0)
    angle = (np.arange(all_rows)[:, None] * wave[None, :] % all_rows) * (2.0 * np.pi / all_rows)
    table = np.concatenate([np.cos(angle), np.sin(angle)], axis=1).reshape(slabs, -1, 2 * kx_all)
    high, low = halves_of(table)
    row_behind = np.concatenate([high, low], axis=2)
    high, low = high.transpose(0, 2, 1), low.transpose(0, 2, 1)
    row_ahead = np.concatenate([high, low], axis=2)
    return ahead, row_ahead, row_behind, behind


def lane_roll(values, shift):
    shift = shift % values.shape[-1]
    return values if shift == 0 else pltpu.roll(values, shift, values.ndim - 1)


def lanes_of(shape):
    return lax.broadcasted_iota(jnp.int32, shape, len(shape) - 1)


def high_low(values):
    high = values.astype(jnp.bfloat16)
    return high, (values - high.astype(jnp.float32)).astype(jnp.bfloat16)


def quarter_turn(values, span, sign):
    half = span // 2
    first = lanes_of(values.shape) % span < half
    back, ahead = lane_roll(values, -half), lane_roll(values, half)
    return jnp.where(first, -back, ahead) if sign > 0 else jnp.where(first, back, -ahead)


def three_way(row_table, values):
    high, low = high_low(values)
    width = row_table.shape[1] // 2
    left = jnp.concatenate([row_table, row_table[:, :width]], axis=1)
    right = jnp.concatenate([high, high, low], axis=0)
    return jnp.dot(left, right, preferred_element_type=jnp.float32)


def two_way(values, table):
    high, low = high_low(values)
    both = jnp.concatenate([high, low], axis=1)
    return jnp.dot(both, jnp.concatenate([table, table], axis=0), preferred_element_type=jnp.float32)


def mix_rows(lines_ref, row_table, rows, span, kx, store):
    block = LANES // span
    mixed = []
    for c in range(0, block, 2):
        pair = [lines_ref[(c + k) * rows : (c + k + 1) * rows] for k in range(2)]
        both = three_way(row_table, jnp.concatenate(pair, axis=1))
        mixed += [both[:, :LANES], both[:, LANES:]]
    lane = lanes_of(mixed[0].shape)
    pairs = []
    for c in range(0, block, 2):
        left = mixed[c] + lane_roll(mixed[c], -span)
        right = mixed[c + 1] + lane_roll(mixed[c + 1], span)
        pairs.append(jnp.where(lane % (2 * span) < span, left, right))
    low_half = lane < LANES // 2
    owners = [
        jnp.where(low_half, pairs[0], lane_roll(pairs[1], LANES // 2)),
        jnp.where(low_half, lane_roll(pairs[0], LANES // 2), pairs[1]),
    ]
    all_kx = owners[0].shape[0] // 2
    slabs = all_kx // kx
    for m, values in enumerate(owners):
        done = values[:all_kx] + quarter_turn(values[all_kx:], span, -1)
        for s in range(slabs):
            store(m * slabs + s, done[s * kx : (s + 1) * kx])


def group_lines(modes_ref, row_table, span):
    block = LANES // span
    owners = modes_ref.shape[0]
    half = owners // 2
    stack = []
    for m in range(2):
        stack.append(jnp.concatenate([modes_ref[m * half + s, 0] for s in range(half)], axis=0))
    full = [jnp.concatenate([one, quarter_turn(one, span, 1)], axis=0) for one in stack]
    rolled = [[lane_roll(one, k * span) for k in range(block)] for one in full]
    lane = lanes_of(full[0].shape)
    even = lane % (2 * span) < span
    low_half = lane < LANES // 2
    sides = []
    for c in range(block):
        first = jnp.where(low_half, rolled[0][(0 - c) % block], rolled[0][(2 - c) % block])
        second = jnp.where(low_half, rolled[1][(1 - c) % block], rolled[1][(3 - c) % block])
        sides.append(jnp.where(even, first, second))
    lines = []
    for c in range(0, block, 2):
        both = three_way(row_table, jnp.concatenate([sides[c], sides[c + 1]], axis=1))
        lines += [both[:, :LANES], both[:, LANES:]]
    return lines


def middle_packed(
    span, x_ref, cot_ref, modes_ref, gain_ref, bias_ref, ahead_ref, row_ref, row_back_ref, behind_ref,
    out_ref, grad_ref, spec_ref, sums_ref, split_ref, lines_ref,
):
    block, rows, cols = cot_ref.shape
    kx = modes_ref.shape[2]
    step = pl.program_id(0)
    scale = math.sqrt(2.0 / math.pi)
    row_table = row_ref[0]

    @pl.when(step == 0)
    def _():
        sums_ref[...] = jnp.zeros_like(sums_ref)

    def ahead(c):
        here = slice(c * rows, (c + 1) * rows)
        both = jnp.concatenate([ahead_ref[0], ahead_ref[0]], axis=0)
        lines_ref[here] = jnp.dot(split_ref[here], both, preferred_element_type=jnp.float32)

    def finish(group):
        def store(owner, values):
            spec_ref[owner, pl.ds(pl.multiple_of(group * kx, kx), kx)] = values
        mix_rows(lines_ref, row_table, rows, span, kx, store)

    lane = lanes_of(sums_ref.shape)
    line = lax.broadcasted_iota(jnp.int32, sums_ref.shape, 0)

    def cell(c, lines):
        channel = step * block + c
        source = x_ref[channel]
        v = two_way(lines, behind_ref[0]) + (gain_ref[channel] * source + bias_ref[channel])
        square = v * v
        inner = v * (scale + (scale * 0.044715) * square)
        up = 0.5 + 0.5 * jnp.tanh(inner)
        out_ref[c] = v * up
        bend = v * (2.0 * scale + (6.0 * scale * 0.044715) * square)
        grad = cot_ref[c] * (up + (up * (1.0 - up)) * bend)
        grad_ref[channel] = grad
        high, low = high_low(grad)
        split_ref[c * rows : (c + 1) * rows, :cols] = high
        split_ref[c * rows : (c + 1) * rows, cols:] = low
        gate = jnp.sum(jnp.sum(grad * source, axis=0, keepdims=True), axis=1, keepdims=True)
        bias = jnp.sum(jnp.sum(grad, axis=0, keepdims=True), axis=1, keepdims=True)
        here = (lane == channel) & (line < 2)
        sums_ref[...] = jnp.where(here, jnp.where(line == 0, gate, bias), sums_ref[...])

    for c in range(block):
        ahead(c)
    lines = group_lines(modes_ref, row_back_ref[0], span)
    for c in range(block // 2):
        cell(c, lines[c])
    finish(jnp.maximum(step - 1, 0))
    for c in range(block // 2, block):
        cell(c, lines[c])

    @pl.when(step == pl.num_programs(0) - 1)
    def _():
        for c in range(block):
            ahead(c)
        finish(step)


def last_packed(
    span, kx, grad_ref, modes_ref, gain_ref, row_back_ref, behind_ref, grads_ref, spec_ref, limit_ref, out_ref, wgrad_ref
):
    block = out_ref.shape[0]
    step = pl.program_id(0)
    lines = group_lines(modes_ref, row_back_ref[0], span)
    count, freqs, outs = wgrad_ref.shape[0], wgrad_ref.shape[1], wgrad_ref.shape[4]
    wide = freqs * kx
    first = lax.axis_index("chan") * (count * pl.num_programs(0)) + step * count
    g_real, g_imag = both_parts(grads_ref, slice(None))
    for i in range(count):
        keep = jnp.broadcast_to(limit_ref[:, :1], (outs, wide)) > first + i
        s_real, s_imag = both_parts(spec_ref, pl.ds(step * count + i, 1))
        real = jnp.where(keep, s_real * g_real + s_imag * g_imag, 0.0)
        imag = jnp.where(keep, s_real * g_imag - s_imag * g_real, 0.0)
        wgrad_ref[i, :, 0] = real.T.reshape(freqs, kx, outs)
        wgrad_ref[i, :, 1] = imag.T.reshape(freqs, kx, outs)
    for c in range(block):
        out_ref[c] = two_way(lines[c], behind_ref[0]) + gain_ref[step * block + c] * grad_ref[step * block + c]


def swap_groups(values, kx):
    lane = lanes_of(values.shape) // kx
    line = lax.broadcasted_iota(jnp.int32, values.shape, 1)
    count = values.shape[1]
    hop = 1
    while hop < count:
        up = lane_roll(pltpu.roll(values, count - hop, 1), hop * kx)
        down = lane_roll(pltpu.roll(values, hop, 1), -hop * kx)
        lane_bit, line_bit = lane // hop % 2, line // hop % 2
        values = jnp.where(lane_bit == line_bit, values, jnp.where(lane_bit == 1, up, down))
        hop *= 2
    return values


def to_lanes(packed, out_ref, kx):
    lines = swap_groups(packed.T.reshape(-1, 8, LANES), kx)
    wide = out_ref.shape[0]
    block = lines.shape[0] // wide
    for c in range(block):
        for j in range(wide):
            out_ref[j, pl.ds(c, 8, stride=block)] = lines[c * wide + j]


def to_rows(wide_ref, block, kx):
    wide = wide_ref.shape[0]
    pieces = []
    for c in range(block):
        for j in range(wide):
            pieces.append(wide_ref[j, pl.ds(c, 8, stride=block)][None])
    return swap_groups(jnp.concatenate(pieces, axis=0), kx).reshape(-1, LANES).T


def both_parts(ref, rows):
    half = ref.shape[0] // 2
    parts = [jnp.concatenate([ref[p * half + j, rows] for j in range(half)], axis=1) for p in range(2)]
    return parts[0], parts[1]


def put_part(ref, rows, part, values):
    half = ref.shape[0] // 2
    for j in range(half):
        ref[part * half + j, rows] = values[:, j * LANES : (j + 1) * LANES]


def other(axis, step, size):
    return lax.rem(lax.axis_index(axis) + step, size)


def send(source, target, sends, recvs, axis, peer):
    copy = pltpu.make_async_remote_copy(
        src_ref=source, dst_ref=target, send_sem=sends, recv_sem=recvs,
        device_id={axis: peer}, device_id_type=pl.DeviceIdType.MESH,
    )
    copy.start()
    return copy


def greet(slabs):
    barrier = pltpu.get_barrier_semaphore()
    targets = [("mode", 1, 2), ("chan", 1, 2)] + [("slab", step, slabs) for step in range(1, slabs)]
    for axis, step, size in targets:
        pl.semaphore_signal(
            barrier, inc=1, device_id={axis: other(axis, step, size)}, device_id_type=pl.DeviceIdType.MESH
        )
    pl.semaphore_wait(barrier, len(targets))


def scatter_sum(part_ref, half_ref, give_ref, take_ref, mode_sems, slab_sems, slabs, between):
    me_mode, me_slab = lax.axis_index("mode"), lax.axis_index("slab")
    peer = other("mode", 1, 2)
    order = [slabs // 2] + [step for step in range(1, slabs) if step != slabs // 2] + [0]
    copies = []
    for step in order:
        slab = other("slab", step, slabs)
        copies.append(send(
            part_ref.at[peer * slabs + slab], half_ref.at[step], mode_sems.at[0, step], mode_sems.at[1, step], "mode", peer
        ))
    waits = list(copies)
    out = []
    for step, copy in zip(order, copies):
        copy.wait_recv()
        slab = other("slab", step, slabs)
        total = part_ref[me_mode * slabs + slab] + half_ref[step]
        if step == 0:
            mine = total
        else:
            give_ref[step] = total
            out.append(send(
                give_ref.at[step], take_ref.at[step], slab_sems.at[0, step], slab_sems.at[1, step], "slab", slab
            ))
    between()
    for copy in out:
        copy.wait_recv()
    for step in range(1, slabs):
        mine = mine + take_ref[step]
    return mine, [copy.wait_send for copy in copies + out]


def gather_start(own_ref, out_ref, mode_sems, slab_sems, slabs):
    me = lax.axis_index("mode") * slabs + lax.axis_index("slab")
    copies = []
    for step in [slabs // 2] + [step for step in range(1, slabs) if step != slabs // 2]:
        copies.append(send(
            own_ref, out_ref.at[me], slab_sems.at[0, step], slab_sems.at[1, step], "slab", other("slab", step, slabs)
        ))
    near = send(own_ref, out_ref.at[me], mode_sems.at[0, 0], mode_sems.at[1, 0], "mode", other("mode", 1, 2))
    out_ref[me] = own_ref[...]
    return copies, near


def gather_finish(state, out_ref, mode_sems, slabs, between):
    copies, near = state
    relays = []
    order = [slabs // 2] + [step for step in range(1, slabs) if step != slabs // 2]
    for k in list(range(1, slabs - 1)) + [0]:
        between(k)
        copies[k].wait_recv()
        step = order[k]
        source = lax.axis_index("mode") * slabs + other("slab", slabs - step, slabs)
        relays.append(send(
            out_ref.at[source], out_ref.at[source], mode_sems.at[0, step], mode_sems.at[1, step], "mode", other("mode", 1, 2)
        ))
    near.wait()
    for copy in relays:
        copy.wait()
    for copy in copies:
        copy.wait_send()


def forward_kernel(
    span, slabs, kx, x_ref, ahead_ref, row_ref, w_ref, limit_ref, weight_ref, out_ref, turned_ref, spec_ref, x_buf,
    part_ref, half_ref, give_ref, take_ref, w_buf, t_buf, sum_ref, peer_ref, own_ref, lines_ref, ahead_buf, row_buf,
    mode_a, slab_a, mode_b, slab_b, chan_sems, x_sems, w_sems, table_sems, t_sems,
):
    ins, freqs, outs = w_ref.shape[0], w_ref.shape[1], w_ref.shape[4]
    rows, cols = x_ref.shape[1:]
    block = LANES // span
    groups = ins // block
    mine_outs = outs // 2
    wide = freqs * kx
    me_mode, me_slab = lax.axis_index("mode"), lax.axis_index("slab")
    peer_mode = other("mode", 1, 2)
    first = lax.axis_index("chan") * ins
    tables = [
        pltpu.make_async_copy(ahead_ref.at[me_mode], ahead_buf, table_sems.at[0]),
        pltpu.make_async_copy(row_ref.at[me_slab], row_buf, table_sems.at[1]),
    ]
    tables[0].start()

    def x_copy(k):
        here = pl.ds(k * (block // 2), block // 2)
        return pltpu.make_async_copy(x_ref.at[here], x_buf.at[here], x_sems.at[k])

    def w_copy(g):
        here = pl.ds(g * block, block)
        return pltpu.make_async_copy(w_ref.at[here], w_buf.at[here], w_sems.at[g])

    for g in range(groups):
        x_copy(2 * g).start()
        x_copy(2 * g + 1).start()
        if g == 0:
            tables[1].start()
        if g > 0:
            w_copy(g - 1).start()
    w_copy(groups - 1).start()
    greet(slabs)

    def t_copy(g):
        here = pl.ds(g * block, block)
        return pltpu.make_async_copy(t_buf.at[here], turned_ref.at[here], t_sems.at[g])

    def place(g):
        return pl.ds(pl.multiple_of(g * kx, kx), kx)

    def mode_copy(g):
        return pltpu.make_async_remote_copy(
            src_ref=part_ref.at[pl.ds(peer_mode * slabs, slabs), place(g)], dst_ref=half_ref.at[:, place(g)],
            send_sem=mode_a.at[0, g], recv_sem=mode_a.at[1, g],
            device_id={"mode": peer_mode}, device_id_type=pl.DeviceIdType.MESH,
        )

    def slab_copy(step, g):
        return pltpu.make_async_remote_copy(
            src_ref=give_ref.at[step, place(g)], dst_ref=take_ref.at[step, place(g)],
            send_sem=slab_a.at[0, step, g], recv_sem=slab_a.at[1, step, g],
            device_id={"slab": other("slab", step, slabs)}, device_id_type=pl.DeviceIdType.MESH,
        )

    def ahead(g):
        x_copy(2 * g).wait()
        x_copy(2 * g + 1).wait()
        values = x_buf[pl.ds(g * block, block)].reshape(block * rows, cols)
        lines_ref[...] = two_way(values, ahead_buf[...])

    def finish(g):
        def store(owner, values):
            part_ref[owner, place(g)] = values
        mix_rows(lines_ref, row_buf[...], rows, span, kx, store)

    def flip(g):
        for k in range(block):
            i = g * block + k
            keep = jnp.broadcast_to(limit_ref[:, :1], (outs, wide)) > first + i
            for p in range(2):
                turned = w_buf[i, :, p].reshape(wide, outs).T
                t_buf[i, :, p * wide : (p + 1) * wide] = jnp.where(keep, turned, 0.0)

    def pass_on(g):
        mode_copy(g).wait_recv()
        for step in [slabs // 2] + [step for step in range(1, slabs) if step != slabs // 2]:
            slab = other("slab", step, slabs)
            give_ref[step, place(g)] = part_ref[me_mode * slabs + slab, place(g)] + half_ref[slab, place(g)]
            slab_copy(step, g).start()

    for table in tables:
        table.wait()
    ahead(0)

    def body(g, carry):
        w_copy(g - 1).wait()
        finish(g - 1)
        flip(g - 1)
        ahead(g)
        t_copy(g - 1).start()
        mode_copy(g - 1).start()

        @pl.when(g > 1)
        def _():
            pass_on(g - 2)
        return carry

    lax.fori_loop(1, groups, body, 0)
    w_copy(groups - 1).wait()
    finish(groups - 1)
    mode_copy(groups - 1).start()
    pass_on(groups - 2)
    flip(groups - 1)
    t_copy(groups - 1).start()
    pass_on(groups - 1)
    mine = part_ref[me_mode * slabs + me_slab] + half_ref[me_slab]

    def landed(g, carry):
        for step in range(1, slabs):
            slab_copy(step, g).wait_recv()
        return carry
    lax.fori_loop(0, groups, landed, 0)
    for step in range(1, slabs):
        mine = mine + take_ref[step]
    to_lanes(mine, spec_ref, kx)

    def contract(i, carry):
        real, imag = carry
        w_real, w_imag = t_buf[i, :, :wide], t_buf[i, :, wide:]
        s_real, s_imag = both_parts(spec_ref, pl.ds(i, 1))
        return real + (s_real * w_real - s_imag * w_imag), imag + (s_real * w_imag + s_imag * w_real)

    zero = jnp.zeros((outs, wide), jnp.float32)
    real, imag = lax.fori_loop(0, ins, contract, (zero, zero))
    put_part(sum_ref, slice(None), 0, real)
    put_part(sum_ref, slice(None), 1, imag)
    theirs = other("chan", 1, 2) * mine_outs
    swap = send(
        sum_ref.at[:, pl.ds(theirs, mine_outs)], peer_ref, chan_sems.at[0], chan_sems.at[1], "chan", other("chan", 1, 2)
    )
    swap.wait_recv()
    for j in range(peer_ref.shape[0]):
        peer_ref[j] = (sum_ref[j, pl.ds(first, mine_outs)] + peer_ref[j]) * weight_ref[j % weight_ref.shape[0]]
    own_ref[...] = to_rows(peer_ref, mine_outs // 8, kx)
    state = gather_start(own_ref, out_ref, mode_b, slab_b, slabs)
    gather_finish(state, out_ref, mode_b, slabs, lambda k: None)
    swap.wait_send()

    def settle(g, carry):
        t_copy(g).wait()
        mode_copy(g).wait_send()
        for step in range(1, slabs):
            slab_copy(step, g).wait_send()
        return carry
    lax.fori_loop(0, groups, settle, 0)


def backward_kernel(
    slabs, kx, part_ref, sums_ref, turned_ref, weight_ref, out_ref, grad_ref, total_ref,
    half_ref, give_ref, take_ref, t_buf, back_ref, own_ref, near_ref, far_ref, pass_ref,
    mode_a, slab_a, mode_b, slab_b, chan_sems, sum_mode, sum_slab, t_sem,
):
    ins, outs, wide = t_buf.shape[0], t_buf.shape[1], t_buf.shape[2] // 2
    mine_outs = outs // 2
    load = pltpu.make_async_copy(turned_ref, t_buf, t_sem)
    load.start()
    greet(slabs)
    first = lax.axis_index("chan") * ins
    near = send(sums_ref, near_ref, sum_mode.at[0], sum_mode.at[1], "mode", other("mode", 1, 2))

    far = []
    def total_up():
        near.wait_recv()
        pass_ref[...] = sums_ref[...] + near_ref[...]
        for step in range(1, slabs):
            far.append(send(
                pass_ref, far_ref.at[step], sum_slab.at[0, step], sum_slab.at[1, step], "slab", other("slab", step, slabs)
            ))

    mine, sent = scatter_sum(part_ref, half_ref, give_ref, take_ref, mode_a, slab_a, slabs, total_up)
    to_lanes(mine, back_ref, kx)
    here = pl.ds(first, mine_outs)
    for j in range(back_ref.shape[0]):
        grad_ref[j, here] = back_ref[j] * weight_ref[j % weight_ref.shape[0]]
    swap = send(
        grad_ref.at[:, here], grad_ref.at[:, here], chan_sems.at[0], chan_sems.at[1], "chan", other("chan", 1, 2)
    )
    load.wait()
    swap.wait_recv()

    def pull(i, carry):
        w_real, w_imag = t_buf[i, :, :wide], t_buf[i, :, wide:]
        g_real, g_imag = both_parts(grad_ref, slice(None))
        put_part(back_ref, pl.ds(i, 1), 0, jnp.sum(g_real * w_real + g_imag * w_imag, axis=0, keepdims=True))
        put_part(back_ref, pl.ds(i, 1), 1, jnp.sum(g_imag * w_real - g_real * w_imag, axis=0, keepdims=True))
        return carry
    lax.fori_loop(0, ins, pull, 0)
    own_ref[...] = to_rows(back_ref, ins // 8, kx)
    state = gather_start(own_ref, out_ref, mode_b, slab_b, slabs)
    gather_finish(state, out_ref, mode_b, slabs, lambda k: None)
    total = pass_ref[...]
    for step, copy in zip(range(1, slabs), far):
        copy.wait()
        total = total + far_ref[step]
    total_ref[...] = total
    near.wait_send()
    swap.wait_send()
    for wait in sent:
        wait()


def fits(shapes, mesh_sizes):
    channels, rows, cols = shapes[0]
    outs, freqs, kx = shapes[2][1], shapes[2][2], shapes[2][4]
    slabs, modes, chans = mesh_sizes
    return (
        modes == 2 and chans == 2 and slabs > 2 and slabs % 2 == 0
        and 8 * kx == LANES and 8 * freqs == LANES and 2 * freqs * channels == 8 * LANES
        and outs == chans * channels
        and rows % LANES == 0 and cols % LANES == 0
    )


def local(source_field, cotangent, spectral_weight, skip_gain, channel_bias, mode_limit, width_limit):
    slabs, modes, chans = (lax.axis_size(axis) for axis in ("slab", "mode", "chan"))
    args = (source_field, cotangent, spectral_weight, skip_gain, channel_bias, mode_limit, width_limit)
    if not fits([one.shape for one in args], (slabs, modes, chans)):
        return local_plain(*args)
    channels, rows, cols = source_field.shape
    outs, freqs, kx = spectral_weight.shape[1], spectral_weight.shape[2], spectral_weight.shape[4]
    span = 2 * freqs
    block = LANES // span
    groups = channels // block
    owners = slabs * modes
    all_kx, all_rows, all_cols = kx * slabs, rows * slabs, cols * modes
    wide = freqs * kx
    ahead, row_ahead, row_behind, behind = (
        jnp.asarray(t) for t in packed_tables(all_rows, all_cols, slabs, modes, freqs, all_kx)
    )
    slab_index, mode_index, chan_index = (lax.axis_index(axis) for axis in ("slab", "mode", "chan"))

    def pick(table, axis):
        return pl.BlockSpec((1,) + table.shape[1:], lambda g: (lax.axis_index(axis), 0, 0))

    cells = pl.BlockSpec((block, rows, cols), lambda g: (g, 0, 0))
    freq_cells = pl.BlockSpec((owners, 1, kx, LANES), lambda g: (0, g, 0, 0))
    scalars = pl.BlockSpec(memory_space=pltpu.SMEM)
    field = jax.ShapeDtypeStruct(source_field.shape, jnp.float32)
    freq_field = jax.ShapeDtypeStruct((owners, groups, kx, LANES), jnp.float32)
    room = lambda size: pltpu.CompilerParams(dimension_semantics=("arbitrary",), vmem_limit_bytes=size * MIB)
    f32 = jnp.float32

    weight = spectral_weight.transpose(0, 2, 3, 4, 1)
    col_freq = mode_index * freqs + jnp.arange(freqs, dtype=jnp.int32)
    row_freq = slab_index * kx + jnp.arange(kx, dtype=jnp.int32)
    limit_rows = lax.dynamic_slice_in_dim(mode_limit, chan_index * channels, channels, 0)
    flat_cols, flat_rows = jnp.repeat(col_freq, kx)[None, :], jnp.tile(row_freq, freqs)[None, :]
    kept = (flat_cols < limit_rows[:, 0:1]) & (
        (flat_rows < limit_rows[:, 1:2]) | (all_kx - flat_rows < limit_rows[:, 1:2])
    )
    scales = jnp.where(flat_cols == 0, 1.0, 2.0).astype(jnp.float32) / (all_rows * all_cols)
    weights = jnp.where(kept, scales, 0.0).reshape(channels, -1, LANES).transpose(1, 0, 2)
    limit = jnp.broadcast_to(width_limit[:, None], (outs, LANES))

    dma, vmem = pltpu.SemaphoreType.DMA, pltpu.VMEM
    in_vmem, anywhere = pl.BlockSpec(memory_space=pltpu.VMEM), pl.BlockSpec(memory_space=pl.ANY)
    piece = (groups * kx, LANES)
    common = [vmem((slabs,) + piece, f32), vmem((slabs,) + piece, f32), vmem((slabs,) + piece, f32)]
    pair = [dma((2, slabs))] * 4
    comm = lambda ident, room: pltpu.CompilerParams(
        collective_id=ident, has_side_effects=True, vmem_limit_bytes=room * MIB
    )
    flat = lambda lines: (2 * wide // LANES, lines, LANES)

    in_hbm = lambda array: pltpu.with_memory_space_constraint(array, pltpu.HBM)
    held = lambda array: pltpu.with_memory_space_constraint(array, pltpu.VMEM)
    modes_shape = (owners,) + piece
    out_modes, turned, spec, source_held = pl.pallas_call(
        functools.partial(forward_kernel, span, slabs, kx),
        in_specs=[anywhere, anywhere, anywhere, anywhere, in_vmem, in_vmem],
        out_specs=[in_vmem, anywhere, in_vmem, in_vmem],
        out_shape=[
            jax.ShapeDtypeStruct(modes_shape, f32), pltpu.HBM((channels, outs, 2 * wide), f32),
            jax.ShapeDtypeStruct(flat(channels), f32), pltpu.VMEM(field.shape, f32),
        ],
        scratch_shapes=[vmem(modes_shape, f32)] + common + [
            vmem(weight.shape, f32), vmem((channels, outs, 2 * wide), f32), vmem(flat(outs), f32), vmem(flat(outs // 2), f32), vmem(piece, f32),
            vmem((block * rows, LANES), f32), vmem(ahead.shape[1:], jnp.bfloat16), vmem(row_ahead.shape[1:], jnp.bfloat16),
            dma((2, groups)), dma((2, slabs, groups)), dma((2, slabs)), dma((2, slabs)), dma((2,)),
            dma((2 * groups,)), dma((groups,)), dma((2,)), dma((groups,)),
        ],
        compiler_params=comm(20, FORWARD),
        name="forward_modes",
    )(in_hbm(source_field), in_hbm(ahead), in_hbm(row_ahead), in_hbm(weight), limit, weights)

    output, grad_sum, grad_partial, sums = pl.pallas_call(
        functools.partial(middle_packed, span),
        grid=(groups,),
        in_specs=[
            in_vmem, cells, freq_cells, scalars, scalars, pick(ahead, "mode"), pick(row_ahead, "slab"),
            pick(row_behind, "slab"), pick(behind, "mode"),
        ],
        out_specs=[cells, in_vmem, in_vmem, in_vmem],
        out_shape=[field, pltpu.VMEM(field.shape, f32), jax.ShapeDtypeStruct(modes_shape, f32), jax.ShapeDtypeStruct((8, LANES), f32)],
        scratch_shapes=[vmem((block * rows, 2 * cols), jnp.bfloat16), vmem((block * rows, LANES), f32)],
        input_output_aliases={0: 1},
        compiler_params=room(MIDDLE),
        name="middle",
    )(
        held(source_held), cotangent, out_modes.reshape(freq_field.shape), skip_gain, channel_bias,
        ahead, row_ahead, row_behind, behind,
    )

    back_modes, all_grads, totals = pl.pallas_call(
        functools.partial(backward_kernel, slabs, kx),
        in_specs=[in_vmem, in_vmem, anywhere, in_vmem],
        out_specs=[in_vmem] * 3,
        out_shape=[jax.ShapeDtypeStruct(modes_shape, f32), jax.ShapeDtypeStruct(flat(outs), f32), jax.ShapeDtypeStruct((8, LANES), f32)],
        scratch_shapes=common + [
            vmem((channels, outs, 2 * wide), f32), vmem(flat(channels), f32), vmem(piece, f32), vmem((8, LANES), f32),
            vmem((slabs, 8, LANES), f32), vmem((8, LANES), f32),
        ] + pair + [dma((2,)), dma((2,)), dma((2, slabs)), dma],
        compiler_params=comm(21, 20),
        name="backward_modes",
    )(grad_partial, sums, in_hbm(turned), weights)

    count = channels // groups
    whole = lambda array: pl.BlockSpec(array.shape, lambda g: (0,) * array.ndim)
    field_grad, weight_grad = pl.pallas_call(
        functools.partial(last_packed, span, kx),
        grid=(groups,),
        in_specs=[
            in_vmem, freq_cells, scalars, pick(row_behind, "slab"), pick(behind, "mode"),
            whole(all_grads), whole(spec), whole(limit),
        ],
        out_specs=[cells, pl.BlockSpec((count,) + weight.shape[1:], lambda g: (g, 0, 0, 0, 0))],
        out_shape=[field, jax.ShapeDtypeStruct(weight.shape, f32)],
        compiler_params=room(LAST),
        name="last",
    )(
        pltpu.with_memory_space_constraint(grad_sum, pltpu.VMEM), back_modes.reshape(freq_field.shape), skip_gain,
        row_behind, behind, all_grads, spec, limit,
    )
    spectral_grad = weight_grad.transpose(0, 4, 1, 2, 3)
    return (output, field_grad, spectral_grad, totals[0, :channels], totals[1, :channels])


def solution(mesh):
    in_specs = (
        P(("member", "chan"), "slab", "mode"),
        P(("member", "chan"), "slab", "mode"),
        P(("member", "chan"), None, "mode", None, "slab"),
        P(("member", "chan")),
        P(("member", "chan")),
        P("member", None),
        P("member"),
    )
    out_specs = (
        P(("member", "chan"), "slab", "mode"),
        P(("member", "chan"), "slab", "mode"),
        P(("member", "chan"), None, "mode", None, "slab"),
        P(("member", "chan")),
        P(("member", "chan")),
    )
    return jax.shard_map(local, mesh=mesh, in_specs=in_specs, out_specs=out_specs, check_vma=False)
```

```python
import functools
import math

import jax
import jax.numpy as jnp
import ml_dtypes
import numpy as np
from jax import lax
from jax.experimental import pallas as pl
from jax.experimental.pallas import tpu as pltpu
from jax.sharding import PartitionSpec as P

LANES = 128
BIG = 60 * 1024 * 1024
MIB = 1024 * 1024
FORWARD, MIDDLE, LAST, BACKWARD = 40, 40, 40, 20


def split_table(table):
    high = lax.reduce_precision(table, 8, 7)
    return high.astype(jnp.bfloat16), (table - high).astype(jnp.bfloat16)


def split_block(values):
    high = values.astype(jnp.bfloat16)
    return high, (values - high.astype(jnp.float32)).astype(jnp.bfloat16)


def dot_pair(left, right):
    left_high, left_low = left
    right_high, right_low = right
    mul = functools.partial(jnp.dot, preferred_element_type=jnp.float32)
    return mul(left_high, right_high) + mul(left_low, right_high) + mul(left_high, right_low)


def tables(extent, waves, first_cell, cell_count):
    cell_index = first_cell + jnp.arange(cell_count, dtype=jnp.int32)
    products = (cell_index[:, None] * waves[None, :] % extent).astype(jnp.float32)
    angles = products * (2.0 * math.pi / extent)
    return jnp.cos(angles), jnp.sin(angles)


def store_spectrum(values, col_pair, row_pair, out_ref):
    block, rows, cols = values.shape
    lines = dot_pair(split_block(values.reshape(block * rows, cols)), col_pair)
    all_kx = row_pair[0].shape[0] // 2
    kx, lanes = out_ref.shape[2:]
    span = lanes // block
    mode_count = lines.shape[1] // span
    slabs = out_ref.shape[0] // mode_count
    done = []
    for c in range(block):
        mixed = dot_pair(row_pair, split_block(lines[c * rows : (c + 1) * rows]))
        done.append(mixed[:all_kx] - turn(mixed[all_kx:], span))
    for m in range(mode_count):
        packed = jnp.concatenate([one[:, m * span : (m + 1) * span] for one in done], axis=1)
        for s in range(slabs):
            out_ref[m * slabs + s, 0] = packed[s * kx : (s + 1) * kx]


def turn(values, span):
    half = span // 2
    pieces = []
    for first in range(0, values.shape[1], span):
        pieces.append(-values[:, first + half : first + span])
        pieces.append(values[:, first : first + half])
    return jnp.concatenate(pieces, axis=1)


def all_modes(modes_ref, mode_count, c, block):
    span = modes_ref.shape[3] // block
    slabs = modes_ref.shape[0] // mode_count
    columns = []
    for m in range(mode_count):
        stack = [modes_ref[m * slabs + s, 0] for s in range(slabs)]
        columns.append(jnp.concatenate(stack, axis=0)[:, c * span : (c + 1) * span])
    return jnp.concatenate(columns, axis=1), span


def synth(modes_and_span, row_pair, col_pair):
    modes, span = modes_and_span
    stacked = jnp.concatenate([modes, turn(modes, span)], axis=0)
    lines = dot_pair(row_pair, split_block(stacked))
    return dot_pair(split_block(lines), col_pair)


def spectrum_kernel(x_ref, ch_ref, cl_ref, rh_ref, rl_ref, out_ref):
    store_spectrum(x_ref[...], (ch_ref[...], cl_ref[...]), (rh_ref[...], rl_ref[...]), out_ref)


def middle_kernel(
    mode_count, x_ref, cot_ref, modes_ref, gain_ref, bias_ref, ch_ref, cl_ref, rh_ref, rl_ref,
    cth_ref, ctl_ref, ih_ref, il_ref, out_ref, grad_ref, spec_ref, sums_ref,
):
    block = x_ref.shape[0]
    row_back = (ih_ref[...], il_ref[...])
    col_back = (cth_ref[...], ctl_ref[...])
    scale = math.sqrt(2.0 / math.pi)
    for c in range(block):
        source = x_ref[c]
        gain = gain_ref[c]
        v = synth(all_modes(modes_ref, mode_count, c, block), row_back, col_back) + gain[:, :1] * source + bias_ref[c][:, :1]
        square = v * v
        t = jnp.tanh(scale * v * (1.0 + 0.044715 * square))
        half_up = 0.5 * (1.0 + t)
        out_ref[c] = v * half_up
        slope = half_up + 0.5 * v * (1.0 - t * t) * (scale * (1.0 + 3.0 * 0.044715 * square))
        grad = cot_ref[c] * slope
        grad_ref[c] = grad
        gate = jnp.sum(jnp.sum(grad * source, axis=0, keepdims=True), axis=1, keepdims=True)
        bias = jnp.sum(jnp.sum(grad, axis=0, keepdims=True), axis=1, keepdims=True)
        lane = lax.broadcasted_iota(jnp.int32, (1, LANES), 1)
        sums_ref[c] = jnp.where(lane == 0, gate, bias)
    store_spectrum(
        grad_ref[...], (ch_ref[...], cl_ref[...]), (rh_ref[...], rl_ref[...]), spec_ref
    )


def last_kernel(mode_count, grad_ref, modes_ref, gain_ref, cth_ref, ctl_ref, ih_ref, il_ref, out_ref):
    block = grad_ref.shape[0]
    for c in range(block):
        modes = all_modes(modes_ref, mode_count, c, block)
        branch = synth(modes, (ih_ref[...], il_ref[...]), (cth_ref[...], ctl_ref[...]))
        out_ref[c] = branch + gain_ref[c][:, :1] * grad_ref[c]


def contract_kernel(w_ref, spec_ref, limit_ref, out_ref):
    block, freqs, _, kx, outs = w_ref.shape
    first = lax.axis_index("chan") * (block * pl.num_programs(0)) + pl.program_id(0) * block

    @pl.when(pl.program_id(0) == 0)
    def _():
        out_ref[...] = jnp.zeros_like(out_ref)

    limit = limit_ref[...]
    for y in range(freqs):
        real = out_ref[y, 0]
        imag = out_ref[y, 1]
        for i in range(block):
            keep = first + i < limit
            spec = spec_ref[0]
            at = 2 * freqs * i + y
            s_real = jnp.where(keep, spec[:, at : at + 1], 0.0)
            s_imag = jnp.where(keep, spec[:, freqs + at : freqs + at + 1], 0.0)
            w_real = w_ref[i, y, 0]
            w_imag = w_ref[i, y, 1]
            real = real + (s_real * w_real - s_imag * w_imag)
            imag = imag + (s_real * w_imag + s_imag * w_real)
        out_ref[y, 0] = real
        out_ref[y, 1] = imag


def back_kernel(w_ref, spec_ref, grads_ref, limit_ref, wgrad_ref, out_ref):
    block, freqs, _, kx, outs = w_ref.shape
    first = lax.axis_index("chan") * (block * pl.num_programs(0)) + pl.program_id(0) * block
    limit = limit_ref[...]
    lane = lax.broadcasted_iota(jnp.int32, out_ref.shape[1:], 1)
    spec = spec_ref[0]
    back = jnp.zeros(out_ref.shape[1:], jnp.float32)
    for i in range(block):
        keep = first + i < limit
        for y in range(freqs):
            at = 2 * freqs * i + y
            g_real = jnp.where(keep, grads_ref[y, 0], 0.0)
            g_imag = jnp.where(keep, grads_ref[y, 1], 0.0)
            s_real = spec[:, at : at + 1]
            s_imag = spec[:, freqs + at : freqs + at + 1]
            wgrad_ref[i, y, 0] = s_real * g_real + s_imag * g_imag
            wgrad_ref[i, y, 1] = s_real * g_imag - s_imag * g_real
            w_real = w_ref[i, y, 0]
            w_imag = w_ref[i, y, 1]
            b_real = jnp.sum(g_real * w_real + g_imag * w_imag, axis=1, keepdims=True)
            b_imag = jnp.sum(g_imag * w_real - g_real * w_imag, axis=1, keepdims=True)
            back = jnp.where(lane == at, b_real, back)
            back = jnp.where(lane == freqs + at, b_imag, back)
    out_ref[0] = back


def exchange_kernel(axes, sizes, gather, x_ref, out_ref, send_sem, recv_sem, own_sem):
    total = math.prod(sizes)
    me = lax.axis_index(axes[0])
    for axis, size in zip(axes[1:], sizes[1:]):
        me = me * size + lax.axis_index(axis)

    def place(index):
        coords = {}
        for axis, size in reversed(list(zip(axes, sizes))):
            coords[axis] = lax.rem(index, size)
            index = lax.div(index, size)
        return coords

    barrier = pltpu.get_barrier_semaphore()
    for step in range(1, total):
        pl.semaphore_signal(
            barrier, inc=1, device_id=place(lax.rem(me + step, total)),
            device_id_type=pl.DeviceIdType.MESH,
        )
    pl.semaphore_wait(barrier, total - 1)
    copies = []
    for step in range(1, total):
        peer = lax.rem(me + step, total)
        copy = pltpu.make_async_remote_copy(
            src_ref=x_ref if gather else x_ref.at[peer],
            dst_ref=out_ref.at[me],
            send_sem=send_sem.at[step],
            recv_sem=recv_sem.at[step],
            device_id=place(peer),
            device_id_type=pl.DeviceIdType.MESH,
        )
        copy.start()
        copies.append(copy)
    own = pltpu.make_async_copy(x_ref if gather else x_ref.at[me], out_ref.at[me], own_sem)
    own.start()
    own.wait()
    for copy in copies:
        copy.wait()


def exchange(values, axes, gather, ident):
    sizes = tuple(lax.axis_size(axis) for axis in axes)
    total = math.prod(sizes)
    piece = values.shape if gather else values.shape[1:]
    flat = values.reshape((-1, LANES) if gather else (total, -1, LANES))
    out = pl.pallas_call(
        functools.partial(exchange_kernel, axes, sizes, gather),
        out_shape=jax.ShapeDtypeStruct((total,) + flat.shape[-2:], jnp.float32),
        in_specs=[pl.BlockSpec(memory_space=pltpu.VMEM)],
        out_specs=pl.BlockSpec(memory_space=pltpu.VMEM),
        scratch_shapes=[
            pltpu.SemaphoreType.DMA((total,)),
            pltpu.SemaphoreType.DMA((total,)),
            pltpu.SemaphoreType.DMA,
        ],
        compiler_params=pltpu.CompilerParams(collective_id=ident, has_side_effects=True),
        name="exchange" + str(ident),
    )(flat)
    return out.reshape((total,) + piece)


def mode_weights(limit_rows, col_freq, row_freq, kx_count, cells_total):
    keep_cols = col_freq[None, :] < limit_rows[:, 0:1]
    keep_rows = (row_freq[None, :] < limit_rows[:, 1:2]) | (
        (kx_count - row_freq)[None, :] < limit_rows[:, 1:2]
    )
    scales = jnp.where(col_freq == 0, 1.0, 2.0).astype(jnp.float32) / cells_total
    joined = keep_rows[:, :, None] & keep_cols[:, None, :]
    return (joined.astype(jnp.float32) * scales[None, None, :])[:, :, None, :]


def local_plain(
    source_field, cotangent, spectral_weight, skip_gain, channel_bias, mode_limit, width_limit
):
    channels, row_count, col_count = source_field.shape
    slabs = lax.axis_size("slab")
    modes = lax.axis_size("mode")
    chans = lax.axis_size("chan")
    slab_index = lax.axis_index("slab")
    mode_index = lax.axis_index("mode")
    chan_index = lax.axis_index("chan")
    outs = spectral_weight.shape[1]
    freqs = spectral_weight.shape[2]
    kx = spectral_weight.shape[4]
    all_freqs = freqs * modes
    all_kx = kx * slabs
    all_rows = row_count * slabs
    all_cols = col_count * modes

    col_waves = jnp.arange(all_freqs, dtype=jnp.int32)
    row_waves = jnp.arange(all_kx, dtype=jnp.int32)
    row_waves = row_waves + jnp.where(2 * row_waves >= all_kx, all_rows - all_kx, 0)
    col_cos, col_sin = tables(all_cols, col_waves, mode_index * col_count, col_count)
    row_cos, row_sin = tables(all_rows, row_waves, slab_index * row_count, row_count)
    col_tab = jnp.stack(
        [col_cos.reshape(-1, modes, freqs), -col_sin.reshape(-1, modes, freqs)], axis=2
    ).reshape(col_count, 2 * all_freqs)
    row_tab = jnp.concatenate([row_cos, row_sin], axis=1)
    col_pair = split_table(col_tab)
    col_back = tuple(part.T for part in col_pair)
    row_back = split_table(row_tab)
    row_pair = tuple(part.T for part in row_back)

    block = LANES // (2 * freqs)
    groups = channels // block
    owners = slabs * modes
    cells = pl.BlockSpec((block, row_count, col_count), lambda c: (c, 0, 0))
    freq_cells = pl.BlockSpec((owners, 1, kx, LANES), lambda c: (0, c, 0, 0))
    per_channel = pl.BlockSpec((block, 1, LANES), lambda c: (c, 0, 0))
    field = jax.ShapeDtypeStruct(source_field.shape, jnp.float32)
    freq_field = jax.ShapeDtypeStruct((owners, groups, kx, LANES), jnp.float32)
    params = pltpu.CompilerParams(
        dimension_semantics=("arbitrary",), vmem_limit_bytes=BIG
    )

    def whole(array):
        return pl.BlockSpec(array.shape, lambda c: (0,) * array.ndim)

    grid = (channels // block,)
    wide = lambda values: jnp.broadcast_to(values[:, None, None], (channels, 1, LANES))
    gain = wide(skip_gain)
    forward = col_pair + row_pair
    back = col_back + row_back

    def spread(partial, ident):
        half = exchange(partial.reshape(modes, -1, LANES), ("mode",), False, ident)
        half = jnp.sum(half, axis=0).reshape(slabs, -1, LANES)
        return jnp.sum(exchange(half, ("slab",), False, ident + 1), axis=0).reshape(
            groups, kx, LANES
        )

    def joined(piece, ident):
        half = exchange(piece, ("slab",), True, ident)
        return exchange(half, ("mode",), True, ident + 1).reshape((owners,) + piece.shape)

    spectra = spread(
        pl.pallas_call(
            spectrum_kernel,
            grid=grid,
            in_specs=[cells] + [whole(t) for t in forward],
            out_specs=freq_cells,
            out_shape=freq_field,
            compiler_params=params,
            name="spectrum",
        )(source_field, *forward),
        0,
    )

    weight = spectral_weight.transpose(0, 2, 3, 4, 1)
    limit = width_limit.reshape(1, outs)
    in_block = block
    w_spec = pl.BlockSpec((in_block, freqs, 2, kx, outs), lambda i: (i, 0, 0, 0, 0))
    s_spec = pl.BlockSpec((1, kx, LANES), lambda i: (i, 0, 0))
    mode_spec = pl.BlockSpec((freqs, 2, kx, outs), lambda i: (0, 0, 0, 0))
    limit_spec = pl.BlockSpec((1, outs), lambda i: (0, 0))
    partial_modes = pl.pallas_call(
        contract_kernel,
        grid=(channels // in_block,),
        in_specs=[w_spec, s_spec, limit_spec],
        out_specs=mode_spec,
        out_shape=jax.ShapeDtypeStruct((freqs, 2, kx, outs), jnp.float32),
        compiler_params=params,
        name="contract",
    )(weight, spectra, limit)
    halves = partial_modes.reshape(freqs, 2, kx, chans, groups, block)
    halves = halves.transpose(3, 4, 2, 5, 1, 0).reshape(chans, groups, kx, LANES)
    summed_modes = jnp.sum(exchange(halves, ("chan",), False, 2), axis=0)

    col_freq = mode_index * freqs + jnp.arange(freqs, dtype=jnp.int32)
    row_freq = slab_index * kx + jnp.arange(kx, dtype=jnp.int32)
    limit_rows = lax.dynamic_slice_in_dim(mode_limit, chan_index * channels, channels, 0)
    weights = mode_weights(limit_rows, col_freq, row_freq, all_kx, all_rows * all_cols)
    weights = jnp.broadcast_to(weights, (channels, kx, 2, freqs))
    weights = weights.reshape(groups, block, kx, 2 * freqs).transpose(0, 2, 1, 3)
    weights = weights.reshape(groups, kx, LANES)
    out_modes = joined(summed_modes * weights, 3)

    output, grad_sum, grad_partial, sums = pl.pallas_call(
        functools.partial(middle_kernel, modes),
        grid=grid,
        in_specs=[cells, cells, freq_cells, per_channel, per_channel]
        + [whole(t) for t in forward + back],
        out_specs=[cells, cells, freq_cells, per_channel],
        out_shape=[
            field,
            field,
            freq_field,
            jax.ShapeDtypeStruct((channels, 1, LANES), jnp.float32),
        ],
        compiler_params=params,
        name="middle",
    )(source_field, cotangent, out_modes, gain, wide(channel_bias), *forward, *back)

    grad_modes = spread(grad_partial, 5) * weights
    all_grads = exchange(grad_modes, ("chan",), True, 7)
    all_grads = all_grads.reshape(chans, groups, kx, block, 2, freqs)
    all_grads = all_grads.transpose(5, 4, 2, 0, 1, 3).reshape(freqs, 2, kx, outs)
    weight_grad, back_modes = pl.pallas_call(
        back_kernel,
        grid=(channels // in_block,),
        in_specs=[w_spec, s_spec, mode_spec, limit_spec],
        out_specs=[w_spec, s_spec],
        out_shape=[
            jax.ShapeDtypeStruct(weight.shape, jnp.float32),
            jax.ShapeDtypeStruct(spectra.shape, jnp.float32),
        ],
        compiler_params=params,
        name="back",
    )(weight, spectra, all_grads, limit)
    spectral_grad = weight_grad.transpose(0, 4, 1, 2, 3)

    sent = back_modes.size // LANES
    row_sums = sums[:, 0, :2].T.reshape(-1)
    extra = -(-row_sums.size // (8 * LANES)) * 8
    row_sums = jnp.pad(row_sums, (0, extra * LANES - row_sums.size)).reshape(extra, LANES)
    packed = jnp.concatenate([back_modes.reshape(sent, LANES), row_sums], axis=0)
    parts = joined(packed, 8)
    field_modes = parts[:, :sent].reshape(owners, groups, kx, LANES)
    totals = jnp.sum(parts[:, sent:], axis=0).reshape(-1)
    gate_grad = totals[:channels]
    bias_grad = totals[channels : 2 * channels]
    field_grad = pl.pallas_call(
        functools.partial(last_kernel, modes),
        grid=grid,
        in_specs=[cells, freq_cells, per_channel] + [whole(t) for t in back],
        out_specs=cells,
        out_shape=field,
        compiler_params=params,
        name="last",
    )(grad_sum, field_modes, gain, *back)
    return (output, field_grad, spectral_grad, gate_grad, bias_grad)


def halves_of(table):
    table = table.astype(np.float32)
    high = table.astype(ml_dtypes.bfloat16)
    low = (table - high.astype(np.float32)).astype(ml_dtypes.bfloat16)
    return high, low


def packed_tables(all_rows, all_cols, slabs, modes, freqs, kx_all):
    cell = np.arange(all_cols)[:, None]
    angle = (cell * np.arange(modes * freqs)[None, :] % all_cols) * (2.0 * np.pi / all_cols)
    parts = np.stack([np.cos(angle), -np.sin(angle)], axis=1).reshape(modes, -1, 2, modes, freqs)
    parts = parts.transpose(0, 1, 3, 2, 4)
    cols = parts.shape[1]
    high, low = halves_of(parts)
    ahead = np.stack([high, low], axis=3).reshape(modes, cols, -1)
    flat_high = high.reshape(modes, cols, -1).transpose(0, 2, 1)
    flat_low = low.reshape(modes, cols, -1).transpose(0, 2, 1)
    behind = np.concatenate([flat_high, flat_low], axis=1)
    wave = np.arange(kx_all)
    wave = wave + np.where(2 * wave >= kx_all, all_rows - kx_all, 0)
    angle = (np.arange(all_rows)[:, None] * wave[None, :] % all_rows) * (2.0 * np.pi / all_rows)
    table = np.concatenate([np.cos(angle), np.sin(angle)], axis=1).reshape(slabs, -1, 2 * kx_all)
    high, low = halves_of(table)
    row_behind = np.concatenate([high, low], axis=2)
    high, low = high.transpose(0, 2, 1), low.transpose(0, 2, 1)
    row_ahead = np.concatenate([high, low], axis=2)
    return ahead, row_ahead, row_behind, behind


def lane_roll(values, shift):
    shift = shift % values.shape[-1]
    return values if shift == 0 else pltpu.roll(values, shift, values.ndim - 1)


def lanes_of(shape):
    return lax.broadcasted_iota(jnp.int32, shape, len(shape) - 1)


def high_low(values):
    high = values.astype(jnp.bfloat16)
    return high, (values - high.astype(jnp.float32)).astype(jnp.bfloat16)


def quarter_turn(values, span, sign):
    half = span // 2
    first = lanes_of(values.shape) % span < half
    back, ahead = lane_roll(values, -half), lane_roll(values, half)
    return jnp.where(first, -back, ahead) if sign > 0 else jnp.where(first, back, -ahead)


def three_way(row_table, values):
    high, low = high_low(values)
    width = row_table.shape[1] // 2
    left = jnp.concatenate([row_table, row_table[:, :width]], axis=1)
    right = jnp.concatenate([high, high, low], axis=0)
    return jnp.dot(left, right, preferred_element_type=jnp.float32)


def two_way(values, table):
    high, low = high_low(values)
    both = jnp.concatenate([high, low], axis=1)
    return jnp.dot(both, jnp.concatenate([table, table], axis=0), preferred_element_type=jnp.float32)


def mix_rows(lines_ref, row_table, rows, span, kx, store):
    block = LANES // span
    mixed = []
    for c in range(0, block, 2):
        pair = [lines_ref[(c + k) * rows : (c + k + 1) * rows] for k in range(2)]
        both = three_way(row_table, jnp.concatenate(pair, axis=1))
        mixed += [both[:, :LANES], both[:, LANES:]]
    lane = lanes_of(mixed[0].shape)
    pairs = []
    for c in range(0, block, 2):
        left = mixed[c] + lane_roll(mixed[c], -span)
        right = mixed[c + 1] + lane_roll(mixed[c + 1], span)
        pairs.append(jnp.where(lane % (2 * span) < span, left, right))
    low_half = lane < LANES // 2
    owners = [
        jnp.where(low_half, pairs[0], lane_roll(pairs[1], LANES // 2)),
        jnp.where(low_half, lane_roll(pairs[0], LANES // 2), pairs[1]),
    ]
    all_kx = owners[0].shape[0] // 2
    slabs = all_kx // kx
    for m, values in enumerate(owners):
        done = values[:all_kx] + quarter_turn(values[all_kx:], span, -1)
        for s in range(slabs):
            store(m * slabs + s, done[s * kx : (s + 1) * kx])


def group_lines(modes_ref, group, kx, row_table, span):
    block = LANES // span
    owners = modes_ref.shape[0]
    half = owners // 2
    here = pl.ds(pl.multiple_of(group * kx, kx), kx)
    stack = []
    for m in range(2):
        stack.append(jnp.concatenate([modes_ref[m * half + s, here] for s in range(half)], axis=0))
    full = [jnp.concatenate([one, quarter_turn(one, span, 1)], axis=0) for one in stack]
    rolled = [[lane_roll(one, k * span) for k in range(block)] for one in full]
    lane = lanes_of(full[0].shape)
    even = lane % (2 * span) < span
    low_half = lane < LANES // 2
    sides = []
    for c in range(block):
        first = jnp.where(low_half, rolled[0][(0 - c) % block], rolled[0][(2 - c) % block])
        second = jnp.where(low_half, rolled[1][(1 - c) % block], rolled[1][(3 - c) % block])
        sides.append(jnp.where(even, first, second))
    lines = []
    for c in range(0, block, 2):
        both = three_way(row_table, jnp.concatenate([sides[c], sides[c + 1]], axis=1))
        lines += [both[:, :LANES], both[:, LANES:]]
    return lines


def middle_packed(
    span, kx, x_ref, cot_ref, modes_ref, gain_ref, bias_ref, ahead_ref, row_ref, row_back_ref, behind_ref,
    out_ref, grad_ref, spec_ref, sums_ref, split_ref, lines_ref, branch_ref, next_ref, held_ref, made_ref,
):
    block, rows, cols = cot_ref.shape
    step = pl.program_id(0)
    scale = math.sqrt(2.0 / math.pi)
    row_table = row_ref[0]

    @pl.when(step == 0)
    def _():
        sums_ref[...] = jnp.zeros_like(sums_ref)

    def ahead(c):
        here = slice(c * rows, (c + 2) * rows)
        table = ahead_ref[0]
        high = jnp.dot(split_ref[here, :cols], table, preferred_element_type=jnp.float32)
        lines_ref[here] = high + jnp.dot(split_ref[here, cols:], table, preferred_element_type=jnp.float32)

    def finish(from_ref, group):
        def store(owner, values):
            spec_ref[owner, pl.ds(pl.multiple_of(group * kx, kx), kx)] = values
        mix_rows(from_ref, row_table, rows, span, kx, store)

    lane = lanes_of(sums_ref.shape)
    line = lax.broadcasted_iota(jnp.int32, sums_ref.shape, 0)

    def cell(c, lines):
        channel = step * block + c
        gain, shift = gain_ref[channel], bias_ref[channel]
        branch_ref[c] = two_way(lines, behind_ref[0])
        gate = jnp.zeros((8, cols), jnp.float32)
        bias = jnp.zeros((8, cols), jnp.float32)
        for r in range(0, rows, 16):
            here = slice(r, r + 16)
            source = x_ref[channel, here]
            v = branch_ref[c, here] + (gain * source + shift)
            square = v * v
            inner = v * (scale + (scale * 0.044715) * square)
            up = 0.5 + 0.5 * jnp.tanh(inner)
            out_ref[c, here] = v * up
            bend = v * (2.0 * scale + (6.0 * scale * 0.044715) * square)
            grad = cot_ref[c, here] * (up + (up * (1.0 - up)) * bend)
            grad_ref[channel, here] = grad
            high, low = high_low(grad)
            there = slice(c * rows + r, c * rows + r + 16)
            split_ref[there, :cols] = high
            split_ref[there, cols:] = low
            both = grad * source
            gate = gate + (both[:8] + both[8:])
            bias = bias + (grad[:8] + grad[8:])
        gate = jnp.sum(jnp.sum(gate, axis=0, keepdims=True), axis=1, keepdims=True)
        bias = jnp.sum(jnp.sum(bias, axis=0, keepdims=True), axis=1, keepdims=True)
        here = (lane == channel) & (line < 2)
        sums_ref[...] = jnp.where(here, jnp.where(line == 0, gate, bias), sums_ref[...])

    def prepare(group):
        for c, lines in enumerate(group_lines(modes_ref, group, kx, row_back_ref[0], span)):
            next_ref[c] = lines

    @pl.when(step == 0)
    def _():
        prepare(0)

    held_ref[...] = next_ref[...]
    made_ref[...] = lines_ref[...]
    for c in range(block):
        if c % 2 == 0:
            ahead(c)
        cell(c, held_ref[c])
        if c == 0:
            finish(made_ref, jnp.maximum(step - 2, 0))
        if c == 1:
            prepare(jnp.minimum(step + 1, pl.num_programs(0) - 1))

    @pl.when(step == pl.num_programs(0) - 1)
    def _():
        finish(lines_ref, step - 1)
        for c in range(0, block, 2):
            ahead(c)
        finish(lines_ref, step)


def last_packed(
    span, kx, grad_ref, modes_ref, gain_ref, row_back_ref, behind_ref, grads_ref, spec_ref, limit_ref, out_ref, wgrad_ref
):
    block = out_ref.shape[0]
    step = pl.program_id(0)
    lines = group_lines(modes_ref, step, kx, row_back_ref[0], span)
    count, freqs, outs = wgrad_ref.shape[0], wgrad_ref.shape[1], wgrad_ref.shape[4]
    wide = freqs * kx
    first = lax.axis_index("chan") * (count * pl.num_programs(0)) + step * count
    g_real, g_imag = both_parts(grads_ref, slice(None))
    limit = column_of(limit_ref[...], outs, 0)
    for i in range(count):
        keep = jnp.broadcast_to(limit, (outs, wide)) > (first + i).astype(jnp.float32)
        s_real, s_imag = both_parts(spec_ref, pl.ds(step * count + i, 1))
        real = jnp.where(keep, s_real * g_real + s_imag * g_imag, 0.0)
        imag = jnp.where(keep, s_real * g_imag - s_imag * g_real, 0.0)
        wgrad_ref[i, :, 0] = real.T.reshape(freqs, kx, outs)
        wgrad_ref[i, :, 1] = imag.T.reshape(freqs, kx, outs)
    for c in range(block):
        out_ref[c] = two_way(lines[c], behind_ref[0]) + gain_ref[step * block + c] * grad_ref[step * block + c]


def swap_groups(values, kx):
    lane = lanes_of(values.shape) // kx
    line = lax.broadcasted_iota(jnp.int32, values.shape, 1)
    count = values.shape[1]
    hop = 1
    while hop < count:
        up = lane_roll(pltpu.roll(values, count - hop, 1), hop * kx)
        down = lane_roll(pltpu.roll(values, hop, 1), -hop * kx)
        lane_bit, line_bit = lane // hop % 2, line // hop % 2
        values = jnp.where(lane_bit == line_bit, values, jnp.where(lane_bit == 1, up, down))
        hop *= 2
    return values


def to_lanes(packed, out_ref, kx):
    lines = swap_groups(packed.T.reshape(-1, 8, LANES), kx)
    wide = out_ref.shape[0]
    block = lines.shape[0] // wide
    for c in range(block):
        for j in range(wide):
            out_ref[j, pl.ds(c, 8, stride=block)] = lines[c * wide + j]


def to_rows(wide_ref, block, kx):
    wide = wide_ref.shape[0]
    pieces = []
    for c in range(block):
        for j in range(wide):
            pieces.append(wide_ref[j, pl.ds(c, 8, stride=block)][None])
    return swap_groups(jnp.concatenate(pieces, axis=0), kx).reshape(-1, LANES).T


def both_parts(ref, rows):
    half = ref.shape[0] // 2
    parts = [jnp.concatenate([ref[p * half + j, rows] for j in range(half)], axis=1) for p in range(2)]
    return parts[0], parts[1]


def put_part(ref, rows, part, values):
    half = ref.shape[0] // 2
    for j in range(half):
        ref[part * half + j, rows] = values[:, j * LANES : (j + 1) * LANES]


def other(axis, step, size):
    return lax.rem(lax.axis_index(axis) + step, size)


def send(source, target, sends, recvs, axis, peer):
    copy = pltpu.make_async_remote_copy(
        src_ref=source, dst_ref=target, send_sem=sends, recv_sem=recvs,
        device_id={axis: peer}, device_id_type=pl.DeviceIdType.MESH,
    )
    copy.start()
    return copy


def column_of(row, count, first):
    shape = (count, row.shape[1])
    hit = lanes_of(shape) == first + lax.broadcasted_iota(jnp.int32, shape, 0)
    return jnp.sum(jnp.where(hit, row.astype(jnp.float32), 0.0), axis=1, keepdims=True)


def mode_scales(limit_ref, shape, kx, cells_total):
    wide, count, _ = shape
    first = lax.axis_index("chan") * count
    cols = jnp.broadcast_to(column_of(limit_ref[0:1], count, first), (count, LANES))
    rows = jnp.broadcast_to(column_of(limit_ref[1:2], count, first), (count, LANES))
    all_kx = (kx * lax.axis_size("slab"))
    tiles = []
    for j in range(wide):
        cell = lanes_of((count, LANES)) + j * LANES
        col = (lax.axis_index("mode") * (wide * LANES // kx) + cell // kx).astype(jnp.float32)
        row = (lax.axis_index("slab") * kx + cell % kx).astype(jnp.float32)
        kept = (col < cols) & ((row < rows) | (all_kx - row < rows))
        scale = jnp.where(col < 0.5, 1.0, 2.0) / cells_total
        tiles.append(jnp.where(kept, scale, 0.0)[None])
    return jnp.concatenate(tiles, axis=0)


def greet(slabs):
    barrier = pltpu.get_barrier_semaphore()
    targets = [("mode", 1, 2), ("chan", 1, 2)] + [("slab", step, slabs) for step in range(1, slabs)]
    for axis, step, size in targets:
        pl.semaphore_signal(
            barrier, inc=1, device_id={axis: other(axis, step, size)}, device_id_type=pl.DeviceIdType.MESH
        )
    pl.semaphore_wait(barrier, len(targets))


def scatter_sum(part_ref, half_ref, give_ref, take_ref, mode_sems, slab_sems, slabs, between):
    me_mode, me_slab = lax.axis_index("mode"), lax.axis_index("slab")
    peer = other("mode", 1, 2)
    order = [slabs // 2] + [step for step in range(1, slabs) if step != slabs // 2] + [0]
    copies = []
    for step in order:
        slab = other("slab", step, slabs)
        copies.append(send(
            part_ref.at[peer * slabs + slab], half_ref.at[step], mode_sems.at[0, step], mode_sems.at[1, step], "mode", peer
        ))
    waits = list(copies)
    out = []
    for step, copy in zip(order, copies):
        copy.wait_recv()
        slab = other("slab", step, slabs)
        total = part_ref[me_mode * slabs + slab] + half_ref[step]
        if step == 0:
            mine = total
        else:
            give_ref[step] = total
            out.append(send(
                give_ref.at[step], take_ref.at[step], slab_sems.at[0, step], slab_sems.at[1, step], "slab", slab
            ))
    between()
    for copy in out:
        copy.wait_recv()
    for step in range(1, slabs):
        mine = mine + take_ref[step]
    return mine, [copy.wait_send for copy in copies + out]


def gather_start(own_ref, out_ref, mode_sems, slab_sems, slabs):
    me = lax.axis_index("mode") * slabs + lax.axis_index("slab")
    copies = []
    for step in [slabs // 2] + [step for step in range(1, slabs) if step != slabs // 2]:
        copies.append(send(
            own_ref, out_ref.at[me], slab_sems.at[0, step], slab_sems.at[1, step], "slab", other("slab", step, slabs)
        ))
    near = send(own_ref, out_ref.at[me], mode_sems.at[0, 0], mode_sems.at[1, 0], "mode", other("mode", 1, 2))
    out_ref[me] = own_ref[...]
    return copies, near


def gather_finish(state, out_ref, mode_sems, slabs, between):
    copies, near = state
    relays = []
    order = [slabs // 2] + [step for step in range(1, slabs) if step != slabs // 2]
    for k in list(range(1, slabs - 1)) + [0]:
        between(k)
        copies[k].wait_recv()
        step = order[k]
        source = lax.axis_index("mode") * slabs + other("slab", slabs - step, slabs)
        relays.append(send(
            out_ref.at[source], out_ref.at[source], mode_sems.at[0, step], mode_sems.at[1, step], "mode", other("mode", 1, 2)
        ))
    near.wait()
    for copy in relays:
        copy.wait()
    for copy in copies:
        copy.wait_send()


def forward_kernel(
    span, slabs, kx, x_ref, ahead_ref, row_ref, w_ref, limit_ref, mode_limit_ref, out_ref, turned_ref, spec_ref, x_buf, kept_ref,
    part_ref, half_ref, give_ref, take_ref, w_buf, t_buf, sum_ref, peer_ref, own_ref, lines_ref, ahead_buf, row_buf,
    mode_a, slab_a, mode_b, slab_b, chan_sems, x_sems, w_sems, table_sems, t_sems,
):
    ins, freqs, outs = w_ref.shape[0], w_ref.shape[1], w_ref.shape[4]
    rows, cols = x_ref.shape[1:]
    block = LANES // span
    groups = ins // block
    mine_outs = outs // 2
    wide = freqs * kx
    me_mode, me_slab = lax.axis_index("mode"), lax.axis_index("slab")
    peer_mode = other("mode", 1, 2)
    first = lax.axis_index("chan") * ins
    tables = [
        pltpu.make_async_copy(ahead_ref.at[me_mode], ahead_buf, table_sems.at[0]),
        pltpu.make_async_copy(row_ref.at[me_slab], row_buf, table_sems.at[1]),
    ]
    tables[0].start()

    def x_copy(k):
        here = pl.ds(k * (block // 2), block // 2)
        return pltpu.make_async_copy(x_ref.at[here], x_buf.at[here], x_sems.at[k])

    def w_copy(g):
        here = pl.ds(g * block, block)
        return pltpu.make_async_copy(w_ref.at[here], w_buf.at[here], w_sems.at[g])

    for g in range(groups):
        x_copy(2 * g).start()
        x_copy(2 * g + 1).start()
        if g == 0:
            tables[1].start()
    for g in range(groups):
        w_copy(g).start()
    greet(slabs)

    def t_copy(g):
        here = pl.ds(g * block, block)
        return pltpu.make_async_copy(t_buf.at[here], turned_ref.at[here], t_sems.at[g])

    def place(g):
        return pl.ds(pl.multiple_of(g * kx, kx), kx)

    def mode_copy(g):
        return pltpu.make_async_remote_copy(
            src_ref=part_ref.at[pl.ds(peer_mode * slabs, slabs), place(g)], dst_ref=half_ref.at[:, place(g)],
            send_sem=mode_a.at[0, g], recv_sem=mode_a.at[1, g],
            device_id={"mode": peer_mode}, device_id_type=pl.DeviceIdType.MESH,
        )

    def slab_copy(step, g):
        return pltpu.make_async_remote_copy(
            src_ref=give_ref.at[step, place(g)], dst_ref=take_ref.at[step, place(g)],
            send_sem=slab_a.at[0, step, g], recv_sem=slab_a.at[1, step, g],
            device_id={"slab": other("slab", step, slabs)}, device_id_type=pl.DeviceIdType.MESH,
        )

    def ahead(g):
        x_copy(2 * g).wait()
        x_copy(2 * g + 1).wait()
        values = x_buf[pl.ds(g * block, block)].reshape(block * rows, cols)
        lines_ref[...] = two_way(values, ahead_buf[...])

    def finish(g):
        def store(owner, values):
            part_ref[owner, place(g)] = values
        mix_rows(lines_ref, row_buf[...], rows, span, kx, store)

    limit = column_of(limit_ref[...], outs, 0)

    def flip(g):
        for k in range(block):
            i = g * block + k
            keep = jnp.broadcast_to(limit, (outs, wide)) > (first + i).astype(jnp.float32)
            for p in range(2):
                turned = w_buf[i, :, p].reshape(wide, outs).T
                t_buf[i, :, p * wide : (p + 1) * wide] = jnp.where(keep, turned, 0.0)

    def pass_on(g):
        mode_copy(g).wait_recv()
        for step in [slabs // 2] + [step for step in range(1, slabs) if step != slabs // 2]:
            slab = other("slab", step, slabs)
            give_ref[step, place(g)] = part_ref[me_mode * slabs + slab, place(g)] + half_ref[slab, place(g)]
            slab_copy(step, g).start()

    for table in tables:
        table.wait()
    ahead(0)

    def body(g, carry):
        finish(g - 1)
        ahead(g)
        mode_copy(g - 1).start()

        @pl.when(g > 1)
        def _():
            pass_on(g - 2)
        return carry

    lax.fori_loop(1, groups, body, 0)
    finish(groups - 1)
    mode_copy(groups - 1).start()
    pass_on(groups - 2)
    pass_on(groups - 1)
    kept_ref[...] = mode_scales(mode_limit_ref, kept_ref.shape, kx, slabs * rows * 2 * cols)

    def turn_over(g, carry):
        w_copy(g).wait()
        flip(g)
        t_copy(g).start()
        return carry
    lax.fori_loop(0, groups, turn_over, 0)
    mine = part_ref[me_mode * slabs + me_slab] + half_ref[me_slab]

    def landed(g, carry):
        for step in range(1, slabs):
            slab_copy(step, g).wait_recv()
        return carry
    lax.fori_loop(0, groups, landed, 0)
    for step in range(1, slabs):
        mine = mine + take_ref[step]
    to_lanes(mine, spec_ref, kx)

    def contract(i, carry):
        real, imag = carry
        w_real, w_imag = t_buf[i, :, :wide], t_buf[i, :, wide:]
        s_real, s_imag = both_parts(spec_ref, pl.ds(i, 1))
        return real + (s_real * w_real - s_imag * w_imag), imag + (s_real * w_imag + s_imag * w_real)

    zero = jnp.zeros((outs, wide), jnp.float32)
    real, imag = lax.fori_loop(0, ins, contract, (zero, zero))
    put_part(sum_ref, slice(None), 0, real)
    put_part(sum_ref, slice(None), 1, imag)
    theirs = other("chan", 1, 2) * mine_outs
    swap = send(
        sum_ref.at[:, pl.ds(theirs, mine_outs)], peer_ref, chan_sems.at[0], chan_sems.at[1], "chan", other("chan", 1, 2)
    )
    swap.wait_recv()
    for j in range(peer_ref.shape[0]):
        peer_ref[j] = (sum_ref[j, pl.ds(first, mine_outs)] + peer_ref[j]) * kept_ref[j % kept_ref.shape[0]]
    own_ref[...] = to_rows(peer_ref, mine_outs // 8, kx)
    state = gather_start(own_ref, out_ref, mode_b, slab_b, slabs)
    gather_finish(state, out_ref, mode_b, slabs, lambda k: None)
    swap.wait_send()

    def settle(g, carry):
        t_copy(g).wait()
        mode_copy(g).wait_send()
        for step in range(1, slabs):
            slab_copy(step, g).wait_send()
        return carry
    lax.fori_loop(0, groups, settle, 0)


def backward_kernel(
    slabs, kx, part_ref, sums_ref, turned_ref, weight_ref, out_ref, grad_ref, total_ref,
    half_ref, give_ref, take_ref, t_buf, back_ref, own_ref, near_ref, far_ref, pass_ref,
    mode_a, slab_a, mode_b, slab_b, chan_sems, sum_mode, sum_slab, t_sem,
):
    ins, outs, wide = t_buf.shape[0], t_buf.shape[1], t_buf.shape[2] // 2
    mine_outs = outs // 2
    load = pltpu.make_async_copy(turned_ref, t_buf, t_sem)
    load.start()
    greet(slabs)
    first = lax.axis_index("chan") * ins
    near = send(sums_ref, near_ref, sum_mode.at[0], sum_mode.at[1], "mode", other("mode", 1, 2))

    far = []
    def total_up():
        near.wait_recv()
        pass_ref[...] = sums_ref[...] + near_ref[...]
        for step in range(1, slabs):
            far.append(send(
                pass_ref, far_ref.at[step], sum_slab.at[0, step], sum_slab.at[1, step], "slab", other("slab", step, slabs)
            ))

    mine, sent = scatter_sum(part_ref, half_ref, give_ref, take_ref, mode_a, slab_a, slabs, total_up)
    to_lanes(mine, back_ref, kx)
    here = pl.ds(first, mine_outs)
    for j in range(back_ref.shape[0]):
        grad_ref[j, here] = back_ref[j] * weight_ref[j % weight_ref.shape[0]]
    swap = send(
        grad_ref.at[:, here], grad_ref.at[:, here], chan_sems.at[0], chan_sems.at[1], "chan", other("chan", 1, 2)
    )
    load.wait()
    swap.wait_recv()

    def pull(i, carry):
        w_real, w_imag = t_buf[i, :, :wide], t_buf[i, :, wide:]
        g_real, g_imag = both_parts(grad_ref, slice(None))
        put_part(back_ref, pl.ds(i, 1), 0, jnp.sum(g_real * w_real + g_imag * w_imag, axis=0, keepdims=True))
        put_part(back_ref, pl.ds(i, 1), 1, jnp.sum(g_imag * w_real - g_real * w_imag, axis=0, keepdims=True))
        return carry
    lax.fori_loop(0, ins, pull, 0)
    own_ref[...] = to_rows(back_ref, ins // 8, kx)
    state = gather_start(own_ref, out_ref, mode_b, slab_b, slabs)
    gather_finish(state, out_ref, mode_b, slabs, lambda k: None)
    total = pass_ref[...]
    for step, copy in zip(range(1, slabs), far):
        copy.wait()
        total = total + far_ref[step]
    total_ref[...] = total
    near.wait_send()
    swap.wait_send()
    for wait in sent:
        wait()


def fits(shapes, mesh_sizes):
    channels, rows, cols = shapes[0]
    outs, freqs, kx = shapes[2][1], shapes[2][2], shapes[2][4]
    slabs, modes, chans = mesh_sizes
    return (
        modes == 2 and chans == 2 and slabs > 2 and slabs % 2 == 0
        and 8 * kx == LANES and 8 * freqs == LANES and 2 * freqs * channels == 8 * LANES
        and outs == chans * channels
        and rows % LANES == 0 and cols % LANES == 0
    )


def local(source_field, cotangent, spectral_weight, skip_gain, channel_bias, mode_limit, width_limit):
    slabs, modes, chans = (lax.axis_size(axis) for axis in ("slab", "mode", "chan"))
    args = (source_field, cotangent, spectral_weight, skip_gain, channel_bias, mode_limit, width_limit)
    if not fits([one.shape for one in args], (slabs, modes, chans)):
        return local_plain(*args)
    channels, rows, cols = source_field.shape
    outs, freqs, kx = spectral_weight.shape[1], spectral_weight.shape[2], spectral_weight.shape[4]
    span = 2 * freqs
    block = LANES // span
    groups = channels // block
    owners = slabs * modes
    all_kx, all_rows, all_cols = kx * slabs, rows * slabs, cols * modes
    wide = freqs * kx
    ahead, row_ahead, row_behind, behind = (
        jnp.asarray(t) for t in packed_tables(all_rows, all_cols, slabs, modes, freqs, all_kx)
    )

    def pick(table, axis):
        return pl.BlockSpec((1,) + table.shape[1:], lambda g: (lax.axis_index(axis), 0, 0))

    cells = pl.BlockSpec((block, rows, cols), lambda g: (g, 0, 0))
    scalars = pl.BlockSpec(memory_space=pltpu.SMEM)
    field = jax.ShapeDtypeStruct(source_field.shape, jnp.float32)
    room = lambda size: pltpu.CompilerParams(dimension_semantics=("arbitrary",), vmem_limit_bytes=size * MIB)
    f32 = jnp.float32

    weight = spectral_weight.transpose(0, 2, 3, 4, 1)
    limit = width_limit.reshape(1, outs)

    dma, vmem = pltpu.SemaphoreType.DMA, pltpu.VMEM
    in_vmem, anywhere = pl.BlockSpec(memory_space=pltpu.VMEM), pl.BlockSpec(memory_space=pl.ANY)
    piece = (groups * kx, LANES)
    common = [vmem((slabs,) + piece, f32), vmem((slabs,) + piece, f32), vmem((slabs,) + piece, f32)]
    pair = [dma((2, slabs))] * 4
    comm = lambda ident, room: pltpu.CompilerParams(
        collective_id=ident, has_side_effects=True, vmem_limit_bytes=room * MIB
    )
    flat = lambda lines: (2 * wide // LANES, lines, LANES)

    in_hbm = lambda array: pltpu.with_memory_space_constraint(array, pltpu.HBM)
    held = lambda array: pltpu.with_memory_space_constraint(array, pltpu.VMEM)
    modes_shape = (owners,) + piece
    out_modes, turned, spec, source_held, weights = pl.pallas_call(
        functools.partial(forward_kernel, span, slabs, kx),
        in_specs=[anywhere, anywhere, anywhere, anywhere, in_vmem, in_vmem],
        out_specs=[in_vmem, anywhere, in_vmem, in_vmem, in_vmem],
        out_shape=[
            jax.ShapeDtypeStruct(modes_shape, f32), pltpu.HBM((channels, outs, 2 * wide), f32),
            jax.ShapeDtypeStruct(flat(channels), f32), pltpu.VMEM(field.shape, f32),
            jax.ShapeDtypeStruct((wide // LANES, channels, LANES), f32),
        ],
        scratch_shapes=[vmem(modes_shape, f32)] + common + [
            vmem(weight.shape, f32), vmem((channels, outs, 2 * wide), f32), vmem(flat(outs), f32), vmem(flat(outs // 2), f32), vmem(piece, f32),
            vmem((block * rows, LANES), f32), vmem(ahead.shape[1:], jnp.bfloat16), vmem(row_ahead.shape[1:], jnp.bfloat16),
            dma((2, groups)), dma((2, slabs, groups)), dma((2, slabs)), dma((2, slabs)), dma((2,)),
            dma((2 * groups,)), dma((groups,)), dma((2,)), dma((groups,)),
        ],
        compiler_params=comm(20, FORWARD),
        name="forward_modes",
    )(in_hbm(source_field), in_hbm(ahead), in_hbm(row_ahead), in_hbm(weight), limit, mode_limit.T)

    output, grad_sum, grad_partial, sums = pl.pallas_call(
        functools.partial(middle_packed, span, kx),
        grid=(groups,),
        in_specs=[
            in_vmem, cells, in_vmem, scalars, scalars, pick(ahead, "mode"), pick(row_ahead, "slab"),
            pick(row_behind, "slab"), pick(behind, "mode"),
        ],
        out_specs=[cells, in_vmem, in_vmem, in_vmem],
        out_shape=[field, pltpu.VMEM(field.shape, f32), jax.ShapeDtypeStruct(modes_shape, f32), jax.ShapeDtypeStruct((8, LANES), f32)],
        scratch_shapes=[
            vmem((block * rows, 2 * cols), jnp.bfloat16), vmem((block * rows, LANES), f32), vmem((block, rows, cols), f32),
            vmem((block, rows, LANES), f32), vmem((block, rows, LANES), f32), vmem((block * rows, LANES), f32),
        ],
        input_output_aliases={0: 1},
        compiler_params=room(MIDDLE),
        name="middle",
    )(
        held(source_held), cotangent, out_modes, skip_gain, channel_bias,
        ahead, row_ahead, row_behind, behind,
    )

    back_modes, all_grads, totals = pl.pallas_call(
        functools.partial(backward_kernel, slabs, kx),
        in_specs=[in_vmem, in_vmem, anywhere, in_vmem],
        out_specs=[in_vmem] * 3,
        out_shape=[jax.ShapeDtypeStruct(modes_shape, f32), jax.ShapeDtypeStruct(flat(outs), f32), jax.ShapeDtypeStruct((8, LANES), f32)],
        scratch_shapes=common + [
            vmem((channels, outs, 2 * wide), f32), vmem(flat(channels), f32), vmem(piece, f32), vmem((8, LANES), f32),
            vmem((slabs, 8, LANES), f32), vmem((8, LANES), f32),
        ] + pair + [dma((2,)), dma((2,)), dma((2, slabs)), dma],
        compiler_params=comm(21, BACKWARD),
        name="backward_modes",
    )(grad_partial, sums, in_hbm(turned), weights)

    count = channels // groups
    whole = lambda array: pl.BlockSpec(array.shape, lambda g: (0,) * array.ndim)
    field_grad, weight_grad = pl.pallas_call(
        functools.partial(last_packed, span, kx),
        grid=(groups,),
        in_specs=[
            in_vmem, in_vmem, scalars, pick(row_behind, "slab"), pick(behind, "mode"),
            whole(all_grads), whole(spec), whole(limit),
        ],
        out_specs=[cells, pl.BlockSpec((count,) + weight.shape[1:], lambda g: (g, 0, 0, 0, 0))],
        out_shape=[field, jax.ShapeDtypeStruct(weight.shape, f32)],
        compiler_params=room(LAST),
        name="last",
    )(
        pltpu.with_memory_space_constraint(grad_sum, pltpu.VMEM), back_modes, skip_gain,
        row_behind, behind, all_grads, spec, limit,
    )
    spectral_grad = weight_grad.transpose(0, 4, 1, 2, 3)
    return (output, field_grad, spectral_grad, totals[0, :channels], totals[1, :channels])


def solution(mesh):
    in_specs = (
        P(("member", "chan"), "slab", "mode"),
        P(("member", "chan"), "slab", "mode"),
        P(("member", "chan"), None, "mode", None, "slab"),
        P(("member", "chan")),
        P(("member", "chan")),
        P("member", None),
        P("member"),
    )
    out_specs = (
        P(("member", "chan"), "slab", "mode"),
        P(("member", "chan"), "slab", "mode"),
        P(("member", "chan"), None, "mode", None, "slab"),
        P(("member", "chan")),
        P(("member", "chan")),
    )
    return jax.shard_map(local, mesh=mesh, in_specs=in_specs, out_specs=out_specs, check_vma=False)
```

```python
import functools
import math

import jax
import jax.numpy as jnp
import ml_dtypes
import numpy as np
from jax import lax
from jax.experimental import pallas as pl
from jax.experimental.pallas import tpu as pltpu
from jax.sharding import PartitionSpec as P

LANES = 128
BIG = 60 * 1024 * 1024
MIB = 1024 * 1024
FORWARD, MIDDLE, LAST, BACKWARD = 40, 40, 40, 20


def split_table(table):
    high = lax.reduce_precision(table, 8, 7)
    return high.astype(jnp.bfloat16), (table - high).astype(jnp.bfloat16)


def split_block(values):
    high = values.astype(jnp.bfloat16)
    return high, (values - high.astype(jnp.float32)).astype(jnp.bfloat16)


def dot_pair(left, right):
    left_high, left_low = left
    right_high, right_low = right
    mul = functools.partial(jnp.dot, preferred_element_type=jnp.float32)
    return mul(left_high, right_high) + mul(left_low, right_high) + mul(left_high, right_low)


def tables(extent, waves, first_cell, cell_count):
    cell_index = first_cell + jnp.arange(cell_count, dtype=jnp.int32)
    products = (cell_index[:, None] * waves[None, :] % extent).astype(jnp.float32)
    angles = products * (2.0 * math.pi / extent)
    return jnp.cos(angles), jnp.sin(angles)


def store_spectrum(values, col_pair, row_pair, out_ref):
    block, rows, cols = values.shape
    lines = dot_pair(split_block(values.reshape(block * rows, cols)), col_pair)
    all_kx = row_pair[0].shape[0] // 2
    kx, lanes = out_ref.shape[2:]
    span = lanes // block
    mode_count = lines.shape[1] // span
    slabs = out_ref.shape[0] // mode_count
    done = []
    for c in range(block):
        mixed = dot_pair(row_pair, split_block(lines[c * rows : (c + 1) * rows]))
        done.append(mixed[:all_kx] - turn(mixed[all_kx:], span))
    for m in range(mode_count):
        packed = jnp.concatenate([one[:, m * span : (m + 1) * span] for one in done], axis=1)
        for s in range(slabs):
            out_ref[m * slabs + s, 0] = packed[s * kx : (s + 1) * kx]


def turn(values, span):
    half = span // 2
    pieces = []
    for first in range(0, values.shape[1], span):
        pieces.append(-values[:, first + half : first + span])
        pieces.append(values[:, first : first + half])
    return jnp.concatenate(pieces, axis=1)


def all_modes(modes_ref, mode_count, c, block):
    span = modes_ref.shape[3] // block
    slabs = modes_ref.shape[0] // mode_count
    columns = []
    for m in range(mode_count):
        stack = [modes_ref[m * slabs + s, 0] for s in range(slabs)]
        columns.append(jnp.concatenate(stack, axis=0)[:, c * span : (c + 1) * span])
    return jnp.concatenate(columns, axis=1), span


def synth(modes_and_span, row_pair, col_pair):
    modes, span = modes_and_span
    stacked = jnp.concatenate([modes, turn(modes, span)], axis=0)
    lines = dot_pair(row_pair, split_block(stacked))
    return dot_pair(split_block(lines), col_pair)


def spectrum_kernel(x_ref, ch_ref, cl_ref, rh_ref, rl_ref, out_ref):
    store_spectrum(x_ref[...], (ch_ref[...], cl_ref[...]), (rh_ref[...], rl_ref[...]), out_ref)


def middle_kernel(
    mode_count, x_ref, cot_ref, modes_ref, gain_ref, bias_ref, ch_ref, cl_ref, rh_ref, rl_ref,
    cth_ref, ctl_ref, ih_ref, il_ref, out_ref, grad_ref, spec_ref, sums_ref,
):
    block = x_ref.shape[0]
    row_back = (ih_ref[...], il_ref[...])
    col_back = (cth_ref[...], ctl_ref[...])
    scale = math.sqrt(2.0 / math.pi)
    for c in range(block):
        source = x_ref[c]
        gain = gain_ref[c]
        v = synth(all_modes(modes_ref, mode_count, c, block), row_back, col_back) + gain[:, :1] * source + bias_ref[c][:, :1]
        square = v * v
        t = jnp.tanh(scale * v * (1.0 + 0.044715 * square))
        half_up = 0.5 * (1.0 + t)
        out_ref[c] = v * half_up
        slope = half_up + 0.5 * v * (1.0 - t * t) * (scale * (1.0 + 3.0 * 0.044715 * square))
        grad = cot_ref[c] * slope
        grad_ref[c] = grad
        gate = jnp.sum(jnp.sum(grad * source, axis=0, keepdims=True), axis=1, keepdims=True)
        bias = jnp.sum(jnp.sum(grad, axis=0, keepdims=True), axis=1, keepdims=True)
        lane = lax.broadcasted_iota(jnp.int32, (1, LANES), 1)
        sums_ref[c] = jnp.where(lane == 0, gate, bias)
    store_spectrum(
        grad_ref[...], (ch_ref[...], cl_ref[...]), (rh_ref[...], rl_ref[...]), spec_ref
    )


def last_kernel(mode_count, grad_ref, modes_ref, gain_ref, cth_ref, ctl_ref, ih_ref, il_ref, out_ref):
    block = grad_ref.shape[0]
    for c in range(block):
        modes = all_modes(modes_ref, mode_count, c, block)
        branch = synth(modes, (ih_ref[...], il_ref[...]), (cth_ref[...], ctl_ref[...]))
        out_ref[c] = branch + gain_ref[c][:, :1] * grad_ref[c]


def contract_kernel(w_ref, spec_ref, limit_ref, out_ref):
    block, freqs, _, kx, outs = w_ref.shape
    first = lax.axis_index("chan") * (block * pl.num_programs(0)) + pl.program_id(0) * block

    @pl.when(pl.program_id(0) == 0)
    def _():
        out_ref[...] = jnp.zeros_like(out_ref)

    limit = limit_ref[...]
    for y in range(freqs):
        real = out_ref[y, 0]
        imag = out_ref[y, 1]
        for i in range(block):
            keep = first + i < limit
            spec = spec_ref[0]
            at = 2 * freqs * i + y
            s_real = jnp.where(keep, spec[:, at : at + 1], 0.0)
            s_imag = jnp.where(keep, spec[:, freqs + at : freqs + at + 1], 0.0)
            w_real = w_ref[i, y, 0]
            w_imag = w_ref[i, y, 1]
            real = real + (s_real * w_real - s_imag * w_imag)
            imag = imag + (s_real * w_imag + s_imag * w_real)
        out_ref[y, 0] = real
        out_ref[y, 1] = imag


def back_kernel(w_ref, spec_ref, grads_ref, limit_ref, wgrad_ref, out_ref):
    block, freqs, _, kx, outs = w_ref.shape
    first = lax.axis_index("chan") * (block * pl.num_programs(0)) + pl.program_id(0) * block
    limit = limit_ref[...]
    lane = lax.broadcasted_iota(jnp.int32, out_ref.shape[1:], 1)
    spec = spec_ref[0]
    back = jnp.zeros(out_ref.shape[1:], jnp.float32)
    for i in range(block):
        keep = first + i < limit
        for y in range(freqs):
            at = 2 * freqs * i + y
            g_real = jnp.where(keep, grads_ref[y, 0], 0.0)
            g_imag = jnp.where(keep, grads_ref[y, 1], 0.0)
            s_real = spec[:, at : at + 1]
            s_imag = spec[:, freqs + at : freqs + at + 1]
            wgrad_ref[i, y, 0] = s_real * g_real + s_imag * g_imag
            wgrad_ref[i, y, 1] = s_real * g_imag - s_imag * g_real
            w_real = w_ref[i, y, 0]
            w_imag = w_ref[i, y, 1]
            b_real = jnp.sum(g_real * w_real + g_imag * w_imag, axis=1, keepdims=True)
            b_imag = jnp.sum(g_imag * w_real - g_real * w_imag, axis=1, keepdims=True)
            back = jnp.where(lane == at, b_real, back)
            back = jnp.where(lane == freqs + at, b_imag, back)
    out_ref[0] = back


def exchange_kernel(axes, sizes, gather, x_ref, out_ref, send_sem, recv_sem, own_sem):
    total = math.prod(sizes)
    me = lax.axis_index(axes[0])
    for axis, size in zip(axes[1:], sizes[1:]):
        me = me * size + lax.axis_index(axis)

    def place(index):
        coords = {}
        for axis, size in reversed(list(zip(axes, sizes))):
            coords[axis] = lax.rem(index, size)
            index = lax.div(index, size)
        return coords

    barrier = pltpu.get_barrier_semaphore()
    for step in range(1, total):
        pl.semaphore_signal(
            barrier, inc=1, device_id=place(lax.rem(me + step, total)),
            device_id_type=pl.DeviceIdType.MESH,
        )
    pl.semaphore_wait(barrier, total - 1)
    copies = []
    for step in range(1, total):
        peer = lax.rem(me + step, total)
        copy = pltpu.make_async_remote_copy(
            src_ref=x_ref if gather else x_ref.at[peer],
            dst_ref=out_ref.at[me],
            send_sem=send_sem.at[step],
            recv_sem=recv_sem.at[step],
            device_id=place(peer),
            device_id_type=pl.DeviceIdType.MESH,
        )
        copy.start()
        copies.append(copy)
    own = pltpu.make_async_copy(x_ref if gather else x_ref.at[me], out_ref.at[me], own_sem)
    own.start()
    own.wait()
    for copy in copies:
        copy.wait()


def exchange(values, axes, gather, ident):
    sizes = tuple(lax.axis_size(axis) for axis in axes)
    total = math.prod(sizes)
    piece = values.shape if gather else values.shape[1:]
    flat = values.reshape((-1, LANES) if gather else (total, -1, LANES))
    out = pl.pallas_call(
        functools.partial(exchange_kernel, axes, sizes, gather),
        out_shape=jax.ShapeDtypeStruct((total,) + flat.shape[-2:], jnp.float32),
        in_specs=[pl.BlockSpec(memory_space=pltpu.VMEM)],
        out_specs=pl.BlockSpec(memory_space=pltpu.VMEM),
        scratch_shapes=[
            pltpu.SemaphoreType.DMA((total,)),
            pltpu.SemaphoreType.DMA((total,)),
            pltpu.SemaphoreType.DMA,
        ],
        compiler_params=pltpu.CompilerParams(collective_id=ident, has_side_effects=True),
        name="exchange" + str(ident),
    )(flat)
    return out.reshape((total,) + piece)


def mode_weights(limit_rows, col_freq, row_freq, kx_count, cells_total):
    keep_cols = col_freq[None, :] < limit_rows[:, 0:1]
    keep_rows = (row_freq[None, :] < limit_rows[:, 1:2]) | (
        (kx_count - row_freq)[None, :] < limit_rows[:, 1:2]
    )
    scales = jnp.where(col_freq == 0, 1.0, 2.0).astype(jnp.float32) / cells_total
    joined = keep_rows[:, :, None] & keep_cols[:, None, :]
    return (joined.astype(jnp.float32) * scales[None, None, :])[:, :, None, :]


def local_plain(
    source_field, cotangent, spectral_weight, skip_gain, channel_bias, mode_limit, width_limit
):
    channels, row_count, col_count = source_field.shape
    slabs = lax.axis_size("slab")
    modes = lax.axis_size("mode")
    chans = lax.axis_size("chan")
    slab_index = lax.axis_index("slab")
    mode_index = lax.axis_index("mode")
    chan_index = lax.axis_index("chan")
    outs = spectral_weight.shape[1]
    freqs = spectral_weight.shape[2]
    kx = spectral_weight.shape[4]
    all_freqs = freqs * modes
    all_kx = kx * slabs
    all_rows = row_count * slabs
    all_cols = col_count * modes

    col_waves = jnp.arange(all_freqs, dtype=jnp.int32)
    row_waves = jnp.arange(all_kx, dtype=jnp.int32)
    row_waves = row_waves + jnp.where(2 * row_waves >= all_kx, all_rows - all_kx, 0)
    col_cos, col_sin = tables(all_cols, col_waves, mode_index * col_count, col_count)
    row_cos, row_sin = tables(all_rows, row_waves, slab_index * row_count, row_count)
    col_tab = jnp.stack(
        [col_cos.reshape(-1, modes, freqs), -col_sin.reshape(-1, modes, freqs)], axis=2
    ).reshape(col_count, 2 * all_freqs)
    row_tab = jnp.concatenate([row_cos, row_sin], axis=1)
    col_pair = split_table(col_tab)
    col_back = tuple(part.T for part in col_pair)
    row_back = split_table(row_tab)
    row_pair = tuple(part.T for part in row_back)

    block = LANES // (2 * freqs)
    groups = channels // block
    owners = slabs * modes
    cells = pl.BlockSpec((block, row_count, col_count), lambda c: (c, 0, 0))
    freq_cells = pl.BlockSpec((owners, 1, kx, LANES), lambda c: (0, c, 0, 0))
    per_channel = pl.BlockSpec((block, 1, LANES), lambda c: (c, 0, 0))
    field = jax.ShapeDtypeStruct(source_field.shape, jnp.float32)
    freq_field = jax.ShapeDtypeStruct((owners, groups, kx, LANES), jnp.float32)
    params = pltpu.CompilerParams(
        dimension_semantics=("arbitrary",), vmem_limit_bytes=BIG
    )

    def whole(array):
        return pl.BlockSpec(array.shape, lambda c: (0,) * array.ndim)

    grid = (channels // block,)
    wide = lambda values: jnp.broadcast_to(values[:, None, None], (channels, 1, LANES))
    gain = wide(skip_gain)
    forward = col_pair + row_pair
    back = col_back + row_back

    def spread(partial, ident):
        half = exchange(partial.reshape(modes, -1, LANES), ("mode",), False, ident)
        half = jnp.sum(half, axis=0).reshape(slabs, -1, LANES)
        return jnp.sum(exchange(half, ("slab",), False, ident + 1), axis=0).reshape(
            groups, kx, LANES
        )

    def joined(piece, ident):
        half = exchange(piece, ("slab",), True, ident)
        return exchange(half, ("mode",), True, ident + 1).reshape((owners,) + piece.shape)

    spectra = spread(
        pl.pallas_call(
            spectrum_kernel,
            grid=grid,
            in_specs=[cells] + [whole(t) for t in forward],
            out_specs=freq_cells,
            out_shape=freq_field,
            compiler_params=params,
            name="spectrum",
        )(source_field, *forward),
        0,
    )

    weight = spectral_weight.transpose(0, 2, 3, 4, 1)
    limit = width_limit.reshape(1, outs)
    in_block = block
    w_spec = pl.BlockSpec((in_block, freqs, 2, kx, outs), lambda i: (i, 0, 0, 0, 0))
    s_spec = pl.BlockSpec((1, kx, LANES), lambda i: (i, 0, 0))
    mode_spec = pl.BlockSpec((freqs, 2, kx, outs), lambda i: (0, 0, 0, 0))
    limit_spec = pl.BlockSpec((1, outs), lambda i: (0, 0))
    partial_modes = pl.pallas_call(
        contract_kernel,
        grid=(channels // in_block,),
        in_specs=[w_spec, s_spec, limit_spec],
        out_specs=mode_spec,
        out_shape=jax.ShapeDtypeStruct((freqs, 2, kx, outs), jnp.float32),
        compiler_params=params,
        name="contract",
    )(weight, spectra, limit)
    halves = partial_modes.reshape(freqs, 2, kx, chans, groups, block)
    halves = halves.transpose(3, 4, 2, 5, 1, 0).reshape(chans, groups, kx, LANES)
    summed_modes = jnp.sum(exchange(halves, ("chan",), False, 2), axis=0)

    col_freq = mode_index * freqs + jnp.arange(freqs, dtype=jnp.int32)
    row_freq = slab_index * kx + jnp.arange(kx, dtype=jnp.int32)
    limit_rows = lax.dynamic_slice_in_dim(mode_limit, chan_index * channels, channels, 0)
    weights = mode_weights(limit_rows, col_freq, row_freq, all_kx, all_rows * all_cols)
    weights = jnp.broadcast_to(weights, (channels, kx, 2, freqs))
    weights = weights.reshape(groups, block, kx, 2 * freqs).transpose(0, 2, 1, 3)
    weights = weights.reshape(groups, kx, LANES)
    out_modes = joined(summed_modes * weights, 3)

    output, grad_sum, grad_partial, sums = pl.pallas_call(
        functools.partial(middle_kernel, modes),
        grid=grid,
        in_specs=[cells, cells, freq_cells, per_channel, per_channel]
        + [whole(t) for t in forward + back],
        out_specs=[cells, cells, freq_cells, per_channel],
        out_shape=[
            field,
            field,
            freq_field,
            jax.ShapeDtypeStruct((channels, 1, LANES), jnp.float32),
        ],
        compiler_params=params,
        name="middle",
    )(source_field, cotangent, out_modes, gain, wide(channel_bias), *forward, *back)

    grad_modes = spread(grad_partial, 5) * weights
    all_grads = exchange(grad_modes, ("chan",), True, 7)
    all_grads = all_grads.reshape(chans, groups, kx, block, 2, freqs)
    all_grads = all_grads.transpose(5, 4, 2, 0, 1, 3).reshape(freqs, 2, kx, outs)
    weight_grad, back_modes = pl.pallas_call(
        back_kernel,
        grid=(channels // in_block,),
        in_specs=[w_spec, s_spec, mode_spec, limit_spec],
        out_specs=[w_spec, s_spec],
        out_shape=[
            jax.ShapeDtypeStruct(weight.shape, jnp.float32),
            jax.ShapeDtypeStruct(spectra.shape, jnp.float32),
        ],
        compiler_params=params,
        name="back",
    )(weight, spectra, all_grads, limit)
    spectral_grad = weight_grad.transpose(0, 4, 1, 2, 3)

    sent = back_modes.size // LANES
    row_sums = sums[:, 0, :2].T.reshape(-1)
    extra = -(-row_sums.size // (8 * LANES)) * 8
    row_sums = jnp.pad(row_sums, (0, extra * LANES - row_sums.size)).reshape(extra, LANES)
    packed = jnp.concatenate([back_modes.reshape(sent, LANES), row_sums], axis=0)
    parts = joined(packed, 8)
    field_modes = parts[:, :sent].reshape(owners, groups, kx, LANES)
    totals = jnp.sum(parts[:, sent:], axis=0).reshape(-1)
    gate_grad = totals[:channels]
    bias_grad = totals[channels : 2 * channels]
    field_grad = pl.pallas_call(
        functools.partial(last_kernel, modes),
        grid=grid,
        in_specs=[cells, freq_cells, per_channel] + [whole(t) for t in back],
        out_specs=cells,
        out_shape=field,
        compiler_params=params,
        name="last",
    )(grad_sum, field_modes, gain, *back)
    return (output, field_grad, spectral_grad, gate_grad, bias_grad)


def halves_of(table):
    table = table.astype(np.float32)
    high = table.astype(ml_dtypes.bfloat16)
    low = (table - high.astype(np.float32)).astype(ml_dtypes.bfloat16)
    return high, low


def packed_tables(all_rows, all_cols, slabs, modes, freqs, kx_all):
    cell = np.arange(all_cols)[:, None]
    angle = (cell * np.arange(modes * freqs)[None, :] % all_cols) * (2.0 * np.pi / all_cols)
    parts = np.stack([np.cos(angle), -np.sin(angle)], axis=1).reshape(modes, -1, 2, modes, freqs)
    parts = parts.transpose(0, 1, 3, 2, 4)
    cols = parts.shape[1]
    high, low = halves_of(parts)
    ahead = np.stack([high, low], axis=3).reshape(modes, cols, -1)
    flat_high = high.reshape(modes, cols, -1).transpose(0, 2, 1)
    flat_low = low.reshape(modes, cols, -1).transpose(0, 2, 1)
    behind = np.concatenate([flat_high, flat_low], axis=1)
    wave = np.arange(kx_all)
    wave = wave + np.where(2 * wave >= kx_all, all_rows - kx_all, 0)
    angle = (np.arange(all_rows)[:, None] * wave[None, :] % all_rows) * (2.0 * np.pi / all_rows)
    table = np.concatenate([np.cos(angle), np.sin(angle)], axis=1).reshape(slabs, -1, 2 * kx_all)
    high, low = halves_of(table)
    row_behind = np.concatenate([high, low], axis=2)
    high, low = high.transpose(0, 2, 1), low.transpose(0, 2, 1)
    row_ahead = np.concatenate([high, low], axis=2)
    return ahead, row_ahead, row_behind, behind


def lane_roll(values, shift):
    shift = shift % values.shape[-1]
    return values if shift == 0 else pltpu.roll(values, shift, values.ndim - 1)


def lanes_of(shape):
    return lax.broadcasted_iota(jnp.int32, shape, len(shape) - 1)


def high_low(values):
    high = values.astype(jnp.bfloat16)
    return high, (values - high.astype(jnp.float32)).astype(jnp.bfloat16)


def quarter_turn(values, span, sign):
    half = span // 2
    first = lanes_of(values.shape) % span < half
    back, ahead = lane_roll(values, -half), lane_roll(values, half)
    return jnp.where(first, -back, ahead) if sign > 0 else jnp.where(first, back, -ahead)


def three_way(row_table, values):
    high, low = high_low(values)
    width = row_table.shape[1] // 2
    left = jnp.concatenate([row_table, row_table[:, :width]], axis=1)
    right = jnp.concatenate([high, high, low], axis=0)
    return jnp.dot(left, right, preferred_element_type=jnp.float32)


def two_way(values, table):
    high, low = high_low(values)
    both = jnp.concatenate([high, low], axis=1)
    return jnp.dot(both, jnp.concatenate([table, table], axis=0), preferred_element_type=jnp.float32)


def mix_rows(lines_ref, row_table, rows, span, kx, store):
    block = LANES // span
    mixed = []
    for c in range(0, block, 2):
        pair = [lines_ref[(c + k) * rows : (c + k + 1) * rows] for k in range(2)]
        both = three_way(row_table, jnp.concatenate(pair, axis=1))
        mixed += [both[:, :LANES], both[:, LANES:]]
    lane = lanes_of(mixed[0].shape)
    pairs = []
    for c in range(0, block, 2):
        left = mixed[c] + lane_roll(mixed[c], -span)
        right = mixed[c + 1] + lane_roll(mixed[c + 1], span)
        pairs.append(jnp.where(lane % (2 * span) < span, left, right))
    low_half = lane < LANES // 2
    owners = [
        jnp.where(low_half, pairs[0], lane_roll(pairs[1], LANES // 2)),
        jnp.where(low_half, lane_roll(pairs[0], LANES // 2), pairs[1]),
    ]
    all_kx = owners[0].shape[0] // 2
    slabs = all_kx // kx
    for m, values in enumerate(owners):
        done = values[:all_kx] + quarter_turn(values[all_kx:], span, -1)
        for s in range(slabs):
            store(m * slabs + s, done[s * kx : (s + 1) * kx])


def group_lines(modes_ref, group, kx, row_table, span):
    block = LANES // span
    owners = modes_ref.shape[0]
    half = owners // 2
    here = pl.ds(pl.multiple_of(group * kx, kx), kx)
    stack = []
    for m in range(2):
        stack.append(jnp.concatenate([modes_ref[m * half + s, here] for s in range(half)], axis=0))
    full = [jnp.concatenate([one, quarter_turn(one, span, 1)], axis=0) for one in stack]
    rolled = [[lane_roll(one, k * span) for k in range(block)] for one in full]
    lane = lanes_of(full[0].shape)
    even = lane % (2 * span) < span
    low_half = lane < LANES // 2
    sides = []
    for c in range(block):
        first = jnp.where(low_half, rolled[0][(0 - c) % block], rolled[0][(2 - c) % block])
        second = jnp.where(low_half, rolled[1][(1 - c) % block], rolled[1][(3 - c) % block])
        sides.append(jnp.where(even, first, second))
    lines = []
    for c in range(0, block, 2):
        both = three_way(row_table, jnp.concatenate([sides[c], sides[c + 1]], axis=1))
        lines += [both[:, :LANES], both[:, LANES:]]
    return lines


def middle_packed(
    span, kx, x_ref, cot_ref, modes_ref, gain_ref, bias_ref, ahead_ref, row_ref, row_back_ref, behind_ref,
    out_ref, grad_ref, spec_ref, sums_ref, split_ref, lines_ref, branch_ref, next_ref, held_ref, made_ref,
):
    block, rows, cols = cot_ref.shape
    step = pl.program_id(0)
    scale = math.sqrt(2.0 / math.pi)
    row_table = row_ref[0]

    @pl.when(step == 0)
    def _():
        sums_ref[...] = jnp.zeros_like(sums_ref)

    def ahead(c):
        here = slice(c * rows, (c + 2) * rows)
        table = ahead_ref[0]
        high = jnp.dot(split_ref[here, :cols], table, preferred_element_type=jnp.float32)
        lines_ref[here] = high + jnp.dot(split_ref[here, cols:], table, preferred_element_type=jnp.float32)

    def finish(from_ref, group):
        def store(owner, values):
            spec_ref[owner, pl.ds(pl.multiple_of(group * kx, kx), kx)] = values
        mix_rows(from_ref, row_table, rows, span, kx, store)

    lane = lanes_of(sums_ref.shape)
    line = lax.broadcasted_iota(jnp.int32, sums_ref.shape, 0)

    def cell(c, lines):
        channel = step * block + c
        gain, shift = gain_ref[channel], bias_ref[channel]
        branch_ref[c] = two_way(lines, behind_ref[0])
        gate = jnp.zeros((8, cols), jnp.float32)
        bias = jnp.zeros((8, cols), jnp.float32)
        for r in range(0, rows, 16):
            here = slice(r, r + 16)
            source = x_ref[channel, here]
            v = branch_ref[c, here] + (gain * source + shift)
            square = v * v
            inner = v * (scale + (scale * 0.044715) * square)
            up = 0.5 + 0.5 * jnp.tanh(inner)
            out_ref[c, here] = v * up
            bend = v * (2.0 * scale + (6.0 * scale * 0.044715) * square)
            grad = cot_ref[c, here] * (up + (up * (1.0 - up)) * bend)
            grad_ref[channel, here] = grad
            high, low = high_low(grad)
            there = slice(c * rows + r, c * rows + r + 16)
            split_ref[there, :cols] = high
            split_ref[there, cols:] = low
            both = grad * source
            gate = gate + (both[:8] + both[8:])
            bias = bias + (grad[:8] + grad[8:])
        gate = jnp.sum(jnp.sum(gate, axis=0, keepdims=True), axis=1, keepdims=True)
        bias = jnp.sum(jnp.sum(bias, axis=0, keepdims=True), axis=1, keepdims=True)
        here = (lane == channel) & (line < 2)
        sums_ref[...] = jnp.where(here, jnp.where(line == 0, gate, bias), sums_ref[...])

    def prepare(group):
        for c, lines in enumerate(group_lines(modes_ref, group, kx, row_back_ref[0], span)):
            next_ref[c] = lines

    @pl.when(step == 0)
    def _():
        prepare(0)

    held_ref[...] = next_ref[...]
    made_ref[...] = lines_ref[...]
    for c in range(block):
        if c % 2 == 0:
            ahead(c)
        cell(c, held_ref[c])
        if c == 0:
            finish(made_ref, jnp.maximum(step - 2, 0))
        if c == 1:
            prepare(jnp.minimum(step + 1, pl.num_programs(0) - 1))

    @pl.when(step == pl.num_programs(0) - 1)
    def _():
        finish(lines_ref, step - 1)
        for c in range(0, block, 2):
            ahead(c)
        finish(lines_ref, step)


def last_packed(
    span, kx, grad_ref, modes_ref, gain_ref, row_back_ref, behind_ref, grads_ref, spec_ref, limit_ref, out_ref, wgrad_ref
):
    block = out_ref.shape[0]
    step = pl.program_id(0)
    lines = group_lines(modes_ref, step, kx, row_back_ref[0], span)
    count, freqs, outs = wgrad_ref.shape[0], wgrad_ref.shape[1], wgrad_ref.shape[4]
    wide = freqs * kx
    first = lax.axis_index("chan") * (count * pl.num_programs(0)) + step * count
    g_real, g_imag = both_parts(grads_ref, slice(None))
    limit = column_of(limit_ref[...], outs, 0)
    for i in range(count):
        keep = jnp.broadcast_to(limit, (outs, wide)) > (first + i).astype(jnp.float32)
        s_real, s_imag = both_parts(spec_ref, pl.ds(step * count + i, 1))
        real = jnp.where(keep, s_real * g_real + s_imag * g_imag, 0.0)
        imag = jnp.where(keep, s_real * g_imag - s_imag * g_real, 0.0)
        wgrad_ref[i, :, 0] = real.T.reshape(freqs, kx, outs)
        wgrad_ref[i, :, 1] = imag.T.reshape(freqs, kx, outs)
    for c in range(block):
        out_ref[c] = two_way(lines[c], behind_ref[0]) + gain_ref[step * block + c] * grad_ref[step * block + c]


def swap_groups(values, kx):
    lane = lanes_of(values.shape) // kx
    line = lax.broadcasted_iota(jnp.int32, values.shape, 1)
    count = values.shape[1]
    hop = 1
    while hop < count:
        up = lane_roll(pltpu.roll(values, count - hop, 1), hop * kx)
        down = lane_roll(pltpu.roll(values, hop, 1), -hop * kx)
        lane_bit, line_bit = lane // hop % 2, line // hop % 2
        values = jnp.where(lane_bit == line_bit, values, jnp.where(lane_bit == 1, up, down))
        hop *= 2
    return values


def to_lanes(packed, out_ref, kx):
    lines = swap_groups(packed.T.reshape(-1, 8, LANES), kx)
    wide = out_ref.shape[0]
    block = lines.shape[0] // wide
    for c in range(block):
        for j in range(wide):
            out_ref[j, pl.ds(c, 8, stride=block)] = lines[c * wide + j]


def to_rows(wide_ref, block, kx):
    wide = wide_ref.shape[0]
    pieces = []
    for c in range(block):
        for j in range(wide):
            pieces.append(wide_ref[j, pl.ds(c, 8, stride=block)][None])
    return swap_groups(jnp.concatenate(pieces, axis=0), kx).reshape(-1, LANES).T


def both_parts(ref, rows):
    half = ref.shape[0] // 2
    parts = [jnp.concatenate([ref[p * half + j, rows] for j in range(half)], axis=1) for p in range(2)]
    return parts[0], parts[1]


def put_part(ref, rows, part, values):
    half = ref.shape[0] // 2
    for j in range(half):
        ref[part * half + j, rows] = values[:, j * LANES : (j + 1) * LANES]


def other(axis, step, size):
    return lax.rem(lax.axis_index(axis) + step, size)


def send(source, target, sends, recvs, axis, peer):
    copy = pltpu.make_async_remote_copy(
        src_ref=source, dst_ref=target, send_sem=sends, recv_sem=recvs,
        device_id={axis: peer}, device_id_type=pl.DeviceIdType.MESH,
    )
    copy.start()
    return copy


def column_of(row, count, first):
    shape = (count, row.shape[1])
    hit = lanes_of(shape) == first + lax.broadcasted_iota(jnp.int32, shape, 0)
    return jnp.sum(jnp.where(hit, row.astype(jnp.float32), 0.0), axis=1, keepdims=True)


def mode_scales(limit_ref, shape, kx, cells_total):
    wide, count, _ = shape
    first = lax.axis_index("chan") * count
    cols = jnp.broadcast_to(column_of(limit_ref[0:1], count, first), (count, LANES))
    rows = jnp.broadcast_to(column_of(limit_ref[1:2], count, first), (count, LANES))
    all_kx = (kx * lax.axis_size("slab"))
    tiles = []
    for j in range(wide):
        cell = lanes_of((count, LANES)) + j * LANES
        col = (lax.axis_index("mode") * (wide * LANES // kx) + cell // kx).astype(jnp.float32)
        row = (lax.axis_index("slab") * kx + cell % kx).astype(jnp.float32)
        kept = (col < cols) & ((row < rows) | (all_kx - row < rows))
        scale = jnp.where(col < 0.5, 1.0, 2.0) / cells_total
        tiles.append(jnp.where(kept, scale, 0.0)[None])
    return jnp.concatenate(tiles, axis=0)


def greet(slabs):
    barrier = pltpu.get_barrier_semaphore()
    targets = [("mode", 1, 2), ("chan", 1, 2)] + [("slab", step, slabs) for step in range(1, slabs)]
    for axis, step, size in targets:
        pl.semaphore_signal(
            barrier, inc=1, device_id={axis: other(axis, step, size)}, device_id_type=pl.DeviceIdType.MESH
        )
    pl.semaphore_wait(barrier, len(targets))


def scatter_sum(part_ref, half_ref, give_ref, take_ref, mode_sems, slab_sems, slabs, between):
    me_mode, me_slab = lax.axis_index("mode"), lax.axis_index("slab")
    peer = other("mode", 1, 2)
    order = [slabs // 2] + [step for step in range(1, slabs) if step != slabs // 2] + [0]
    copies = []
    for step in order:
        slab = other("slab", step, slabs)
        copies.append(send(
            part_ref.at[peer * slabs + slab], half_ref.at[step], mode_sems.at[0, step], mode_sems.at[1, step], "mode", peer
        ))
    waits = list(copies)
    out = []
    for step, copy in zip(order, copies):
        copy.wait_recv()
        slab = other("slab", step, slabs)
        total = part_ref[me_mode * slabs + slab] + half_ref[step]
        if step == 0:
            mine = total
        else:
            give_ref[step] = total
            out.append(send(
                give_ref.at[step], take_ref.at[step], slab_sems.at[0, step], slab_sems.at[1, step], "slab", slab
            ))
    between()
    for copy in out:
        copy.wait_recv()
    for step in range(1, slabs):
        mine = mine + take_ref[step]
    return mine, [copy.wait_send for copy in copies + out]


def gather_start(own_ref, out_ref, mode_sems, slab_sems, slabs):
    me = lax.axis_index("mode") * slabs + lax.axis_index("slab")
    copies = []
    for step in [slabs // 2] + [step for step in range(1, slabs) if step != slabs // 2]:
        copies.append(send(
            own_ref, out_ref.at[me], slab_sems.at[0, step], slab_sems.at[1, step], "slab", other("slab", step, slabs)
        ))
    near = send(own_ref, out_ref.at[me], mode_sems.at[0, 0], mode_sems.at[1, 0], "mode", other("mode", 1, 2))
    out_ref[me] = own_ref[...]
    return copies, near


def gather_finish(state, out_ref, mode_sems, slabs, between):
    copies, near = state
    relays = []
    order = [slabs // 2] + [step for step in range(1, slabs) if step != slabs // 2]
    for k in list(range(1, slabs - 1)) + [0]:
        between(k)
        copies[k].wait_recv()
        step = order[k]
        source = lax.axis_index("mode") * slabs + other("slab", slabs - step, slabs)
        relays.append(send(
            out_ref.at[source], out_ref.at[source], mode_sems.at[0, step], mode_sems.at[1, step], "mode", other("mode", 1, 2)
        ))
    near.wait()
    for copy in relays:
        copy.wait()
    for copy in copies:
        copy.wait_send()


def forward_kernel(
    span, slabs, kx, x_ref, ahead_ref, row_ref, w_ref, limit_ref, mode_limit_ref, out_ref, turned_ref, spec_ref, x_buf, kept_ref,
    part_ref, half_ref, give_ref, take_ref, w_buf, t_buf, sum_ref, peer_ref, own_ref, lines_ref, ahead_buf, row_buf,
    mode_a, slab_a, mode_b, slab_b, chan_sems, x_sems, w_sems, table_sems, t_sems,
):
    ins, freqs, outs = w_ref.shape[0], w_ref.shape[1], w_ref.shape[4]
    rows, cols = x_ref.shape[1:]
    block = LANES // span
    groups = ins // block
    mine_outs = outs // 2
    wide = freqs * kx
    me_mode, me_slab = lax.axis_index("mode"), lax.axis_index("slab")
    peer_mode = other("mode", 1, 2)
    first = lax.axis_index("chan") * ins
    tables = [
        pltpu.make_async_copy(ahead_ref.at[me_mode], ahead_buf, table_sems.at[0]),
        pltpu.make_async_copy(row_ref.at[me_slab], row_buf, table_sems.at[1]),
    ]
    tables[0].start()

    def x_copy(k):
        here = pl.ds(k * (block // 2), block // 2)
        return pltpu.make_async_copy(x_ref.at[here], x_buf.at[here], x_sems.at[k])

    def w_copy(g):
        here = pl.ds(g * block, block)
        return pltpu.make_async_copy(w_ref.at[here], w_buf.at[here], w_sems.at[g])

    for g in range(2):
        x_copy(2 * g).start()
        x_copy(2 * g + 1).start()
        if g == 0:
            tables[1].start()
    greet(slabs)

    def t_copy(g):
        here = pl.ds(g * block, block)
        return pltpu.make_async_copy(t_buf.at[here], turned_ref.at[here], t_sems.at[g])

    def place(g):
        return pl.ds(pl.multiple_of(g * kx, kx), kx)

    def mode_copy(g):
        return pltpu.make_async_remote_copy(
            src_ref=part_ref.at[pl.ds(peer_mode * slabs, slabs), place(g)], dst_ref=half_ref.at[:, place(g)],
            send_sem=mode_a.at[0, g], recv_sem=mode_a.at[1, g],
            device_id={"mode": peer_mode}, device_id_type=pl.DeviceIdType.MESH,
        )

    def slab_copy(step, g):
        return pltpu.make_async_remote_copy(
            src_ref=give_ref.at[step, place(g)], dst_ref=take_ref.at[step, place(g)],
            send_sem=slab_a.at[0, step, g], recv_sem=slab_a.at[1, step, g],
            device_id={"slab": other("slab", step, slabs)}, device_id_type=pl.DeviceIdType.MESH,
        )

    def ahead(g):
        x_copy(2 * g).wait()
        x_copy(2 * g + 1).wait()

        @pl.when(g + 2 < groups)
        def _():
            x_copy(2 * g + 4).start()
            x_copy(2 * g + 5).start()

        @pl.when(g + 2 >= groups)
        def _():
            for k in range(groups // 2):
                w_copy((g + 2 - groups) * (groups // 2) + k).start()
        values = x_buf[pl.ds(g * block, block)].reshape(block * rows, cols)
        lines_ref[...] = two_way(values, ahead_buf[...])

    def finish(g):
        def store(owner, values):
            part_ref[owner, place(g)] = values
        mix_rows(lines_ref, row_buf[...], rows, span, kx, store)

    limit = column_of(limit_ref[...], outs, 0)

    def flip(g):
        for k in range(block):
            i = g * block + k
            keep = jnp.broadcast_to(limit, (outs, wide)) > (first + i).astype(jnp.float32)
            for p in range(2):
                turned = w_buf[i, :, p].reshape(wide, outs).T
                t_buf[i, :, p * wide : (p + 1) * wide] = jnp.where(keep, turned, 0.0)

    def pass_on(g):
        mode_copy(g).wait_recv()
        for step in [slabs // 2] + [step for step in range(1, slabs) if step != slabs // 2]:
            slab = other("slab", step, slabs)
            give_ref[step, place(g)] = part_ref[me_mode * slabs + slab, place(g)] + half_ref[slab, place(g)]
            slab_copy(step, g).start()

    for table in tables:
        table.wait()
    ahead(0)

    def body(g, carry):
        finish(g - 1)
        ahead(g)
        mode_copy(g - 1).start()

        @pl.when(g > 1)
        def _():
            pass_on(g - 2)
        return carry

    lax.fori_loop(1, groups, body, 0)
    finish(groups - 1)
    mode_copy(groups - 1).start()
    pass_on(groups - 2)
    pass_on(groups - 1)
    kept_ref[...] = mode_scales(mode_limit_ref, kept_ref.shape, kx, slabs * rows * 2 * cols)

    def turn_over(g, carry):
        w_copy(g).wait()
        flip(g)
        t_copy(g).start()
        return carry
    lax.fori_loop(0, groups, turn_over, 0)
    mine = part_ref[me_mode * slabs + me_slab] + half_ref[me_slab]

    def landed(g, carry):
        for step in range(1, slabs):
            slab_copy(step, g).wait_recv()
        return carry
    lax.fori_loop(0, groups, landed, 0)
    for step in range(1, slabs):
        mine = mine + take_ref[step]
    to_lanes(mine, spec_ref, kx)

    def contract(i, carry):
        real, imag = carry
        w_real, w_imag = t_buf[i, :, :wide], t_buf[i, :, wide:]
        s_real, s_imag = both_parts(spec_ref, pl.ds(i, 1))
        return real + (s_real * w_real - s_imag * w_imag), imag + (s_real * w_imag + s_imag * w_real)

    zero = jnp.zeros((outs, wide), jnp.float32)
    real, imag = lax.fori_loop(0, ins, contract, (zero, zero))
    put_part(sum_ref, slice(None), 0, real)
    put_part(sum_ref, slice(None), 1, imag)
    theirs = other("chan", 1, 2) * mine_outs
    swap = send(
        sum_ref.at[:, pl.ds(theirs, mine_outs)], peer_ref, chan_sems.at[0], chan_sems.at[1], "chan", other("chan", 1, 2)
    )
    swap.wait_recv()
    for j in range(peer_ref.shape[0]):
        peer_ref[j] = (sum_ref[j, pl.ds(first, mine_outs)] + peer_ref[j]) * kept_ref[j % kept_ref.shape[0]]
    own_ref[...] = to_rows(peer_ref, mine_outs // 8, kx)
    state = gather_start(own_ref, out_ref, mode_b, slab_b, slabs)
    gather_finish(state, out_ref, mode_b, slabs, lambda k: None)
    swap.wait_send()

    def settle(g, carry):
        t_copy(g).wait()
        mode_copy(g).wait_send()
        for step in range(1, slabs):
            slab_copy(step, g).wait_send()
        return carry
    lax.fori_loop(0, groups, settle, 0)


def backward_kernel(
    slabs, kx, part_ref, sums_ref, turned_ref, weight_ref, out_ref, grad_ref, total_ref,
    half_ref, give_ref, take_ref, t_buf, back_ref, own_ref, near_ref, far_ref, pass_ref,
    mode_a, slab_a, mode_b, slab_b, chan_sems, sum_mode, sum_slab, t_sem,
):
    ins, outs, wide = t_buf.shape[0], t_buf.shape[1], t_buf.shape[2] // 2
    mine_outs = outs // 2
    load = pltpu.make_async_copy(turned_ref, t_buf, t_sem)
    load.start()
    greet(slabs)
    first = lax.axis_index("chan") * ins
    near = send(sums_ref, near_ref, sum_mode.at[0], sum_mode.at[1], "mode", other("mode", 1, 2))

    far = []
    def total_up():
        near.wait_recv()
        pass_ref[...] = sums_ref[...] + near_ref[...]
        for step in range(1, slabs):
            far.append(send(
                pass_ref, far_ref.at[step], sum_slab.at[0, step], sum_slab.at[1, step], "slab", other("slab", step, slabs)
            ))

    mine, sent = scatter_sum(part_ref, half_ref, give_ref, take_ref, mode_a, slab_a, slabs, total_up)
    to_lanes(mine, back_ref, kx)
    here = pl.ds(first, mine_outs)
    for j in range(back_ref.shape[0]):
        grad_ref[j, here] = back_ref[j] * weight_ref[j % weight_ref.shape[0]]
    swap = send(
        grad_ref.at[:, here], grad_ref.at[:, here], chan_sems.at[0], chan_sems.at[1], "chan", other("chan", 1, 2)
    )
    load.wait()
    swap.wait_recv()

    def pull(i, carry):
        w_real, w_imag = t_buf[i, :, :wide], t_buf[i, :, wide:]
        g_real, g_imag = both_parts(grad_ref, slice(None))
        put_part(back_ref, pl.ds(i, 1), 0, jnp.sum(g_real * w_real + g_imag * w_imag, axis=0, keepdims=True))
        put_part(back_ref, pl.ds(i, 1), 1, jnp.sum(g_imag * w_real - g_real * w_imag, axis=0, keepdims=True))
        return carry
    lax.fori_loop(0, ins, pull, 0)
    own_ref[...] = to_rows(back_ref, ins // 8, kx)
    state = gather_start(own_ref, out_ref, mode_b, slab_b, slabs)
    gather_finish(state, out_ref, mode_b, slabs, lambda k: None)
    total = pass_ref[...]
    for step, copy in zip(range(1, slabs), far):
        copy.wait()
        total = total + far_ref[step]
    total_ref[...] = total
    near.wait_send()
    swap.wait_send()
    for wait in sent:
        wait()


def fits(shapes, mesh_sizes):
    channels, rows, cols = shapes[0]
    outs, freqs, kx = shapes[2][1], shapes[2][2], shapes[2][4]
    slabs, modes, chans = mesh_sizes
    return (
        modes == 2 and chans == 2 and slabs > 2 and slabs % 2 == 0
        and 8 * kx == LANES and 8 * freqs == LANES and 2 * freqs * channels == 8 * LANES
        and outs == chans * channels
        and rows % LANES == 0 and cols % LANES == 0
    )


def local(source_field, cotangent, spectral_weight, skip_gain, channel_bias, mode_limit, width_limit):
    slabs, modes, chans = (lax.axis_size(axis) for axis in ("slab", "mode", "chan"))
    args = (source_field, cotangent, spectral_weight, skip_gain, channel_bias, mode_limit, width_limit)
    if not fits([one.shape for one in args], (slabs, modes, chans)):
        return local_plain(*args)
    channels, rows, cols = source_field.shape
    outs, freqs, kx = spectral_weight.shape[1], spectral_weight.shape[2], spectral_weight.shape[4]
    span = 2 * freqs
    block = LANES // span
    groups = channels // block
    owners = slabs * modes
    all_kx, all_rows, all_cols = kx * slabs, rows * slabs, cols * modes
    wide = freqs * kx
    ahead, row_ahead, row_behind, behind = (
        jnp.asarray(t) for t in packed_tables(all_rows, all_cols, slabs, modes, freqs, all_kx)
    )

    def pick(table, axis):
        return pl.BlockSpec((1,) + table.shape[1:], lambda g: (lax.axis_index(axis), 0, 0))

    cells = pl.BlockSpec((block, rows, cols), lambda g: (g, 0, 0))
    scalars = pl.BlockSpec(memory_space=pltpu.SMEM)
    field = jax.ShapeDtypeStruct(source_field.shape, jnp.float32)
    room = lambda size: pltpu.CompilerParams(dimension_semantics=("arbitrary",), vmem_limit_bytes=size * MIB)
    f32 = jnp.float32

    weight = spectral_weight.transpose(0, 2, 3, 4, 1)
    limit = width_limit.reshape(1, outs)

    dma, vmem = pltpu.SemaphoreType.DMA, pltpu.VMEM
    in_vmem, anywhere = pl.BlockSpec(memory_space=pltpu.VMEM), pl.BlockSpec(memory_space=pl.ANY)
    piece = (groups * kx, LANES)
    common = [vmem((slabs,) + piece, f32), vmem((slabs,) + piece, f32), vmem((slabs,) + piece, f32)]
    pair = [dma((2, slabs))] * 4
    comm = lambda ident, room: pltpu.CompilerParams(
        collective_id=ident, has_side_effects=True, vmem_limit_bytes=room * MIB
    )
    flat = lambda lines: (2 * wide // LANES, lines, LANES)

    in_hbm = lambda array: pltpu.with_memory_space_constraint(array, pltpu.HBM)
    held = lambda array: pltpu.with_memory_space_constraint(array, pltpu.VMEM)
    modes_shape = (owners,) + piece
    out_modes, turned, spec, source_held, weights = pl.pallas_call(
        functools.partial(forward_kernel, span, slabs, kx),
        in_specs=[anywhere, anywhere, anywhere, anywhere, in_vmem, in_vmem],
        out_specs=[in_vmem, anywhere, in_vmem, in_vmem, in_vmem],
        out_shape=[
            jax.ShapeDtypeStruct(modes_shape, f32), pltpu.HBM((channels, outs, 2 * wide), f32),
            jax.ShapeDtypeStruct(flat(channels), f32), pltpu.VMEM(field.shape, f32),
            jax.ShapeDtypeStruct((wide // LANES, channels, LANES), f32),
        ],
        scratch_shapes=[vmem(modes_shape, f32)] + common + [
            vmem(weight.shape, f32), vmem((channels, outs, 2 * wide), f32), vmem(flat(outs), f32), vmem(flat(outs // 2), f32), vmem(piece, f32),
            vmem((block * rows, LANES), f32), vmem(ahead.shape[1:], jnp.bfloat16), vmem(row_ahead.shape[1:], jnp.bfloat16),
            dma((2, groups)), dma((2, slabs, groups)), dma((2, slabs)), dma((2, slabs)), dma((2,)),
            dma((2 * groups,)), dma((groups,)), dma((2,)), dma((groups,)),
        ],
        compiler_params=comm(20, FORWARD),
        name="forward_modes",
    )(in_hbm(source_field), in_hbm(ahead), in_hbm(row_ahead), in_hbm(weight), limit, mode_limit.T)

    output, grad_sum, grad_partial, sums = pl.pallas_call(
        functools.partial(middle_packed, span, kx),
        grid=(groups,),
        in_specs=[
            in_vmem, cells, in_vmem, scalars, scalars, pick(ahead, "mode"), pick(row_ahead, "slab"),
            pick(row_behind, "slab"), pick(behind, "mode"),
        ],
        out_specs=[cells, in_vmem, in_vmem, in_vmem],
        out_shape=[field, pltpu.VMEM(field.shape, f32), jax.ShapeDtypeStruct(modes_shape, f32), jax.ShapeDtypeStruct((8, LANES), f32)],
        scratch_shapes=[
            vmem((block * rows, 2 * cols), jnp.bfloat16), vmem((block * rows, LANES), f32), vmem((block, rows, cols), f32),
            vmem((block, rows, LANES), f32), vmem((block, rows, LANES), f32), vmem((block * rows, LANES), f32),
        ],
        input_output_aliases={0: 1},
        compiler_params=room(MIDDLE),
        name="middle",
    )(
        held(source_held), cotangent, out_modes, skip_gain, channel_bias,
        ahead, row_ahead, row_behind, behind,
    )

    back_modes, all_grads, totals = pl.pallas_call(
        functools.partial(backward_kernel, slabs, kx),
        in_specs=[in_vmem, in_vmem, anywhere, in_vmem],
        out_specs=[in_vmem] * 3,
        out_shape=[pltpu.HBM(modes_shape, f32), pltpu.HBM(flat(outs), f32), jax.ShapeDtypeStruct((8, LANES), f32)],
        scratch_shapes=common + [
            vmem((channels, outs, 2 * wide), f32), vmem(flat(channels), f32), vmem(piece, f32), vmem((8, LANES), f32),
            vmem((slabs, 8, LANES), f32), vmem((8, LANES), f32),
        ] + pair + [dma((2,)), dma((2,)), dma((2, slabs)), dma],
        compiler_params=comm(21, BACKWARD),
        name="backward_modes",
    )(in_hbm(grad_partial), in_hbm(sums), in_hbm(turned), in_hbm(weights))

    count = channels // groups
    whole = lambda array: pl.BlockSpec(array.shape, lambda g: (0,) * array.ndim)
    field_grad, weight_grad = pl.pallas_call(
        functools.partial(last_packed, span, kx),
        grid=(groups,),
        in_specs=[
            in_vmem, in_vmem, scalars, pick(row_behind, "slab"), pick(behind, "mode"),
            whole(all_grads), whole(spec), whole(limit),
        ],
        out_specs=[cells, pl.BlockSpec((count,) + weight.shape[1:], lambda g: (g, 0, 0, 0, 0))],
        out_shape=[field, jax.ShapeDtypeStruct(weight.shape, f32)],
        compiler_params=room(LAST),
        name="last",
    )(
        pltpu.with_memory_space_constraint(grad_sum, pltpu.VMEM), back_modes, skip_gain,
        row_behind, behind, all_grads, spec, limit,
    )
    spectral_grad = weight_grad.transpose(0, 4, 1, 2, 3)
    return (output, field_grad, spectral_grad, totals[0, :channels], totals[1, :channels])


def solution(mesh):
    in_specs = (
        P(("member", "chan"), "slab", "mode"),
        P(("member", "chan"), "slab", "mode"),
        P(("member", "chan"), None, "mode", None, "slab"),
        P(("member", "chan")),
        P(("member", "chan")),
        P("member", None),
        P("member"),
    )
    out_specs = (
        P(("member", "chan"), "slab", "mode"),
        P(("member", "chan"), "slab", "mode"),
        P(("member", "chan"), None, "mode", None, "slab"),
        P(("member", "chan")),
        P(("member", "chan")),
    )
    return jax.shard_map(local, mesh=mesh, in_specs=in_specs, out_specs=out_specs, check_vma=False)
```

```python
import functools
import math

import jax
import jax.numpy as jnp
import ml_dtypes
import numpy as np
from jax import lax
from jax.experimental import pallas as pl
from jax.experimental.pallas import tpu as pltpu
from jax.sharding import PartitionSpec as P

LANES = 128
BIG = 60 * 1024 * 1024
MIB = 1024 * 1024
CHUNKS = 4
FORWARD, MIDDLE, LAST, BACKWARD = 40, 40, 40, 20


def split_table(table):
    high = lax.reduce_precision(table, 8, 7)
    return high.astype(jnp.bfloat16), (table - high).astype(jnp.bfloat16)


def split_block(values):
    high = values.astype(jnp.bfloat16)
    return high, (values - high.astype(jnp.float32)).astype(jnp.bfloat16)


def dot_pair(left, right):
    left_high, left_low = left
    right_high, right_low = right
    mul = functools.partial(jnp.dot, preferred_element_type=jnp.float32)
    return mul(left_high, right_high) + mul(left_low, right_high) + mul(left_high, right_low)


def tables(extent, waves, first_cell, cell_count):
    cell_index = first_cell + jnp.arange(cell_count, dtype=jnp.int32)
    products = (cell_index[:, None] * waves[None, :] % extent).astype(jnp.float32)
    angles = products * (2.0 * math.pi / extent)
    return jnp.cos(angles), jnp.sin(angles)


def store_spectrum(values, col_pair, row_pair, out_ref):
    block, rows, cols = values.shape
    lines = dot_pair(split_block(values.reshape(block * rows, cols)), col_pair)
    all_kx = row_pair[0].shape[0] // 2
    kx, lanes = out_ref.shape[2:]
    span = lanes // block
    mode_count = lines.shape[1] // span
    slabs = out_ref.shape[0] // mode_count
    done = []
    for c in range(block):
        mixed = dot_pair(row_pair, split_block(lines[c * rows : (c + 1) * rows]))
        done.append(mixed[:all_kx] - turn(mixed[all_kx:], span))
    for m in range(mode_count):
        packed = jnp.concatenate([one[:, m * span : (m + 1) * span] for one in done], axis=1)
        for s in range(slabs):
            out_ref[m * slabs + s, 0] = packed[s * kx : (s + 1) * kx]


def turn(values, span):
    half = span // 2
    pieces = []
    for first in range(0, values.shape[1], span):
        pieces.append(-values[:, first + half : first + span])
        pieces.append(values[:, first : first + half])
    return jnp.concatenate(pieces, axis=1)


def all_modes(modes_ref, mode_count, c, block):
    span = modes_ref.shape[3] // block
    slabs = modes_ref.shape[0] // mode_count
    columns = []
    for m in range(mode_count):
        stack = [modes_ref[m * slabs + s, 0] for s in range(slabs)]
        columns.append(jnp.concatenate(stack, axis=0)[:, c * span : (c + 1) * span])
    return jnp.concatenate(columns, axis=1), span


def synth(modes_and_span, row_pair, col_pair):
    modes, span = modes_and_span
    stacked = jnp.concatenate([modes, turn(modes, span)], axis=0)
    lines = dot_pair(row_pair, split_block(stacked))
    return dot_pair(split_block(lines), col_pair)


def spectrum_kernel(x_ref, ch_ref, cl_ref, rh_ref, rl_ref, out_ref):
    store_spectrum(x_ref[...], (ch_ref[...], cl_ref[...]), (rh_ref[...], rl_ref[...]), out_ref)


def middle_kernel(
    mode_count, x_ref, cot_ref, modes_ref, gain_ref, bias_ref, ch_ref, cl_ref, rh_ref, rl_ref,
    cth_ref, ctl_ref, ih_ref, il_ref, out_ref, grad_ref, spec_ref, sums_ref,
):
    block = x_ref.shape[0]
    row_back = (ih_ref[...], il_ref[...])
    col_back = (cth_ref[...], ctl_ref[...])
    scale = math.sqrt(2.0 / math.pi)
    for c in range(block):
        source = x_ref[c]
        gain = gain_ref[c]
        v = synth(all_modes(modes_ref, mode_count, c, block), row_back, col_back) + gain[:, :1] * source + bias_ref[c][:, :1]
        square = v * v
        t = jnp.tanh(scale * v * (1.0 + 0.044715 * square))
        half_up = 0.5 * (1.0 + t)
        out_ref[c] = v * half_up
        slope = half_up + 0.5 * v * (1.0 - t * t) * (scale * (1.0 + 3.0 * 0.044715 * square))
        grad = cot_ref[c] * slope
        grad_ref[c] = grad
        gate = jnp.sum(jnp.sum(grad * source, axis=0, keepdims=True), axis=1, keepdims=True)
        bias = jnp.sum(jnp.sum(grad, axis=0, keepdims=True), axis=1, keepdims=True)
        lane = lax.broadcasted_iota(jnp.int32, (1, LANES), 1)
        sums_ref[c] = jnp.where(lane == 0, gate, bias)
    store_spectrum(
        grad_ref[...], (ch_ref[...], cl_ref[...]), (rh_ref[...], rl_ref[...]), spec_ref
    )


def last_kernel(mode_count, grad_ref, modes_ref, gain_ref, cth_ref, ctl_ref, ih_ref, il_ref, out_ref):
    block = grad_ref.shape[0]
    for c in range(block):
        modes = all_modes(modes_ref, mode_count, c, block)
        branch = synth(modes, (ih_ref[...], il_ref[...]), (cth_ref[...], ctl_ref[...]))
        out_ref[c] = branch + gain_ref[c][:, :1] * grad_ref[c]


def contract_kernel(w_ref, spec_ref, limit_ref, out_ref):
    block, freqs, _, kx, outs = w_ref.shape
    first = lax.axis_index("chan") * (block * pl.num_programs(0)) + pl.program_id(0) * block

    @pl.when(pl.program_id(0) == 0)
    def _():
        out_ref[...] = jnp.zeros_like(out_ref)

    limit = limit_ref[...]
    for y in range(freqs):
        real = out_ref[y, 0]
        imag = out_ref[y, 1]
        for i in range(block):
            keep = first + i < limit
            spec = spec_ref[0]
            at = 2 * freqs * i + y
            s_real = jnp.where(keep, spec[:, at : at + 1], 0.0)
            s_imag = jnp.where(keep, spec[:, freqs + at : freqs + at + 1], 0.0)
            w_real = w_ref[i, y, 0]
            w_imag = w_ref[i, y, 1]
            real = real + (s_real * w_real - s_imag * w_imag)
            imag = imag + (s_real * w_imag + s_imag * w_real)
        out_ref[y, 0] = real
        out_ref[y, 1] = imag


def back_kernel(w_ref, spec_ref, grads_ref, limit_ref, wgrad_ref, out_ref):
    block, freqs, _, kx, outs = w_ref.shape
    first = lax.axis_index("chan") * (block * pl.num_programs(0)) + pl.program_id(0) * block
    limit = limit_ref[...]
    lane = lax.broadcasted_iota(jnp.int32, out_ref.shape[1:], 1)
    spec = spec_ref[0]
    back = jnp.zeros(out_ref.shape[1:], jnp.float32)
    for i in range(block):
        keep = first + i < limit
        for y in range(freqs):
            at = 2 * freqs * i + y
            g_real = jnp.where(keep, grads_ref[y, 0], 0.0)
            g_imag = jnp.where(keep, grads_ref[y, 1], 0.0)
            s_real = spec[:, at : at + 1]
            s_imag = spec[:, freqs + at : freqs + at + 1]
            wgrad_ref[i, y, 0] = s_real * g_real + s_imag * g_imag
            wgrad_ref[i, y, 1] = s_real * g_imag - s_imag * g_real
            w_real = w_ref[i, y, 0]
            w_imag = w_ref[i, y, 1]
            b_real = jnp.sum(g_real * w_real + g_imag * w_imag, axis=1, keepdims=True)
            b_imag = jnp.sum(g_imag * w_real - g_real * w_imag, axis=1, keepdims=True)
            back = jnp.where(lane == at, b_real, back)
            back = jnp.where(lane == freqs + at, b_imag, back)
    out_ref[0] = back


def exchange_kernel(axes, sizes, gather, x_ref, out_ref, send_sem, recv_sem, own_sem):
    total = math.prod(sizes)
    me = lax.axis_index(axes[0])
    for axis, size in zip(axes[1:], sizes[1:]):
        me = me * size + lax.axis_index(axis)

    def place(index):
        coords = {}
        for axis, size in reversed(list(zip(axes, sizes))):
            coords[axis] = lax.rem(index, size)
            index = lax.div(index, size)
        return coords

    barrier = pltpu.get_barrier_semaphore()
    for step in range(1, total):
        pl.semaphore_signal(
            barrier, inc=1, device_id=place(lax.rem(me + step, total)),
            device_id_type=pl.DeviceIdType.MESH,
        )
    pl.semaphore_wait(barrier, total - 1)
    copies = []
    for step in range(1, total):
        peer = lax.rem(me + step, total)
        copy = pltpu.make_async_remote_copy(
            src_ref=x_ref if gather else x_ref.at[peer],
            dst_ref=out_ref.at[me],
            send_sem=send_sem.at[step],
            recv_sem=recv_sem.at[step],
            device_id=place(peer),
            device_id_type=pl.DeviceIdType.MESH,
        )
        copy.start()
        copies.append(copy)
    own = pltpu.make_async_copy(x_ref if gather else x_ref.at[me], out_ref.at[me], own_sem)
    own.start()
    own.wait()
    for copy in copies:
        copy.wait()


def exchange(values, axes, gather, ident):
    sizes = tuple(lax.axis_size(axis) for axis in axes)
    total = math.prod(sizes)
    piece = values.shape if gather else values.shape[1:]
    flat = values.reshape((-1, LANES) if gather else (total, -1, LANES))
    out = pl.pallas_call(
        functools.partial(exchange_kernel, axes, sizes, gather),
        out_shape=jax.ShapeDtypeStruct((total,) + flat.shape[-2:], jnp.float32),
        in_specs=[pl.BlockSpec(memory_space=pltpu.VMEM)],
        out_specs=pl.BlockSpec(memory_space=pltpu.VMEM),
        scratch_shapes=[
            pltpu.SemaphoreType.DMA((total,)),
            pltpu.SemaphoreType.DMA((total,)),
            pltpu.SemaphoreType.DMA,
        ],
        compiler_params=pltpu.CompilerParams(collective_id=ident, has_side_effects=True),
        name="exchange" + str(ident),
    )(flat)
    return out.reshape((total,) + piece)


def mode_weights(limit_rows, col_freq, row_freq, kx_count, cells_total):
    keep_cols = col_freq[None, :] < limit_rows[:, 0:1]
    keep_rows = (row_freq[None, :] < limit_rows[:, 1:2]) | (
        (kx_count - row_freq)[None, :] < limit_rows[:, 1:2]
    )
    scales = jnp.where(col_freq == 0, 1.0, 2.0).astype(jnp.float32) / cells_total
    joined = keep_rows[:, :, None] & keep_cols[:, None, :]
    return (joined.astype(jnp.float32) * scales[None, None, :])[:, :, None, :]


def local_plain(
    source_field, cotangent, spectral_weight, skip_gain, channel_bias, mode_limit, width_limit
):
    channels, row_count, col_count = source_field.shape
    slabs = lax.axis_size("slab")
    modes = lax.axis_size("mode")
    chans = lax.axis_size("chan")
    slab_index = lax.axis_index("slab")
    mode_index = lax.axis_index("mode")
    chan_index = lax.axis_index("chan")
    outs = spectral_weight.shape[1]
    freqs = spectral_weight.shape[2]
    kx = spectral_weight.shape[4]
    all_freqs = freqs * modes
    all_kx = kx * slabs
    all_rows = row_count * slabs
    all_cols = col_count * modes

    col_waves = jnp.arange(all_freqs, dtype=jnp.int32)
    row_waves = jnp.arange(all_kx, dtype=jnp.int32)
    row_waves = row_waves + jnp.where(2 * row_waves >= all_kx, all_rows - all_kx, 0)
    col_cos, col_sin = tables(all_cols, col_waves, mode_index * col_count, col_count)
    row_cos, row_sin = tables(all_rows, row_waves, slab_index * row_count, row_count)
    col_tab = jnp.stack(
        [col_cos.reshape(-1, modes, freqs), -col_sin.reshape(-1, modes, freqs)], axis=2
    ).reshape(col_count, 2 * all_freqs)
    row_tab = jnp.concatenate([row_cos, row_sin], axis=1)
    col_pair = split_table(col_tab)
    col_back = tuple(part.T for part in col_pair)
    row_back = split_table(row_tab)
    row_pair = tuple(part.T for part in row_back)

    block = LANES // (2 * freqs)
    groups = channels // block
    owners = slabs * modes
    cells = pl.BlockSpec((block, row_count, col_count), lambda c: (c, 0, 0))
    freq_cells = pl.BlockSpec((owners, 1, kx, LANES), lambda c: (0, c, 0, 0))
    per_channel = pl.BlockSpec((block, 1, LANES), lambda c: (c, 0, 0))
    field = jax.ShapeDtypeStruct(source_field.shape, jnp.float32)
    freq_field = jax.ShapeDtypeStruct((owners, groups, kx, LANES), jnp.float32)
    params = pltpu.CompilerParams(
        dimension_semantics=("arbitrary",), vmem_limit_bytes=BIG
    )

    def whole(array):
        return pl.BlockSpec(array.shape, lambda c: (0,) * array.ndim)

    grid = (channels // block,)
    wide = lambda values: jnp.broadcast_to(values[:, None, None], (channels, 1, LANES))
    gain = wide(skip_gain)
    forward = col_pair + row_pair
    back = col_back + row_back

    def spread(partial, ident):
        half = exchange(partial.reshape(modes, -1, LANES), ("mode",), False, ident)
        half = jnp.sum(half, axis=0).reshape(slabs, -1, LANES)
        return jnp.sum(exchange(half, ("slab",), False, ident + 1), axis=0).reshape(
            groups, kx, LANES
        )

    def joined(piece, ident):
        half = exchange(piece, ("slab",), True, ident)
        return exchange(half, ("mode",), True, ident + 1).reshape((owners,) + piece.shape)

    spectra = spread(
        pl.pallas_call(
            spectrum_kernel,
            grid=grid,
            in_specs=[cells] + [whole(t) for t in forward],
            out_specs=freq_cells,
            out_shape=freq_field,
            compiler_params=params,
            name="spectrum",
        )(source_field, *forward),
        0,
    )

    weight = spectral_weight.transpose(0, 2, 3, 4, 1)
    limit = width_limit.reshape(1, outs)
    in_block = block
    w_spec = pl.BlockSpec((in_block, freqs, 2, kx, outs), lambda i: (i, 0, 0, 0, 0))
    s_spec = pl.BlockSpec((1, kx, LANES), lambda i: (i, 0, 0))
    mode_spec = pl.BlockSpec((freqs, 2, kx, outs), lambda i: (0, 0, 0, 0))
    limit_spec = pl.BlockSpec((1, outs), lambda i: (0, 0))
    partial_modes = pl.pallas_call(
        contract_kernel,
        grid=(channels // in_block,),
        in_specs=[w_spec, s_spec, limit_spec],
        out_specs=mode_spec,
        out_shape=jax.ShapeDtypeStruct((freqs, 2, kx, outs), jnp.float32),
        compiler_params=params,
        name="contract",
    )(weight, spectra, limit)
    halves = partial_modes.reshape(freqs, 2, kx, chans, groups, block)
    halves = halves.transpose(3, 4, 2, 5, 1, 0).reshape(chans, groups, kx, LANES)
    summed_modes = jnp.sum(exchange(halves, ("chan",), False, 2), axis=0)

    col_freq = mode_index * freqs + jnp.arange(freqs, dtype=jnp.int32)
    row_freq = slab_index * kx + jnp.arange(kx, dtype=jnp.int32)
    limit_rows = lax.dynamic_slice_in_dim(mode_limit, chan_index * channels, channels, 0)
    weights = mode_weights(limit_rows, col_freq, row_freq, all_kx, all_rows * all_cols)
    weights = jnp.broadcast_to(weights, (channels, kx, 2, freqs))
    weights = weights.reshape(groups, block, kx, 2 * freqs).transpose(0, 2, 1, 3)
    weights = weights.reshape(groups, kx, LANES)
    out_modes = joined(summed_modes * weights, 3)

    output, grad_sum, grad_partial, sums = pl.pallas_call(
        functools.partial(middle_kernel, modes),
        grid=grid,
        in_specs=[cells, cells, freq_cells, per_channel, per_channel]
        + [whole(t) for t in forward + back],
        out_specs=[cells, cells, freq_cells, per_channel],
        out_shape=[
            field,
            field,
            freq_field,
            jax.ShapeDtypeStruct((channels, 1, LANES), jnp.float32),
        ],
        compiler_params=params,
        name="middle",
    )(source_field, cotangent, out_modes, gain, wide(channel_bias), *forward, *back)

    grad_modes = spread(grad_partial, 5) * weights
    all_grads = exchange(grad_modes, ("chan",), True, 7)
    all_grads = all_grads.reshape(chans, groups, kx, block, 2, freqs)
    all_grads = all_grads.transpose(5, 4, 2, 0, 1, 3).reshape(freqs, 2, kx, outs)
    weight_grad, back_modes = pl.pallas_call(
        back_kernel,
        grid=(channels // in_block,),
        in_specs=[w_spec, s_spec, mode_spec, limit_spec],
        out_specs=[w_spec, s_spec],
        out_shape=[
            jax.ShapeDtypeStruct(weight.shape, jnp.float32),
            jax.ShapeDtypeStruct(spectra.shape, jnp.float32),
        ],
        compiler_params=params,
        name="back",
    )(weight, spectra, all_grads, limit)
    spectral_grad = weight_grad.transpose(0, 4, 1, 2, 3)

    sent = back_modes.size // LANES
    row_sums = sums[:, 0, :2].T.reshape(-1)
    extra = -(-row_sums.size // (8 * LANES)) * 8
    row_sums = jnp.pad(row_sums, (0, extra * LANES - row_sums.size)).reshape(extra, LANES)
    packed = jnp.concatenate([back_modes.reshape(sent, LANES), row_sums], axis=0)
    parts = joined(packed, 8)
    field_modes = parts[:, :sent].reshape(owners, groups, kx, LANES)
    totals = jnp.sum(parts[:, sent:], axis=0).reshape(-1)
    gate_grad = totals[:channels]
    bias_grad = totals[channels : 2 * channels]
    field_grad = pl.pallas_call(
        functools.partial(last_kernel, modes),
        grid=grid,
        in_specs=[cells, freq_cells, per_channel] + [whole(t) for t in back],
        out_specs=cells,
        out_shape=field,
        compiler_params=params,
        name="last",
    )(grad_sum, field_modes, gain, *back)
    return (output, field_grad, spectral_grad, gate_grad, bias_grad)


def halves_of(table):
    table = table.astype(np.float32)
    high = table.astype(ml_dtypes.bfloat16)
    low = (table - high.astype(np.float32)).astype(ml_dtypes.bfloat16)
    return high, low


def packed_tables(all_rows, all_cols, slabs, modes, freqs, kx_all):
    cell = np.arange(all_cols)[:, None]
    angle = (cell * np.arange(modes * freqs)[None, :] % all_cols) * (2.0 * np.pi / all_cols)
    parts = np.stack([np.cos(angle), -np.sin(angle)], axis=1).reshape(modes, -1, 2, modes, freqs)
    parts = parts.transpose(0, 1, 3, 2, 4)
    cols = parts.shape[1]
    high, low = halves_of(parts)
    ahead = np.stack([high, low], axis=3).reshape(modes, cols, -1)
    flat_high = high.reshape(modes, cols, -1).transpose(0, 2, 1)
    flat_low = low.reshape(modes, cols, -1).transpose(0, 2, 1)
    behind = np.concatenate([flat_high, flat_low], axis=1)
    wave = np.arange(kx_all)
    wave = wave + np.where(2 * wave >= kx_all, all_rows - kx_all, 0)
    angle = (np.arange(all_rows)[:, None] * wave[None, :] % all_rows) * (2.0 * np.pi / all_rows)
    table = np.concatenate([np.cos(angle), np.sin(angle)], axis=1).reshape(slabs, -1, 2 * kx_all)
    high, low = halves_of(table)
    row_behind = np.concatenate([high, low], axis=2)
    high, low = high.transpose(0, 2, 1), low.transpose(0, 2, 1)
    row_ahead = np.concatenate([high, low], axis=2)
    return ahead, row_ahead, row_behind, behind


def lane_roll(values, shift):
    shift = shift % values.shape[-1]
    return values if shift == 0 else pltpu.roll(values, shift, values.ndim - 1)


def lanes_of(shape):
    return lax.broadcasted_iota(jnp.int32, shape, len(shape) - 1)


def high_low(values):
    high = values.astype(jnp.bfloat16)
    return high, (values - high.astype(jnp.float32)).astype(jnp.bfloat16)


def quarter_turn(values, span, sign):
    half = span // 2
    first = lanes_of(values.shape) % span < half
    back, ahead = lane_roll(values, -half), lane_roll(values, half)
    return jnp.where(first, -back, ahead) if sign > 0 else jnp.where(first, back, -ahead)


def three_way(row_table, values):
    high, low = high_low(values)
    width = row_table.shape[1] // 2
    left = jnp.concatenate([row_table, row_table[:, :width]], axis=1)
    right = jnp.concatenate([high, high, low], axis=0)
    return jnp.dot(left, right, preferred_element_type=jnp.float32)


def two_way(values, table):
    high, low = high_low(values)
    both = jnp.concatenate([high, low], axis=1)
    return jnp.dot(both, jnp.concatenate([table, table], axis=0), preferred_element_type=jnp.float32)


def mix_rows(lines_ref, row_table, rows, span, kx, store):
    block = LANES // span
    mixed = []
    for c in range(0, block, 2):
        pair = [lines_ref[(c + k) * rows : (c + k + 1) * rows] for k in range(2)]
        both = three_way(row_table, jnp.concatenate(pair, axis=1))
        mixed += [both[:, :LANES], both[:, LANES:]]
    lane = lanes_of(mixed[0].shape)
    pairs = []
    for c in range(0, block, 2):
        left = mixed[c] + lane_roll(mixed[c], -span)
        right = mixed[c + 1] + lane_roll(mixed[c + 1], span)
        pairs.append(jnp.where(lane % (2 * span) < span, left, right))
    low_half = lane < LANES // 2
    owners = [
        jnp.where(low_half, pairs[0], lane_roll(pairs[1], LANES // 2)),
        jnp.where(low_half, lane_roll(pairs[0], LANES // 2), pairs[1]),
    ]
    all_kx = owners[0].shape[0] // 2
    slabs = all_kx // kx
    for m, values in enumerate(owners):
        done = values[:all_kx] + quarter_turn(values[all_kx:], span, -1)
        for s in range(slabs):
            store(m * slabs + s, done[s * kx : (s + 1) * kx])


def group_lines(modes_ref, group, kx, row_table, span):
    block = LANES // span
    owners = modes_ref.shape[0]
    half = owners // 2
    here = pl.ds(pl.multiple_of(group * kx, kx), kx)
    stack = []
    for m in range(2):
        stack.append(jnp.concatenate([modes_ref[m * half + s, here] for s in range(half)], axis=0))
    full = [jnp.concatenate([one, quarter_turn(one, span, 1)], axis=0) for one in stack]
    rolled = [[lane_roll(one, k * span) for k in range(block)] for one in full]
    lane = lanes_of(full[0].shape)
    even = lane % (2 * span) < span
    low_half = lane < LANES // 2
    sides = []
    for c in range(block):
        first = jnp.where(low_half, rolled[0][(0 - c) % block], rolled[0][(2 - c) % block])
        second = jnp.where(low_half, rolled[1][(1 - c) % block], rolled[1][(3 - c) % block])
        sides.append(jnp.where(even, first, second))
    lines = []
    for c in range(0, block, 2):
        both = three_way(row_table, jnp.concatenate([sides[c], sides[c + 1]], axis=1))
        lines += [both[:, :LANES], both[:, LANES:]]
    return lines


def middle_packed(
    span, kx, x_ref, cot_ref, modes_ref, gain_ref, bias_ref, ahead_ref, row_ref, row_back_ref, behind_ref,
    out_ref, grad_ref, spec_ref, sums_ref, split_ref, lines_ref, branch_ref, next_ref, held_ref, made_ref,
):
    block, rows, cols = cot_ref.shape
    step = pl.program_id(0)
    scale = math.sqrt(2.0 / math.pi)
    row_table = row_ref[0]

    @pl.when(step == 0)
    def _():
        sums_ref[...] = jnp.zeros_like(sums_ref)

    def ahead(c):
        here = slice(c * rows, (c + 2) * rows)
        table = ahead_ref[0]
        high = jnp.dot(split_ref[here, :cols], table, preferred_element_type=jnp.float32)
        lines_ref[here] = high + jnp.dot(split_ref[here, cols:], table, preferred_element_type=jnp.float32)

    def finish(from_ref, group):
        def store(owner, values):
            spec_ref[owner, pl.ds(pl.multiple_of(group * kx, kx), kx)] = values
        mix_rows(from_ref, row_table, rows, span, kx, store)

    lane = lanes_of(sums_ref.shape)
    line = lax.broadcasted_iota(jnp.int32, sums_ref.shape, 0)

    def cell(c, lines):
        channel = step * block + c
        gain, shift = gain_ref[channel], bias_ref[channel]
        branch_ref[c] = two_way(lines, behind_ref[0])
        gate = jnp.zeros((8, cols), jnp.float32)
        bias = jnp.zeros((8, cols), jnp.float32)
        for r in range(0, rows, 16):
            here = slice(r, r + 16)
            source = x_ref[channel, here]
            v = branch_ref[c, here] + (gain * source + shift)
            square = v * v
            inner = v * (scale + (scale * 0.044715) * square)
            up = 0.5 + 0.5 * jnp.tanh(inner)
            out_ref[c, here] = v * up
            bend = v * (2.0 * scale + (6.0 * scale * 0.044715) * square)
            grad = cot_ref[c, here] * (up + (up * (1.0 - up)) * bend)
            grad_ref[channel, here] = grad
            high, low = high_low(grad)
            there = slice(c * rows + r, c * rows + r + 16)
            split_ref[there, :cols] = high
            split_ref[there, cols:] = low
            both = grad * source
            gate = gate + (both[:8] + both[8:])
            bias = bias + (grad[:8] + grad[8:])
        gate = jnp.sum(jnp.sum(gate, axis=0, keepdims=True), axis=1, keepdims=True)
        bias = jnp.sum(jnp.sum(bias, axis=0, keepdims=True), axis=1, keepdims=True)
        here = (lane == channel) & (line < 2)
        sums_ref[...] = jnp.where(here, jnp.where(line == 0, gate, bias), sums_ref[...])

    def prepare(group):
        for c, lines in enumerate(group_lines(modes_ref, group, kx, row_back_ref[0], span)):
            next_ref[c] = lines

    @pl.when(step == 0)
    def _():
        prepare(0)

    held_ref[...] = next_ref[...]
    made_ref[...] = lines_ref[...]
    for c in range(block):
        if c % 2 == 0:
            ahead(c)
        cell(c, held_ref[c])
        if c == 0:
            finish(made_ref, jnp.maximum(step - 2, 0))
        if c == 1:
            prepare(jnp.minimum(step + 1, pl.num_programs(0) - 1))

    @pl.when(step == pl.num_programs(0) - 1)
    def _():
        finish(lines_ref, step - 1)
        for c in range(0, block, 2):
            ahead(c)
        finish(lines_ref, step)


def last_packed(
    span, kx, grad_ref, modes_ref, gain_ref, row_back_ref, behind_ref, grads_ref, spec_ref, limit_ref, total_ref,
    out_ref, wgrad_ref, gate_ref, bias_ref,
):
    block = out_ref.shape[0]
    step = pl.program_id(0)
    lines = group_lines(modes_ref, step, kx, row_back_ref[0], span)
    count, freqs, outs = wgrad_ref.shape[0], wgrad_ref.shape[1], wgrad_ref.shape[4]
    wide = freqs * kx
    first = lax.axis_index("chan") * (count * pl.num_programs(0)) + step * count
    gate_ref[...] = total_ref[0:1, : gate_ref.shape[1]]
    bias_ref[...] = total_ref[1:2, : bias_ref.shape[1]]
    g_real, g_imag = both_parts(grads_ref, slice(None))
    limit = column_of(limit_ref[...], outs, 0)
    for i in range(count):
        keep = jnp.broadcast_to(limit, (outs, wide)) > (first + i).astype(jnp.float32)
        s_real, s_imag = both_parts(spec_ref, pl.ds(step * count + i, 1))
        real = jnp.where(keep, s_real * g_real + s_imag * g_imag, 0.0)
        imag = jnp.where(keep, s_real * g_imag - s_imag * g_real, 0.0)
        wgrad_ref[i, :, 0] = real.T.reshape(freqs, kx, outs)
        wgrad_ref[i, :, 1] = imag.T.reshape(freqs, kx, outs)
    for c in range(block):
        out_ref[c] = two_way(lines[c], behind_ref[0]) + gain_ref[step * block + c] * grad_ref[step * block + c]


def swap_groups(values, kx):
    lane = lanes_of(values.shape) // kx
    line = lax.broadcasted_iota(jnp.int32, values.shape, 1)
    count = values.shape[1]
    hop = 1
    while hop < count:
        up = lane_roll(pltpu.roll(values, count - hop, 1), hop * kx)
        down = lane_roll(pltpu.roll(values, hop, 1), -hop * kx)
        lane_bit, line_bit = lane // hop % 2, line // hop % 2
        values = jnp.where(lane_bit == line_bit, values, jnp.where(lane_bit == 1, up, down))
        hop *= 2
    return values


def to_lanes(packed, out_ref, kx):
    lines = swap_groups(packed.T.reshape(-1, 8, LANES), kx)
    wide = out_ref.shape[0]
    block = lines.shape[0] // wide
    for c in range(block):
        for j in range(wide):
            out_ref[j, pl.ds(c, 8, stride=block)] = lines[c * wide + j]


def to_rows(wide_ref, block, kx):
    wide = wide_ref.shape[0]
    pieces = []
    for c in range(block):
        for j in range(wide):
            pieces.append(wide_ref[j, pl.ds(c, 8, stride=block)][None])
    return swap_groups(jnp.concatenate(pieces, axis=0), kx).reshape(-1, LANES).T


def both_parts(ref, rows):
    half = ref.shape[0] // 2
    parts = [jnp.concatenate([ref[p * half + j, rows] for j in range(half)], axis=1) for p in range(2)]
    return parts[0], parts[1]


def put_part(ref, rows, part, values):
    half = ref.shape[0] // 2
    for j in range(half):
        ref[part * half + j, rows] = values[:, j * LANES : (j + 1) * LANES]


def other(axis, step, size):
    return lax.rem(lax.axis_index(axis) + step, size)


def send(source, target, sends, recvs, axis, peer):
    copy = pltpu.make_async_remote_copy(
        src_ref=source, dst_ref=target, send_sem=sends, recv_sem=recvs,
        device_id={axis: peer}, device_id_type=pl.DeviceIdType.MESH,
    )
    copy.start()
    return copy


def column_of(row, count, first):
    shape = (count, row.shape[1])
    hit = lanes_of(shape) == first + lax.broadcasted_iota(jnp.int32, shape, 0)
    return jnp.sum(jnp.where(hit, row.astype(jnp.float32), 0.0), axis=1, keepdims=True)


def mode_scales(limit_ref, shape, kx, cells_total):
    wide, count, _ = shape
    first = lax.axis_index("chan") * count
    cols = jnp.broadcast_to(column_of(limit_ref[0:1], count, first), (count, LANES))
    rows = jnp.broadcast_to(column_of(limit_ref[1:2], count, first), (count, LANES))
    all_kx = (kx * lax.axis_size("slab"))
    tiles = []
    for j in range(wide):
        cell = lanes_of((count, LANES)) + j * LANES
        col = (lax.axis_index("mode") * (wide * LANES // kx) + cell // kx).astype(jnp.float32)
        row = (lax.axis_index("slab") * kx + cell % kx).astype(jnp.float32)
        kept = (col < cols) & ((row < rows) | (all_kx - row < rows))
        scale = jnp.where(col < 0.5, 1.0, 2.0) / cells_total
        tiles.append(jnp.where(kept, scale, 0.0)[None])
    return jnp.concatenate(tiles, axis=0)


def greet(slabs):
    barrier = pltpu.get_barrier_semaphore()
    targets = [("mode", 1, 2), ("chan", 1, 2)] + [("slab", step, slabs) for step in range(1, slabs)]
    for axis, step, size in targets:
        pl.semaphore_signal(
            barrier, inc=1, device_id={axis: other(axis, step, size)}, device_id_type=pl.DeviceIdType.MESH
        )
    pl.semaphore_wait(barrier, len(targets))


def far_first(slabs):
    return [slabs // 2] + [step for step in range(1, slabs) if step != slabs // 2]


def chunk(rows, k):
    size = rows // CHUNKS
    return pl.ds(k * size, size)


def scatter_sum(part_ref, half_ref, give_ref, take_ref, mode_sems, slab_sems, slabs, between):
    me_mode, me_slab = lax.axis_index("mode"), lax.axis_index("slab")
    peer = other("mode", 1, 2)
    rows = part_ref.shape[1]
    copies = []
    for k in range(CHUNKS):
        here = chunk(rows, k)
        copies.append(send(
            part_ref.at[pl.ds(peer * slabs, slabs), here], half_ref.at[:, here],
            mode_sems.at[0, 0, k], mode_sems.at[1, 0, k], "mode", peer,
        ))
    out = []
    for k in range(CHUNKS):
        here = chunk(rows, k)
        copies[k].wait_recv()
        for step in far_first(slabs):
            slab = other("slab", step, slabs)
            give_ref[step, here] = part_ref[me_mode * slabs + slab, here] + half_ref[slab, here]
            out.append(send(
                give_ref.at[step, here], take_ref.at[step, here],
                slab_sems.at[0, step, k], slab_sems.at[1, step, k], "slab", slab,
            ))
    between()
    mine = part_ref[me_mode * slabs + me_slab] + half_ref[me_slab]
    for copy in out:
        copy.wait_recv()
    for step in range(1, slabs):
        mine = mine + take_ref[step]
    return mine, [copy.wait_send for copy in copies + out]


def gather(own_ref, out_ref, mode_sems, slab_sems, slabs):
    me = lax.axis_index("mode") * slabs + lax.axis_index("slab")
    rows = own_ref.shape[0]
    copies, relays = [], []
    for k in range(CHUNKS):
        here = chunk(rows, k)
        for step in far_first(slabs):
            copies.append((step, here, k, send(
                own_ref.at[here], out_ref.at[me, here], slab_sems.at[0, step, k], slab_sems.at[1, step, k],
                "slab", other("slab", step, slabs),
            )))
    near = send(
        own_ref, out_ref.at[me], mode_sems.at[0, 0, 0], mode_sems.at[1, 0, 0], "mode", other("mode", 1, 2)
    )
    out_ref[me] = own_ref[...]
    for k in range(CHUNKS):
        for step in list(range(1, slabs, 2)) + list(range(2, slabs, 2)):
            for other_step, here, other_k, copy in copies:
                if (other_step, other_k) == (step, k):
                    copy.wait_recv()
                    source = lax.axis_index("mode") * slabs + other("slab", slabs - step, slabs)
                    relays.append(send(
                        out_ref.at[source, here], out_ref.at[source, here],
                        mode_sems.at[0, step, k], mode_sems.at[1, step, k], "mode", other("mode", 1, 2),
                    ))
    near.wait()
    for copy in relays:
        copy.wait()
    for one in copies:
        one[3].wait_send()


def forward_kernel(
    span, slabs, kx, x_ref, ahead_ref, row_ref, w_ref, limit_ref, mode_limit_ref, out_ref, turned_ref, spec_ref, x_buf, kept_ref,
    part_ref, half_ref, give_ref, take_ref, w_buf, t_buf, sum_ref, peer_ref, own_ref, lines_ref, ahead_buf, row_buf,
    mode_a, slab_a, mode_b, slab_b, chan_sems, x_sems, w_sems, table_sems, t_sems,
):
    ins, freqs, outs = w_ref.shape[0], w_ref.shape[1], w_ref.shape[4]
    rows, cols = x_ref.shape[1:]
    block = LANES // span
    groups = ins // block
    mine_outs = outs // 2
    wide = freqs * kx
    me_mode, me_slab = lax.axis_index("mode"), lax.axis_index("slab")
    peer_mode = other("mode", 1, 2)
    first = lax.axis_index("chan") * ins
    tables = [
        pltpu.make_async_copy(ahead_ref.at[me_mode], ahead_buf, table_sems.at[0]),
        pltpu.make_async_copy(row_ref.at[me_slab], row_buf, table_sems.at[1]),
    ]
    tables[0].start()

    def x_copy(k):
        here = pl.ds(k * (block // 2), block // 2)
        return pltpu.make_async_copy(x_ref.at[here], x_buf.at[here], x_sems.at[k])

    def w_copy(g):
        here = pl.ds(g * block, block)
        return pltpu.make_async_copy(w_ref.at[here], w_buf.at[here], w_sems.at[g])

    for g in range(2):
        x_copy(2 * g).start()
        x_copy(2 * g + 1).start()
        if g == 0:
            tables[1].start()
    greet(slabs)

    def t_copy(g):
        here = pl.ds(g * block, block)
        return pltpu.make_async_copy(t_buf.at[here], turned_ref.at[here], t_sems.at[g])

    def place(g):
        return pl.ds(pl.multiple_of(g * kx, kx), kx)

    def mode_copy(g):
        return pltpu.make_async_remote_copy(
            src_ref=part_ref.at[pl.ds(peer_mode * slabs, slabs), place(g)], dst_ref=half_ref.at[:, place(g)],
            send_sem=mode_a.at[0, g], recv_sem=mode_a.at[1, g],
            device_id={"mode": peer_mode}, device_id_type=pl.DeviceIdType.MESH,
        )

    def slab_copy(step, g):
        return pltpu.make_async_remote_copy(
            src_ref=give_ref.at[step, place(g)], dst_ref=take_ref.at[step, place(g)],
            send_sem=slab_a.at[0, step, g], recv_sem=slab_a.at[1, step, g],
            device_id={"slab": other("slab", step, slabs)}, device_id_type=pl.DeviceIdType.MESH,
        )

    def ahead(g):
        x_copy(2 * g).wait()
        x_copy(2 * g + 1).wait()

        @pl.when(g + 2 < groups)
        def _():
            x_copy(2 * g + 4).start()
            x_copy(2 * g + 5).start()

        @pl.when(g + 2 >= groups)
        def _():
            for k in range(groups // 2):
                w_copy((g + 2 - groups) * (groups // 2) + k).start()
        values = x_buf[pl.ds(g * block, block)].reshape(block * rows, cols)
        lines_ref[...] = two_way(values, ahead_buf[...])

    def finish(g):
        def store(owner, values):
            part_ref[owner, place(g)] = values
        mix_rows(lines_ref, row_buf[...], rows, span, kx, store)

    limit = column_of(limit_ref[...], outs, 0)

    def flip(g):
        for k in range(block):
            i = g * block + k
            keep = jnp.broadcast_to(limit, (outs, wide)) > (first + i).astype(jnp.float32)
            for p in range(2):
                turned = w_buf[i, :, p].reshape(wide, outs).T
                t_buf[i, :, p * wide : (p + 1) * wide] = jnp.where(keep, turned, 0.0)

    def pass_on(g):
        mode_copy(g).wait_recv()
        for step in [slabs // 2] + [step for step in range(1, slabs) if step != slabs // 2]:
            slab = other("slab", step, slabs)
            give_ref[step, place(g)] = part_ref[me_mode * slabs + slab, place(g)] + half_ref[slab, place(g)]
            slab_copy(step, g).start()

    for table in tables:
        table.wait()
    ahead(0)

    def body(g, carry):
        finish(g - 1)
        ahead(g)
        mode_copy(g - 1).start()

        @pl.when(g > 1)
        def _():
            pass_on(g - 2)
        return carry

    lax.fori_loop(1, groups, body, 0)
    finish(groups - 1)
    mode_copy(groups - 1).start()
    pass_on(groups - 2)
    pass_on(groups - 1)
    kept_ref[...] = mode_scales(mode_limit_ref, kept_ref.shape, kx, slabs * rows * 2 * cols)

    def turn_over(g, carry):
        w_copy(g).wait()
        flip(g)
        t_copy(g).start()
        return carry
    lax.fori_loop(0, groups, turn_over, 0)
    mine = part_ref[me_mode * slabs + me_slab] + half_ref[me_slab]

    def landed(g, carry):
        for step in range(1, slabs):
            slab_copy(step, g).wait_recv()
        return carry
    lax.fori_loop(0, groups, landed, 0)
    for step in range(1, slabs):
        mine = mine + take_ref[step]
    to_lanes(mine, spec_ref, kx)

    def contract(i, carry):
        real, imag = carry
        w_real, w_imag = t_buf[i, :, :wide], t_buf[i, :, wide:]
        s_real, s_imag = both_parts(spec_ref, pl.ds(i, 1))
        return real + (s_real * w_real - s_imag * w_imag), imag + (s_real * w_imag + s_imag * w_real)

    zero = jnp.zeros((outs, wide), jnp.float32)
    real, imag = lax.fori_loop(0, ins, contract, (zero, zero))
    put_part(sum_ref, slice(None), 0, real)
    put_part(sum_ref, slice(None), 1, imag)
    theirs = other("chan", 1, 2) * mine_outs
    swap = send(
        sum_ref.at[:, pl.ds(theirs, mine_outs)], peer_ref, chan_sems.at[0], chan_sems.at[1], "chan", other("chan", 1, 2)
    )
    swap.wait_recv()
    for j in range(peer_ref.shape[0]):
        peer_ref[j] = (sum_ref[j, pl.ds(first, mine_outs)] + peer_ref[j]) * kept_ref[j % kept_ref.shape[0]]
    own_ref[...] = to_rows(peer_ref, mine_outs // 8, kx)
    gather(own_ref, out_ref, mode_b, slab_b, slabs)
    swap.wait_send()

    def settle(g, carry):
        t_copy(g).wait()
        mode_copy(g).wait_send()
        for step in range(1, slabs):
            slab_copy(step, g).wait_send()
        return carry
    lax.fori_loop(0, groups, settle, 0)


def backward_kernel(
    slabs, kx, part_ref, sums_ref, turned_ref, weight_ref, out_ref, grad_ref, total_ref,
    half_ref, give_ref, take_ref, t_buf, back_ref, own_ref, near_ref, far_ref, pass_ref,
    mode_a, slab_a, mode_b, slab_b, chan_sems, sum_mode, sum_slab, t_sem,
):
    ins, outs, wide = t_buf.shape[0], t_buf.shape[1], t_buf.shape[2] // 2
    mine_outs = outs // 2
    load = pltpu.make_async_copy(turned_ref, t_buf, t_sem)
    load.start()
    greet(slabs)
    first = lax.axis_index("chan") * ins
    near = send(sums_ref, near_ref, sum_mode.at[0], sum_mode.at[1], "mode", other("mode", 1, 2))

    far = []
    def total_up():
        near.wait_recv()
        pass_ref[...] = sums_ref[...] + near_ref[...]
        for step in range(1, slabs):
            far.append(send(
                pass_ref, far_ref.at[step], sum_slab.at[0, step], sum_slab.at[1, step], "slab", other("slab", step, slabs)
            ))

    mine, sent = scatter_sum(part_ref, half_ref, give_ref, take_ref, mode_a, slab_a, slabs, total_up)
    to_lanes(mine, back_ref, kx)
    here = pl.ds(first, mine_outs)
    for j in range(back_ref.shape[0]):
        grad_ref[j, here] = back_ref[j] * weight_ref[j % weight_ref.shape[0]]
    swap = send(
        grad_ref.at[:, here], grad_ref.at[:, here], chan_sems.at[0], chan_sems.at[1], "chan", other("chan", 1, 2)
    )
    load.wait()
    swap.wait_recv()

    def pull(i, carry):
        w_real, w_imag = t_buf[i, :, :wide], t_buf[i, :, wide:]
        g_real, g_imag = both_parts(grad_ref, slice(None))
        put_part(back_ref, pl.ds(i, 1), 0, jnp.sum(g_real * w_real + g_imag * w_imag, axis=0, keepdims=True))
        put_part(back_ref, pl.ds(i, 1), 1, jnp.sum(g_imag * w_real - g_real * w_imag, axis=0, keepdims=True))
        return carry
    lax.fori_loop(0, ins, pull, 0)
    own_ref[...] = to_rows(back_ref, ins // 8, kx)
    gather(own_ref, out_ref, mode_b, slab_b, slabs)
    total = pass_ref[...]
    for step, copy in zip(range(1, slabs), far):
        copy.wait()
        total = total + far_ref[step]
    total_ref[...] = total
    near.wait_send()
    swap.wait_send()
    for wait in sent:
        wait()


def fits(shapes, mesh_sizes):
    channels, rows, cols = shapes[0]
    outs, freqs, kx = shapes[2][1], shapes[2][2], shapes[2][4]
    slabs, modes, chans = mesh_sizes
    return (
        modes == 2 and chans == 2 and slabs > 2 and slabs % 2 == 0
        and 8 * kx == LANES and 8 * freqs == LANES and 2 * freqs * channels == 8 * LANES
        and outs == chans * channels
        and rows % LANES == 0 and cols % LANES == 0
    )


def local(source_field, cotangent, spectral_weight, skip_gain, channel_bias, mode_limit, width_limit):
    slabs, modes, chans = (lax.axis_size(axis) for axis in ("slab", "mode", "chan"))
    args = (source_field, cotangent, spectral_weight, skip_gain, channel_bias, mode_limit, width_limit)
    if not fits([one.shape for one in args], (slabs, modes, chans)):
        return local_plain(*args)
    channels, rows, cols = source_field.shape
    outs, freqs, kx = spectral_weight.shape[1], spectral_weight.shape[2], spectral_weight.shape[4]
    span = 2 * freqs
    block = LANES // span
    groups = channels // block
    owners = slabs * modes
    all_kx, all_rows, all_cols = kx * slabs, rows * slabs, cols * modes
    wide = freqs * kx
    ahead, row_ahead, row_behind, behind = (
        jnp.asarray(t) for t in packed_tables(all_rows, all_cols, slabs, modes, freqs, all_kx)
    )

    def pick(table, axis):
        return pl.BlockSpec((1,) + table.shape[1:], lambda g: (lax.axis_index(axis), 0, 0))

    cells = pl.BlockSpec((block, rows, cols), lambda g: (g, 0, 0))
    scalars = pl.BlockSpec(memory_space=pltpu.SMEM)
    field = jax.ShapeDtypeStruct(source_field.shape, jnp.float32)
    room = lambda size: pltpu.CompilerParams(dimension_semantics=("arbitrary",), vmem_limit_bytes=size * MIB)
    f32 = jnp.float32

    weight = spectral_weight.transpose(0, 2, 3, 4, 1)
    limit = width_limit.reshape(1, outs)

    dma, vmem = pltpu.SemaphoreType.DMA, pltpu.VMEM
    in_vmem, anywhere = pl.BlockSpec(memory_space=pltpu.VMEM), pl.BlockSpec(memory_space=pl.ANY)
    piece = (groups * kx, LANES)
    common = [vmem((slabs,) + piece, f32), vmem((slabs,) + piece, f32), vmem((slabs,) + piece, f32)]
    pair = [dma((2, slabs, CHUNKS))] * 4
    comm = lambda ident, room: pltpu.CompilerParams(
        collective_id=ident, has_side_effects=True, vmem_limit_bytes=room * MIB
    )
    flat = lambda lines: (2 * wide // LANES, lines, LANES)

    in_hbm = lambda array: pltpu.with_memory_space_constraint(array, pltpu.HBM)
    held = lambda array: pltpu.with_memory_space_constraint(array, pltpu.VMEM)
    modes_shape = (owners,) + piece
    out_modes, turned, spec, source_held, weights = pl.pallas_call(
        functools.partial(forward_kernel, span, slabs, kx),
        in_specs=[anywhere, anywhere, anywhere, anywhere, in_vmem, in_vmem],
        out_specs=[in_vmem, anywhere, in_vmem, in_vmem, in_vmem],
        out_shape=[
            jax.ShapeDtypeStruct(modes_shape, f32), pltpu.HBM((channels, outs, 2 * wide), f32),
            jax.ShapeDtypeStruct(flat(channels), f32), pltpu.VMEM(field.shape, f32),
            jax.ShapeDtypeStruct((wide // LANES, channels, LANES), f32),
        ],
        scratch_shapes=[vmem(modes_shape, f32)] + common + [
            vmem(weight.shape, f32), vmem((channels, outs, 2 * wide), f32), vmem(flat(outs), f32), vmem(flat(outs // 2), f32), vmem(piece, f32),
            vmem((block * rows, LANES), f32), vmem(ahead.shape[1:], jnp.bfloat16), vmem(row_ahead.shape[1:], jnp.bfloat16),
            dma((2, groups)), dma((2, slabs, groups)), dma((2, slabs, CHUNKS)), dma((2, slabs, CHUNKS)), dma((2,)),
            dma((2 * groups,)), dma((groups,)), dma((2,)), dma((groups,)),
        ],
        compiler_params=comm(20, FORWARD),
        name="forward_modes",
    )(in_hbm(source_field), in_hbm(ahead), in_hbm(row_ahead), in_hbm(weight), limit, mode_limit.T)

    output, grad_sum, grad_partial, sums = pl.pallas_call(
        functools.partial(middle_packed, span, kx),
        grid=(groups,),
        in_specs=[
            in_vmem, cells, in_vmem, scalars, scalars, pick(ahead, "mode"), pick(row_ahead, "slab"),
            pick(row_behind, "slab"), pick(behind, "mode"),
        ],
        out_specs=[cells, in_vmem, in_vmem, in_vmem],
        out_shape=[field, pltpu.VMEM(field.shape, f32), jax.ShapeDtypeStruct(modes_shape, f32), jax.ShapeDtypeStruct((8, LANES), f32)],
        scratch_shapes=[
            vmem((block * rows, 2 * cols), jnp.bfloat16), vmem((block * rows, LANES), f32), vmem((block, rows, cols), f32),
            vmem((block, rows, LANES), f32), vmem((block, rows, LANES), f32), vmem((block * rows, LANES), f32),
        ],
        input_output_aliases={0: 1},
        compiler_params=room(MIDDLE),
        name="middle",
    )(
        held(source_held), cotangent, out_modes, skip_gain, channel_bias,
        ahead, row_ahead, row_behind, behind,
    )

    back_modes, all_grads, totals = pl.pallas_call(
        functools.partial(backward_kernel, slabs, kx),
        in_specs=[in_vmem, in_vmem, anywhere, in_vmem],
        out_specs=[in_vmem] * 3,
        out_shape=[pltpu.HBM(modes_shape, f32), pltpu.HBM(flat(outs), f32), pltpu.HBM((8, LANES), f32)],
        scratch_shapes=common + [
            vmem((channels, outs, 2 * wide), f32), vmem(flat(channels), f32), vmem(piece, f32), vmem((8, LANES), f32),
            vmem((slabs, 8, LANES), f32), vmem((8, LANES), f32),
        ] + pair + [dma((2,)), dma((2,)), dma((2, slabs)), dma],
        compiler_params=comm(21, BACKWARD),
        name="backward_modes",
    )(in_hbm(grad_partial), in_hbm(sums), in_hbm(turned), in_hbm(weights))

    count = channels // groups
    whole = lambda array: pl.BlockSpec(array.shape, lambda g: (0,) * len(array.shape))
    line = jax.ShapeDtypeStruct((1, channels), f32)
    field_grad, weight_grad, gate_grad, bias_grad = pl.pallas_call(
        functools.partial(last_packed, span, kx),
        grid=(groups,),
        in_specs=[
            in_vmem, in_vmem, scalars, pick(row_behind, "slab"), pick(behind, "mode"),
            whole(all_grads), whole(spec), whole(limit), whole(totals),
        ],
        out_specs=[cells, pl.BlockSpec((count,) + weight.shape[1:], lambda g: (g, 0, 0, 0, 0)), whole(line), whole(line)],
        out_shape=[field, jax.ShapeDtypeStruct(weight.shape, f32), line, line],
        compiler_params=room(LAST),
        name="last",
    )(
        pltpu.with_memory_space_constraint(grad_sum, pltpu.VMEM), back_modes, skip_gain,
        row_behind, behind, all_grads, spec, limit, totals,
    )
    spectral_grad = weight_grad.transpose(0, 4, 1, 2, 3)
    return (output, field_grad, spectral_grad, gate_grad.reshape(-1), bias_grad.reshape(-1))


def solution(mesh):
    in_specs = (
        P(("member", "chan"), "slab", "mode"),
        P(("member", "chan"), "slab", "mode"),
        P(("member", "chan"), None, "mode", None, "slab"),
        P(("member", "chan")),
        P(("member", "chan")),
        P("member", None),
        P("member"),
    )
    out_specs = (
        P(("member", "chan"), "slab", "mode"),
        P(("member", "chan"), "slab", "mode"),
        P(("member", "chan"), None, "mode", None, "slab"),
        P(("member", "chan")),
        P(("member", "chan")),
    )
    return jax.shard_map(local, mesh=mesh, in_specs=in_specs, out_specs=out_specs, check_vma=False)
```

```python
import functools
import math

import jax
import jax.numpy as jnp
import ml_dtypes
import numpy as np
from jax import lax
from jax.experimental import pallas as pl
from jax.experimental.pallas import tpu as pltpu
from jax.sharding import PartitionSpec as P

LANES = 128
BIG = 60 * 1024 * 1024
MIB = 1024 * 1024
FORWARD, MIDDLE, LAST, BACKWARD = 40, 40, 40, 20


def split_table(table):
    high = lax.reduce_precision(table, 8, 7)
    return high.astype(jnp.bfloat16), (table - high).astype(jnp.bfloat16)


def split_block(values):
    high = values.astype(jnp.bfloat16)
    return high, (values - high.astype(jnp.float32)).astype(jnp.bfloat16)


def dot_pair(left, right):
    left_high, left_low = left
    right_high, right_low = right
    mul = functools.partial(jnp.dot, preferred_element_type=jnp.float32)
    return mul(left_high, right_high) + mul(left_low, right_high) + mul(left_high, right_low)


def tables(extent, waves, first_cell, cell_count):
    cell_index = first_cell + jnp.arange(cell_count, dtype=jnp.int32)
    products = (cell_index[:, None] * waves[None, :] % extent).astype(jnp.float32)
    angles = products * (2.0 * math.pi / extent)
    return jnp.cos(angles), jnp.sin(angles)


def store_spectrum(values, col_pair, row_pair, out_ref):
    block, rows, cols = values.shape
    lines = dot_pair(split_block(values.reshape(block * rows, cols)), col_pair)
    all_kx = row_pair[0].shape[0] // 2
    kx, lanes = out_ref.shape[2:]
    span = lanes // block
    mode_count = lines.shape[1] // span
    slabs = out_ref.shape[0] // mode_count
    done = []
    for c in range(block):
        mixed = dot_pair(row_pair, split_block(lines[c * rows : (c + 1) * rows]))
        done.append(mixed[:all_kx] - turn(mixed[all_kx:], span))
    for m in range(mode_count):
        packed = jnp.concatenate([one[:, m * span : (m + 1) * span] for one in done], axis=1)
        for s in range(slabs):
            out_ref[m * slabs + s, 0] = packed[s * kx : (s + 1) * kx]


def turn(values, span):
    half = span // 2
    pieces = []
    for first in range(0, values.shape[1], span):
        pieces.append(-values[:, first + half : first + span])
        pieces.append(values[:, first : first + half])
    return jnp.concatenate(pieces, axis=1)


def all_modes(modes_ref, mode_count, c, block):
    span = modes_ref.shape[3] // block
    slabs = modes_ref.shape[0] // mode_count
    columns = []
    for m in range(mode_count):
        stack = [modes_ref[m * slabs + s, 0] for s in range(slabs)]
        columns.append(jnp.concatenate(stack, axis=0)[:, c * span : (c + 1) * span])
    return jnp.concatenate(columns, axis=1), span


def synth(modes_and_span, row_pair, col_pair):
    modes, span = modes_and_span
    stacked = jnp.concatenate([modes, turn(modes, span)], axis=0)
    lines = dot_pair(row_pair, split_block(stacked))
    return dot_pair(split_block(lines), col_pair)


def spectrum_kernel(x_ref, ch_ref, cl_ref, rh_ref, rl_ref, out_ref):
    store_spectrum(x_ref[...], (ch_ref[...], cl_ref[...]), (rh_ref[...], rl_ref[...]), out_ref)


def middle_kernel(
    mode_count, x_ref, cot_ref, modes_ref, gain_ref, bias_ref, ch_ref, cl_ref, rh_ref, rl_ref,
    cth_ref, ctl_ref, ih_ref, il_ref, out_ref, grad_ref, spec_ref, sums_ref,
):
    block = x_ref.shape[0]
    row_back = (ih_ref[...], il_ref[...])
    col_back = (cth_ref[...], ctl_ref[...])
    scale = math.sqrt(2.0 / math.pi)
    for c in range(block):
        source = x_ref[c]
        gain = gain_ref[c]
        v = synth(all_modes(modes_ref, mode_count, c, block), row_back, col_back) + gain[:, :1] * source + bias_ref[c][:, :1]
        square = v * v
        t = jnp.tanh(scale * v * (1.0 + 0.044715 * square))
        half_up = 0.5 * (1.0 + t)
        out_ref[c] = v * half_up
        slope = half_up + 0.5 * v * (1.0 - t * t) * (scale * (1.0 + 3.0 * 0.044715 * square))
        grad = cot_ref[c] * slope
        grad_ref[c] = grad
        gate = jnp.sum(jnp.sum(grad * source, axis=0, keepdims=True), axis=1, keepdims=True)
        bias = jnp.sum(jnp.sum(grad, axis=0, keepdims=True), axis=1, keepdims=True)
        lane = lax.broadcasted_iota(jnp.int32, (1, LANES), 1)
        sums_ref[c] = jnp.where(lane == 0, gate, bias)
    store_spectrum(
        grad_ref[...], (ch_ref[...], cl_ref[...]), (rh_ref[...], rl_ref[...]), spec_ref
    )


def last_kernel(mode_count, grad_ref, modes_ref, gain_ref, cth_ref, ctl_ref, ih_ref, il_ref, out_ref):
    block = grad_ref.shape[0]
    for c in range(block):
        modes = all_modes(modes_ref, mode_count, c, block)
        branch = synth(modes, (ih_ref[...], il_ref[...]), (cth_ref[...], ctl_ref[...]))
        out_ref[c] = branch + gain_ref[c][:, :1] * grad_ref[c]


def contract_kernel(w_ref, spec_ref, limit_ref, out_ref):
    block, freqs, _, kx, outs = w_ref.shape
    first = lax.axis_index("chan") * (block * pl.num_programs(0)) + pl.program_id(0) * block

    @pl.when(pl.program_id(0) == 0)
    def _():
        out_ref[...] = jnp.zeros_like(out_ref)

    limit = limit_ref[...]
    for y in range(freqs):
        real = out_ref[y, 0]
        imag = out_ref[y, 1]
        for i in range(block):
            keep = first + i < limit
            spec = spec_ref[0]
            at = 2 * freqs * i + y
            s_real = jnp.where(keep, spec[:, at : at + 1], 0.0)
            s_imag = jnp.where(keep, spec[:, freqs + at : freqs + at + 1], 0.0)
            w_real = w_ref[i, y, 0]
            w_imag = w_ref[i, y, 1]
            real = real + (s_real * w_real - s_imag * w_imag)
            imag = imag + (s_real * w_imag + s_imag * w_real)
        out_ref[y, 0] = real
        out_ref[y, 1] = imag


def back_kernel(w_ref, spec_ref, grads_ref, limit_ref, wgrad_ref, out_ref):
    block, freqs, _, kx, outs = w_ref.shape
    first = lax.axis_index("chan") * (block * pl.num_programs(0)) + pl.program_id(0) * block
    limit = limit_ref[...]
    lane = lax.broadcasted_iota(jnp.int32, out_ref.shape[1:], 1)
    spec = spec_ref[0]
    back = jnp.zeros(out_ref.shape[1:], jnp.float32)
    for i in range(block):
        keep = first + i < limit
        for y in range(freqs):
            at = 2 * freqs * i + y
            g_real = jnp.where(keep, grads_ref[y, 0], 0.0)
            g_imag = jnp.where(keep, grads_ref[y, 1], 0.0)
            s_real = spec[:, at : at + 1]
            s_imag = spec[:, freqs + at : freqs + at + 1]
            wgrad_ref[i, y, 0] = s_real * g_real + s_imag * g_imag
            wgrad_ref[i, y, 1] = s_real * g_imag - s_imag * g_real
            w_real = w_ref[i, y, 0]
            w_imag = w_ref[i, y, 1]
            b_real = jnp.sum(g_real * w_real + g_imag * w_imag, axis=1, keepdims=True)
            b_imag = jnp.sum(g_imag * w_real - g_real * w_imag, axis=1, keepdims=True)
            back = jnp.where(lane == at, b_real, back)
            back = jnp.where(lane == freqs + at, b_imag, back)
    out_ref[0] = back


def exchange_kernel(axes, sizes, gather, x_ref, out_ref, send_sem, recv_sem, own_sem):
    total = math.prod(sizes)
    me = lax.axis_index(axes[0])
    for axis, size in zip(axes[1:], sizes[1:]):
        me = me * size + lax.axis_index(axis)

    def place(index):
        coords = {}
        for axis, size in reversed(list(zip(axes, sizes))):
            coords[axis] = lax.rem(index, size)
            index = lax.div(index, size)
        return coords

    barrier = pltpu.get_barrier_semaphore()
    for step in range(1, total):
        pl.semaphore_signal(
            barrier, inc=1, device_id=place(lax.rem(me + step, total)),
            device_id_type=pl.DeviceIdType.MESH,
        )
    pl.semaphore_wait(barrier, total - 1)
    copies = []
    for step in range(1, total):
        peer = lax.rem(me + step, total)
        copy = pltpu.make_async_remote_copy(
            src_ref=x_ref if gather else x_ref.at[peer],
            dst_ref=out_ref.at[me],
            send_sem=send_sem.at[step],
            recv_sem=recv_sem.at[step],
            device_id=place(peer),
            device_id_type=pl.DeviceIdType.MESH,
        )
        copy.start()
        copies.append(copy)
    own = pltpu.make_async_copy(x_ref if gather else x_ref.at[me], out_ref.at[me], own_sem)
    own.start()
    own.wait()
    for copy in copies:
        copy.wait()


def exchange(values, axes, gather, ident):
    sizes = tuple(lax.axis_size(axis) for axis in axes)
    total = math.prod(sizes)
    piece = values.shape if gather else values.shape[1:]
    flat = values.reshape((-1, LANES) if gather else (total, -1, LANES))
    out = pl.pallas_call(
        functools.partial(exchange_kernel, axes, sizes, gather),
        out_shape=jax.ShapeDtypeStruct((total,) + flat.shape[-2:], jnp.float32),
        in_specs=[pl.BlockSpec(memory_space=pltpu.VMEM)],
        out_specs=pl.BlockSpec(memory_space=pltpu.VMEM),
        scratch_shapes=[
            pltpu.SemaphoreType.DMA((total,)),
            pltpu.SemaphoreType.DMA((total,)),
            pltpu.SemaphoreType.DMA,
        ],
        compiler_params=pltpu.CompilerParams(collective_id=ident, has_side_effects=True),
        name="exchange" + str(ident),
    )(flat)
    return out.reshape((total,) + piece)


def mode_weights(limit_rows, col_freq, row_freq, kx_count, cells_total):
    keep_cols = col_freq[None, :] < limit_rows[:, 0:1]
    keep_rows = (row_freq[None, :] < limit_rows[:, 1:2]) | (
        (kx_count - row_freq)[None, :] < limit_rows[:, 1:2]
    )
    scales = jnp.where(col_freq == 0, 1.0, 2.0).astype(jnp.float32) / cells_total
    joined = keep_rows[:, :, None] & keep_cols[:, None, :]
    return (joined.astype(jnp.float32) * scales[None, None, :])[:, :, None, :]


def local_plain(
    source_field, cotangent, spectral_weight, skip_gain, channel_bias, mode_limit, width_limit
):
    channels, row_count, col_count = source_field.shape
    slabs = lax.axis_size("slab")
    modes = lax.axis_size("mode")
    chans = lax.axis_size("chan")
    slab_index = lax.axis_index("slab")
    mode_index = lax.axis_index("mode")
    chan_index = lax.axis_index("chan")
    outs = spectral_weight.shape[1]
    freqs = spectral_weight.shape[2]
    kx = spectral_weight.shape[4]
    all_freqs = freqs * modes
    all_kx = kx * slabs
    all_rows = row_count * slabs
    all_cols = col_count * modes

    col_waves = jnp.arange(all_freqs, dtype=jnp.int32)
    row_waves = jnp.arange(all_kx, dtype=jnp.int32)
    row_waves = row_waves + jnp.where(2 * row_waves >= all_kx, all_rows - all_kx, 0)
    col_cos, col_sin = tables(all_cols, col_waves, mode_index * col_count, col_count)
    row_cos, row_sin = tables(all_rows, row_waves, slab_index * row_count, row_count)
    col_tab = jnp.stack(
        [col_cos.reshape(-1, modes, freqs), -col_sin.reshape(-1, modes, freqs)], axis=2
    ).reshape(col_count, 2 * all_freqs)
    row_tab = jnp.concatenate([row_cos, row_sin], axis=1)
    col_pair = split_table(col_tab)
    col_back = tuple(part.T for part in col_pair)
    row_back = split_table(row_tab)
    row_pair = tuple(part.T for part in row_back)

    block = LANES // (2 * freqs)
    groups = channels // block
    owners = slabs * modes
    cells = pl.BlockSpec((block, row_count, col_count), lambda c: (c, 0, 0))
    freq_cells = pl.BlockSpec((owners, 1, kx, LANES), lambda c: (0, c, 0, 0))
    per_channel = pl.BlockSpec((block, 1, LANES), lambda c: (c, 0, 0))
    field = jax.ShapeDtypeStruct(source_field.shape, jnp.float32)
    freq_field = jax.ShapeDtypeStruct((owners, groups, kx, LANES), jnp.float32)
    params = pltpu.CompilerParams(
        dimension_semantics=("arbitrary",), vmem_limit_bytes=BIG
    )

    def whole(array):
        return pl.BlockSpec(array.shape, lambda c: (0,) * array.ndim)

    grid = (channels // block,)
    wide = lambda values: jnp.broadcast_to(values[:, None, None], (channels, 1, LANES))
    gain = wide(skip_gain)
    forward = col_pair + row_pair
    back = col_back + row_back

    def spread(partial, ident):
        half = exchange(partial.reshape(modes, -1, LANES), ("mode",), False, ident)
        half = jnp.sum(half, axis=0).reshape(slabs, -1, LANES)
        return jnp.sum(exchange(half, ("slab",), False, ident + 1), axis=0).reshape(
            groups, kx, LANES
        )

    def joined(piece, ident):
        half = exchange(piece, ("slab",), True, ident)
        return exchange(half, ("mode",), True, ident + 1).reshape((owners,) + piece.shape)

    spectra = spread(
        pl.pallas_call(
            spectrum_kernel,
            grid=grid,
            in_specs=[cells] + [whole(t) for t in forward],
            out_specs=freq_cells,
            out_shape=freq_field,
            compiler_params=params,
            name="spectrum",
        )(source_field, *forward),
        0,
    )

    weight = spectral_weight.transpose(0, 2, 3, 4, 1)
    limit = width_limit.reshape(1, outs)
    in_block = block
    w_spec = pl.BlockSpec((in_block, freqs, 2, kx, outs), lambda i: (i, 0, 0, 0, 0))
    s_spec = pl.BlockSpec((1, kx, LANES), lambda i: (i, 0, 0))
    mode_spec = pl.BlockSpec((freqs, 2, kx, outs), lambda i: (0, 0, 0, 0))
    limit_spec = pl.BlockSpec((1, outs), lambda i: (0, 0))
    partial_modes = pl.pallas_call(
        contract_kernel,
        grid=(channels // in_block,),
        in_specs=[w_spec, s_spec, limit_spec],
        out_specs=mode_spec,
        out_shape=jax.ShapeDtypeStruct((freqs, 2, kx, outs), jnp.float32),
        compiler_params=params,
        name="contract",
    )(weight, spectra, limit)
    halves = partial_modes.reshape(freqs, 2, kx, chans, groups, block)
    halves = halves.transpose(3, 4, 2, 5, 1, 0).reshape(chans, groups, kx, LANES)
    summed_modes = jnp.sum(exchange(halves, ("chan",), False, 2), axis=0)

    col_freq = mode_index * freqs + jnp.arange(freqs, dtype=jnp.int32)
    row_freq = slab_index * kx + jnp.arange(kx, dtype=jnp.int32)
    limit_rows = lax.dynamic_slice_in_dim(mode_limit, chan_index * channels, channels, 0)
    weights = mode_weights(limit_rows, col_freq, row_freq, all_kx, all_rows * all_cols)
    weights = jnp.broadcast_to(weights, (channels, kx, 2, freqs))
    weights = weights.reshape(groups, block, kx, 2 * freqs).transpose(0, 2, 1, 3)
    weights = weights.reshape(groups, kx, LANES)
    out_modes = joined(summed_modes * weights, 3)

    output, grad_sum, grad_partial, sums = pl.pallas_call(
        functools.partial(middle_kernel, modes),
        grid=grid,
        in_specs=[cells, cells, freq_cells, per_channel, per_channel]
        + [whole(t) for t in forward + back],
        out_specs=[cells, cells, freq_cells, per_channel],
        out_shape=[
            field,
            field,
            freq_field,
            jax.ShapeDtypeStruct((channels, 1, LANES), jnp.float32),
        ],
        compiler_params=params,
        name="middle",
    )(source_field, cotangent, out_modes, gain, wide(channel_bias), *forward, *back)

    grad_modes = spread(grad_partial, 5) * weights
    all_grads = exchange(grad_modes, ("chan",), True, 7)
    all_grads = all_grads.reshape(chans, groups, kx, block, 2, freqs)
    all_grads = all_grads.transpose(5, 4, 2, 0, 1, 3).reshape(freqs, 2, kx, outs)
    weight_grad, back_modes = pl.pallas_call(
        back_kernel,
        grid=(channels // in_block,),
        in_specs=[w_spec, s_spec, mode_spec, limit_spec],
        out_specs=[w_spec, s_spec],
        out_shape=[
            jax.ShapeDtypeStruct(weight.shape, jnp.float32),
            jax.ShapeDtypeStruct(spectra.shape, jnp.float32),
        ],
        compiler_params=params,
        name="back",
    )(weight, spectra, all_grads, limit)
    spectral_grad = weight_grad.transpose(0, 4, 1, 2, 3)

    sent = back_modes.size // LANES
    row_sums = sums[:, 0, :2].T.reshape(-1)
    extra = -(-row_sums.size // (8 * LANES)) * 8
    row_sums = jnp.pad(row_sums, (0, extra * LANES - row_sums.size)).reshape(extra, LANES)
    packed = jnp.concatenate([back_modes.reshape(sent, LANES), row_sums], axis=0)
    parts = joined(packed, 8)
    field_modes = parts[:, :sent].reshape(owners, groups, kx, LANES)
    totals = jnp.sum(parts[:, sent:], axis=0).reshape(-1)
    gate_grad = totals[:channels]
    bias_grad = totals[channels : 2 * channels]
    field_grad = pl.pallas_call(
        functools.partial(last_kernel, modes),
        grid=grid,
        in_specs=[cells, freq_cells, per_channel] + [whole(t) for t in back],
        out_specs=cells,
        out_shape=field,
        compiler_params=params,
        name="last",
    )(grad_sum, field_modes, gain, *back)
    return (output, field_grad, spectral_grad, gate_grad, bias_grad)


def halves_of(table):
    table = table.astype(np.float32)
    high = table.astype(ml_dtypes.bfloat16)
    low = (table - high.astype(np.float32)).astype(ml_dtypes.bfloat16)
    return high, low


def packed_tables(all_rows, all_cols, slabs, modes, freqs, kx_all):
    cell = np.arange(all_cols)[:, None]
    angle = (cell * np.arange(modes * freqs)[None, :] % all_cols) * (2.0 * np.pi / all_cols)
    parts = np.stack([np.cos(angle), -np.sin(angle)], axis=1).reshape(modes, -1, 2, modes, freqs)
    parts = parts.transpose(0, 1, 3, 2, 4)
    cols = parts.shape[1]
    high, low = halves_of(parts)
    ahead = np.stack([high, low], axis=3).reshape(modes, cols, -1)
    flat_high = high.reshape(modes, cols, -1).transpose(0, 2, 1)
    flat_low = low.reshape(modes, cols, -1).transpose(0, 2, 1)
    behind = np.concatenate([flat_high, flat_low], axis=1)
    wave = np.arange(kx_all)
    wave = wave + np.where(2 * wave >= kx_all, all_rows - kx_all, 0)
    angle = (np.arange(all_rows)[:, None] * wave[None, :] % all_rows) * (2.0 * np.pi / all_rows)
    table = np.concatenate([np.cos(angle), np.sin(angle)], axis=1).reshape(slabs, -1, 2 * kx_all)
    high, low = halves_of(table)
    row_behind = np.concatenate([high, low], axis=2)
    high, low = high.transpose(0, 2, 1), low.transpose(0, 2, 1)
    row_ahead = np.concatenate([high, low], axis=2)
    return ahead, row_ahead, row_behind, behind


def lane_roll(values, shift):
    shift = shift % values.shape[-1]
    return values if shift == 0 else pltpu.roll(values, shift, values.ndim - 1)


def lanes_of(shape):
    return lax.broadcasted_iota(jnp.int32, shape, len(shape) - 1)


def high_low(values):
    high = values.astype(jnp.bfloat16)
    return high, (values - high.astype(jnp.float32)).astype(jnp.bfloat16)


def quarter_turn(values, span, sign):
    half = span // 2
    first = lanes_of(values.shape) % span < half
    back, ahead = lane_roll(values, -half), lane_roll(values, half)
    return jnp.where(first, -back, ahead) if sign > 0 else jnp.where(first, back, -ahead)


def three_way(row_table, values):
    high, low = high_low(values)
    width = row_table.shape[1] // 2
    left = jnp.concatenate([row_table, row_table[:, :width]], axis=1)
    right = jnp.concatenate([high, high, low], axis=0)
    return jnp.dot(left, right, preferred_element_type=jnp.float32)


def two_way(values, table):
    high, low = high_low(values)
    both = jnp.concatenate([high, low], axis=1)
    return jnp.dot(both, jnp.concatenate([table, table], axis=0), preferred_element_type=jnp.float32)


def mix_rows(lines_ref, row_table, rows, span, kx, store):
    block = LANES // span
    mixed = []
    for c in range(0, block, 2):
        pair = [lines_ref[(c + k) * rows : (c + k + 1) * rows] for k in range(2)]
        both = three_way(row_table, jnp.concatenate(pair, axis=1))
        mixed += [both[:, :LANES], both[:, LANES:]]
    lane = lanes_of(mixed[0].shape)
    pairs = []
    for c in range(0, block, 2):
        left = mixed[c] + lane_roll(mixed[c], -span)
        right = mixed[c + 1] + lane_roll(mixed[c + 1], span)
        pairs.append(jnp.where(lane % (2 * span) < span, left, right))
    low_half = lane < LANES // 2
    owners = [
        jnp.where(low_half, pairs[0], lane_roll(pairs[1], LANES // 2)),
        jnp.where(low_half, lane_roll(pairs[0], LANES // 2), pairs[1]),
    ]
    all_kx = owners[0].shape[0] // 2
    slabs = all_kx // kx
    for m, values in enumerate(owners):
        done = values[:all_kx] + quarter_turn(values[all_kx:], span, -1)
        for s in range(slabs):
            store(m * slabs + s, done[s * kx : (s + 1) * kx])


def group_lines(modes_ref, group, kx, row_table, span):
    block = LANES // span
    owners = modes_ref.shape[0]
    half = owners // 2
    here = pl.ds(pl.multiple_of(group * kx, kx), kx)
    stack = []
    for m in range(2):
        stack.append(jnp.concatenate([modes_ref[m * half + s, here] for s in range(half)], axis=0))
    full = [jnp.concatenate([one, quarter_turn(one, span, 1)], axis=0) for one in stack]
    rolled = [[lane_roll(one, k * span) for k in range(block)] for one in full]
    lane = lanes_of(full[0].shape)
    even = lane % (2 * span) < span
    low_half = lane < LANES // 2
    sides = []
    for c in range(block):
        first = jnp.where(low_half, rolled[0][(0 - c) % block], rolled[0][(2 - c) % block])
        second = jnp.where(low_half, rolled[1][(1 - c) % block], rolled[1][(3 - c) % block])
        sides.append(jnp.where(even, first, second))
    lines = []
    for c in range(0, block, 2):
        both = three_way(row_table, jnp.concatenate([sides[c], sides[c + 1]], axis=1))
        lines += [both[:, :LANES], both[:, LANES:]]
    return lines


def middle_packed(
    span, kx, x_ref, cot_ref, modes_ref, gain_ref, bias_ref, ahead_ref, row_ref, row_back_ref, behind_ref,
    out_ref, grad_ref, spec_ref, sums_ref, split_ref, lines_ref, branch_ref, next_ref, held_ref, made_ref,
):
    block, rows, cols = cot_ref.shape
    step = pl.program_id(0)
    scale = math.sqrt(2.0 / math.pi)
    row_table = row_ref[0]

    @pl.when(step == 0)
    def _():
        sums_ref[...] = jnp.zeros_like(sums_ref)

    def ahead(c):
        here = slice(c * rows, (c + 2) * rows)
        table = ahead_ref[0]
        high = jnp.dot(split_ref[0, c // 2], table, preferred_element_type=jnp.float32)
        lines_ref[here] = high + jnp.dot(split_ref[1, c // 2], table, preferred_element_type=jnp.float32)

    def finish(from_ref, group):
        def store(owner, values):
            spec_ref[owner, pl.ds(pl.multiple_of(group * kx, kx), kx)] = values
        mix_rows(from_ref, row_table, rows, span, kx, store)

    lane = lanes_of(sums_ref.shape)
    line = lax.broadcasted_iota(jnp.int32, sums_ref.shape, 0)

    def cell(c, lines):
        channel = step * block + c
        gain, shift = gain_ref[channel], bias_ref[channel]
        branch_ref[c] = two_way(lines, behind_ref[0])
        gate = jnp.zeros((8, cols), jnp.float32)
        bias = jnp.zeros((8, cols), jnp.float32)
        for r in range(0, rows, 16):
            here = slice(r, r + 16)
            source = x_ref[channel, here]
            v = branch_ref[c, here] + (gain * source + shift)
            square = v * v
            inner = v * (scale + (scale * 0.044715) * square)
            up = 0.5 + 0.5 * jnp.tanh(inner)
            out_ref[c, here] = v * up
            bend = v * (2.0 * scale + (6.0 * scale * 0.044715) * square)
            grad = cot_ref[c, here] * (up + (up * (1.0 - up)) * bend)
            grad_ref[channel, here] = grad
            high, low = high_low(grad)
            there = slice(c % 2 * rows + r, c % 2 * rows + r + 16)
            split_ref[0, c // 2, there] = high
            split_ref[1, c // 2, there] = low
            both = grad * source
            gate = gate + (both[:8] + both[8:])
            bias = bias + (grad[:8] + grad[8:])
        gate = jnp.sum(jnp.sum(gate, axis=0, keepdims=True), axis=1, keepdims=True)
        bias = jnp.sum(jnp.sum(bias, axis=0, keepdims=True), axis=1, keepdims=True)
        here = (lane == channel) & (line < 2)
        sums_ref[...] = jnp.where(here, jnp.where(line == 0, gate, bias), sums_ref[...])

    def prepare(group):
        for c, lines in enumerate(group_lines(modes_ref, group, kx, row_back_ref[0], span)):
            next_ref[c] = lines

    @pl.when(step == 0)
    def _():
        prepare(0)

    held_ref[...] = next_ref[...]
    made_ref[...] = lines_ref[...]
    for c in range(block):
        if c % 2 == 0:
            ahead(c)
        cell(c, held_ref[c])
        if c == 0:
            finish(made_ref, jnp.maximum(step - 2, 0))
        if c == 1:
            prepare(jnp.minimum(step + 1, pl.num_programs(0) - 1))

    @pl.when(step == pl.num_programs(0) - 1)
    def _():
        finish(lines_ref, step - 1)
        for c in range(0, block, 2):
            ahead(c)
        finish(lines_ref, step)


def last_packed(
    span, kx, grad_ref, modes_ref, gain_ref, row_back_ref, behind_ref, grads_ref, spec_ref, limit_ref, total_ref,
    out_ref, wgrad_ref, gate_ref, bias_ref,
):
    block = out_ref.shape[0]
    step = pl.program_id(0)
    lines = group_lines(modes_ref, step, kx, row_back_ref[0], span)
    count, freqs, outs = wgrad_ref.shape[0], wgrad_ref.shape[1], wgrad_ref.shape[4]
    wide = freqs * kx
    first = lax.axis_index("chan") * (count * pl.num_programs(0)) + step * count
    gate_ref[...] = total_ref[0:1, : gate_ref.shape[1]]
    bias_ref[...] = total_ref[1:2, : bias_ref.shape[1]]
    g_real, g_imag = both_parts(grads_ref, slice(None))
    limit = column_of(limit_ref[...], outs, 0)
    for i in range(count):
        keep = jnp.broadcast_to(limit, (outs, wide)) > (first + i).astype(jnp.float32)
        s_real, s_imag = both_parts(spec_ref, pl.ds(step * count + i, 1))
        real = jnp.where(keep, s_real * g_real + s_imag * g_imag, 0.0)
        imag = jnp.where(keep, s_real * g_imag - s_imag * g_real, 0.0)
        wgrad_ref[i, :, 0] = real.T.reshape(freqs, kx, outs)
        wgrad_ref[i, :, 1] = imag.T.reshape(freqs, kx, outs)
    for c in range(block):
        out_ref[c] = two_way(lines[c], behind_ref[0]) + gain_ref[step * block + c] * grad_ref[step * block + c]


def swap_groups(values, kx):
    lane = lanes_of(values.shape) // kx
    line = lax.broadcasted_iota(jnp.int32, values.shape, 1)
    count = values.shape[1]
    hop = 1
    while hop < count:
        up = lane_roll(pltpu.roll(values, count - hop, 1), hop * kx)
        down = lane_roll(pltpu.roll(values, hop, 1), -hop * kx)
        lane_bit, line_bit = lane // hop % 2, line // hop % 2
        values = jnp.where(lane_bit == line_bit, values, jnp.where(lane_bit == 1, up, down))
        hop *= 2
    return values


def to_lanes(packed, out_ref, kx):
    lines = swap_groups(packed.T.reshape(-1, 8, LANES), kx)
    wide = out_ref.shape[0]
    block = lines.shape[0] // wide
    for c in range(block):
        for j in range(wide):
            out_ref[j, pl.ds(c, 8, stride=block)] = lines[c * wide + j]


def to_rows(wide_ref, block, kx):
    wide = wide_ref.shape[0]
    pieces = []
    for c in range(block):
        for j in range(wide):
            pieces.append(wide_ref[j, pl.ds(c, 8, stride=block)][None])
    return swap_groups(jnp.concatenate(pieces, axis=0), kx).reshape(-1, LANES).T


def both_parts(ref, rows):
    half = ref.shape[0] // 2
    parts = [jnp.concatenate([ref[p * half + j, rows] for j in range(half)], axis=1) for p in range(2)]
    return parts[0], parts[1]


def put_part(ref, rows, part, values):
    half = ref.shape[0] // 2
    for j in range(half):
        ref[part * half + j, rows] = values[:, j * LANES : (j + 1) * LANES]


def other(axis, step, size):
    return lax.rem(lax.axis_index(axis) + step, size)


def send(source, target, sends, recvs, axis, peer):
    copy = pltpu.make_async_remote_copy(
        src_ref=source, dst_ref=target, send_sem=sends, recv_sem=recvs,
        device_id={axis: peer}, device_id_type=pl.DeviceIdType.MESH,
    )
    copy.start()
    return copy


def column_of(row, count, first):
    shape = (count, row.shape[1])
    hit = lanes_of(shape) == first + lax.broadcasted_iota(jnp.int32, shape, 0)
    return jnp.sum(jnp.where(hit, row.astype(jnp.float32), 0.0), axis=1, keepdims=True)


def mode_scales(limit_ref, shape, kx, cells_total):
    wide, count, _ = shape
    first = lax.axis_index("chan") * count
    cols = jnp.broadcast_to(column_of(limit_ref[0:1], count, first), (count, LANES))
    rows = jnp.broadcast_to(column_of(limit_ref[1:2], count, first), (count, LANES))
    all_kx = (kx * lax.axis_size("slab"))
    tiles = []
    for j in range(wide):
        cell = lanes_of((count, LANES)) + j * LANES
        col = (lax.axis_index("mode") * (wide * LANES // kx) + cell // kx).astype(jnp.float32)
        row = (lax.axis_index("slab") * kx + cell % kx).astype(jnp.float32)
        kept = (col < cols) & ((row < rows) | (all_kx - row < rows))
        scale = jnp.where(col < 0.5, 1.0, 2.0) / cells_total
        tiles.append(jnp.where(kept, scale, 0.0)[None])
    return jnp.concatenate(tiles, axis=0)


def greet(slabs):
    barrier = pltpu.get_barrier_semaphore()
    targets = [("mode", 1, 2), ("chan", 1, 2)] + [("slab", step, slabs) for step in range(1, slabs)]
    for axis, step, size in targets:
        pl.semaphore_signal(
            barrier, inc=1, device_id={axis: other(axis, step, size)}, device_id_type=pl.DeviceIdType.MESH
        )
    pl.semaphore_wait(barrier, len(targets))


def scatter_sum(part_ref, half_ref, give_ref, take_ref, mode_sems, slab_sems, slabs, between):
    me_mode, me_slab = lax.axis_index("mode"), lax.axis_index("slab")
    peer = other("mode", 1, 2)
    order = [slabs // 2] + [step for step in range(1, slabs) if step != slabs // 2] + [0]
    copies = []
    for step in order:
        slab = other("slab", step, slabs)
        copies.append(send(
            part_ref.at[peer * slabs + slab], half_ref.at[step], mode_sems.at[0, step], mode_sems.at[1, step], "mode", peer
        ))
    waits = list(copies)
    out = []
    for step, copy in zip(order, copies):
        copy.wait_recv()
        slab = other("slab", step, slabs)
        total = part_ref[me_mode * slabs + slab] + half_ref[step]
        if step == 0:
            mine = total
        else:
            give_ref[step] = total
            out.append(send(
                give_ref.at[step], take_ref.at[step], slab_sems.at[0, step], slab_sems.at[1, step], "slab", slab
            ))
    between()
    for copy in out:
        copy.wait_recv()
    for step in range(1, slabs):
        mine = mine + take_ref[step]
    return mine, [copy.wait_send for copy in copies + out]


def gather_start(own_ref, out_ref, mode_sems, slab_sems, slabs):
    me = lax.axis_index("mode") * slabs + lax.axis_index("slab")
    copies = []
    for step in [slabs // 2] + [step for step in range(1, slabs) if step != slabs // 2]:
        copies.append(send(
            own_ref, out_ref.at[me], slab_sems.at[0, step], slab_sems.at[1, step], "slab", other("slab", step, slabs)
        ))
    near = send(own_ref, out_ref.at[me], mode_sems.at[0, 0], mode_sems.at[1, 0], "mode", other("mode", 1, 2))
    out_ref[me] = own_ref[...]
    return copies, near


def gather_finish(state, out_ref, mode_sems, slabs, between):
    copies, near = state
    relays = []
    order = [slabs // 2] + [step for step in range(1, slabs) if step != slabs // 2]
    for k in list(range(1, slabs - 1)) + [0]:
        between(k)
        copies[k].wait_recv()
        step = order[k]
        source = lax.axis_index("mode") * slabs + other("slab", slabs - step, slabs)
        relays.append(send(
            out_ref.at[source], out_ref.at[source], mode_sems.at[0, step], mode_sems.at[1, step], "mode", other("mode", 1, 2)
        ))
    near.wait()
    for copy in relays:
        copy.wait()
    for copy in copies:
        copy.wait_send()


def forward_kernel(
    span, slabs, kx, x_ref, ahead_ref, row_ref, w_ref, limit_ref, mode_limit_ref, out_ref, turned_ref, spec_ref, x_buf, kept_ref,
    part_ref, half_ref, give_ref, take_ref, w_buf, t_buf, sum_ref, peer_ref, own_ref, lines_ref, ahead_buf, row_buf,
    mode_a, slab_a, mode_b, slab_b, chan_sems, x_sems, w_sems, table_sems, t_sems,
):
    ins, freqs, outs = w_ref.shape[0], w_ref.shape[1], w_ref.shape[4]
    rows, cols = x_ref.shape[1:]
    block = LANES // span
    groups = ins // block
    mine_outs = outs // 2
    wide = freqs * kx
    me_mode, me_slab = lax.axis_index("mode"), lax.axis_index("slab")
    peer_mode = other("mode", 1, 2)
    first = lax.axis_index("chan") * ins
    tables = [
        pltpu.make_async_copy(ahead_ref.at[me_mode], ahead_buf, table_sems.at[0]),
        pltpu.make_async_copy(row_ref.at[me_slab], row_buf, table_sems.at[1]),
    ]
    tables[0].start()

    def x_copy(k):
        here = pl.ds(k * (block // 2), block // 2)
        return pltpu.make_async_copy(x_ref.at[here], x_buf.at[here], x_sems.at[k])

    def w_copy(g):
        here = pl.ds(g * block, block)
        return pltpu.make_async_copy(w_ref.at[here], w_buf.at[here], w_sems.at[g])

    for g in range(2):
        x_copy(2 * g).start()
        x_copy(2 * g + 1).start()
        if g == 0:
            tables[1].start()
    greet(slabs)

    def t_copy(g):
        here = pl.ds(g * block, block)
        return pltpu.make_async_copy(t_buf.at[here], turned_ref.at[here], t_sems.at[g])

    def place(g):
        return pl.ds(pl.multiple_of(g * kx, kx), kx)

    def mode_copy(g):
        return pltpu.make_async_remote_copy(
            src_ref=part_ref.at[pl.ds(peer_mode * slabs, slabs), place(g)], dst_ref=half_ref.at[:, place(g)],
            send_sem=mode_a.at[0, g], recv_sem=mode_a.at[1, g],
            device_id={"mode": peer_mode}, device_id_type=pl.DeviceIdType.MESH,
        )

    def slab_copy(step, g):
        return pltpu.make_async_remote_copy(
            src_ref=give_ref.at[step, place(g)], dst_ref=take_ref.at[step, place(g)],
            send_sem=slab_a.at[0, step, g], recv_sem=slab_a.at[1, step, g],
            device_id={"slab": other("slab", step, slabs)}, device_id_type=pl.DeviceIdType.MESH,
        )

    def ahead(g):
        x_copy(2 * g).wait()
        x_copy(2 * g + 1).wait()

        @pl.when(g + 2 < groups)
        def _():
            x_copy(2 * g + 4).start()
            x_copy(2 * g + 5).start()

        @pl.when(g + 2 >= groups)
        def _():
            for k in range(groups // 2):
                w_copy((g + 2 - groups) * (groups // 2) + k).start()
        values = x_buf[pl.ds(g * block, block)].reshape(block * rows, cols)
        lines_ref[...] = two_way(values, ahead_buf[...])

    def finish(g):
        def store(owner, values):
            part_ref[owner, place(g)] = values
        mix_rows(lines_ref, row_buf[...], rows, span, kx, store)

    limit = column_of(limit_ref[...], outs, 0)

    def flip(g):
        for k in range(block):
            i = g * block + k
            keep = jnp.broadcast_to(limit, (outs, wide)) > (first + i).astype(jnp.float32)
            for p in range(2):
                turned = w_buf[i, :, p].reshape(wide, outs).T
                t_buf[i, :, p * wide : (p + 1) * wide] = jnp.where(keep, turned, 0.0)

    def pass_on(g):
        mode_copy(g).wait_recv()
        for step in [slabs // 2] + [step for step in range(1, slabs) if step != slabs // 2]:
            slab = other("slab", step, slabs)
            give_ref[step, place(g)] = part_ref[me_mode * slabs + slab, place(g)] + half_ref[slab, place(g)]
            slab_copy(step, g).start()

    for table in tables:
        table.wait()
    ahead(0)

    def body(g, carry):
        finish(g - 1)
        ahead(g)
        mode_copy(g - 1).start()

        @pl.when(g > 1)
        def _():
            pass_on(g - 2)
        return carry

    lax.fori_loop(1, groups, body, 0)
    finish(groups - 1)
    mode_copy(groups - 1).start()
    pass_on(groups - 2)
    pass_on(groups - 1)
    kept_ref[...] = mode_scales(mode_limit_ref, kept_ref.shape, kx, slabs * rows * 2 * cols)

    def turn_over(g, carry):
        w_copy(g).wait()
        flip(g)
        t_copy(g).start()
        return carry
    lax.fori_loop(0, groups, turn_over, 0)
    mine = part_ref[me_mode * slabs + me_slab] + half_ref[me_slab]

    def landed(g, carry):
        for step in range(1, slabs):
            slab_copy(step, g).wait_recv()
        return carry
    lax.fori_loop(0, groups, landed, 0)
    for step in range(1, slabs):
        mine = mine + take_ref[step]
    to_lanes(mine, spec_ref, kx)

    def contract(i, carry):
        real, imag = carry
        w_real, w_imag = t_buf[i, :, :wide], t_buf[i, :, wide:]
        s_real, s_imag = both_parts(spec_ref, pl.ds(i, 1))
        return real + (s_real * w_real - s_imag * w_imag), imag + (s_real * w_imag + s_imag * w_real)

    zero = jnp.zeros((outs, wide), jnp.float32)
    real, imag = lax.fori_loop(0, ins, contract, (zero, zero))
    put_part(sum_ref, slice(None), 0, real)
    put_part(sum_ref, slice(None), 1, imag)
    theirs = other("chan", 1, 2) * mine_outs
    swap = send(
        sum_ref.at[:, pl.ds(theirs, mine_outs)], peer_ref, chan_sems.at[0], chan_sems.at[1], "chan", other("chan", 1, 2)
    )
    swap.wait_recv()
    for j in range(peer_ref.shape[0]):
        peer_ref[j] = (sum_ref[j, pl.ds(first, mine_outs)] + peer_ref[j]) * kept_ref[j % kept_ref.shape[0]]
    own_ref[...] = to_rows(peer_ref, mine_outs // 8, kx)
    state = gather_start(own_ref, out_ref, mode_b, slab_b, slabs)
    gather_finish(state, out_ref, mode_b, slabs, lambda k: None)
    swap.wait_send()

    def settle(g, carry):
        t_copy(g).wait()
        mode_copy(g).wait_send()
        for step in range(1, slabs):
            slab_copy(step, g).wait_send()
        return carry
    lax.fori_loop(0, groups, settle, 0)


def backward_kernel(
    slabs, kx, part_ref, sums_ref, turned_ref, weight_ref, out_ref, grad_ref, total_ref,
    half_ref, give_ref, take_ref, t_buf, back_ref, own_ref, near_ref, far_ref, pass_ref,
    mode_a, slab_a, mode_b, slab_b, chan_sems, sum_mode, sum_slab, t_sem,
):
    ins, outs, wide = t_buf.shape[0], t_buf.shape[1], t_buf.shape[2] // 2
    mine_outs = outs // 2
    load = pltpu.make_async_copy(turned_ref, t_buf, t_sem)
    load.start()
    greet(slabs)
    first = lax.axis_index("chan") * ins
    near = send(sums_ref, near_ref, sum_mode.at[0], sum_mode.at[1], "mode", other("mode", 1, 2))

    far = []
    def total_up():
        near.wait_recv()
        pass_ref[...] = sums_ref[...] + near_ref[...]
        for step in range(1, slabs):
            far.append(send(
                pass_ref, far_ref.at[step], sum_slab.at[0, step], sum_slab.at[1, step], "slab", other("slab", step, slabs)
            ))

    mine, sent = scatter_sum(part_ref, half_ref, give_ref, take_ref, mode_a, slab_a, slabs, total_up)
    to_lanes(mine, back_ref, kx)
    here = pl.ds(first, mine_outs)
    for j in range(back_ref.shape[0]):
        grad_ref[j, here] = back_ref[j] * weight_ref[j % weight_ref.shape[0]]
    swap = send(
        grad_ref.at[:, here], grad_ref.at[:, here], chan_sems.at[0], chan_sems.at[1], "chan", other("chan", 1, 2)
    )
    load.wait()
    swap.wait_recv()

    def pull(i, carry):
        w_real, w_imag = t_buf[i, :, :wide], t_buf[i, :, wide:]
        g_real, g_imag = both_parts(grad_ref, slice(None))
        put_part(back_ref, pl.ds(i, 1), 0, jnp.sum(g_real * w_real + g_imag * w_imag, axis=0, keepdims=True))
        put_part(back_ref, pl.ds(i, 1), 1, jnp.sum(g_imag * w_real - g_real * w_imag, axis=0, keepdims=True))
        return carry
    lax.fori_loop(0, ins, pull, 0)
    own_ref[...] = to_rows(back_ref, ins // 8, kx)
    state = gather_start(own_ref, out_ref, mode_b, slab_b, slabs)
    gather_finish(state, out_ref, mode_b, slabs, lambda k: None)
    total = pass_ref[...]
    for step, copy in zip(range(1, slabs), far):
        copy.wait()
        total = total + far_ref[step]
    total_ref[...] = total
    near.wait_send()
    swap.wait_send()
    for wait in sent:
        wait()


def fits(shapes, mesh_sizes):
    channels, rows, cols = shapes[0]
    outs, freqs, kx = shapes[2][1], shapes[2][2], shapes[2][4]
    slabs, modes, chans = mesh_sizes
    return (
        modes == 2 and chans == 2 and slabs > 2 and slabs % 2 == 0
        and 8 * kx == LANES and 8 * freqs == LANES and 2 * freqs * channels == 8 * LANES
        and outs == chans * channels
        and rows % LANES == 0 and cols % LANES == 0
    )


def local(source_field, cotangent, spectral_weight, skip_gain, channel_bias, mode_limit, width_limit):
    slabs, modes, chans = (lax.axis_size(axis) for axis in ("slab", "mode", "chan"))
    args = (source_field, cotangent, spectral_weight, skip_gain, channel_bias, mode_limit, width_limit)
    if not fits([one.shape for one in args], (slabs, modes, chans)):
        return local_plain(*args)
    channels, rows, cols = source_field.shape
    outs, freqs, kx = spectral_weight.shape[1], spectral_weight.shape[2], spectral_weight.shape[4]
    span = 2 * freqs
    block = LANES // span
    groups = channels // block
    owners = slabs * modes
    all_kx, all_rows, all_cols = kx * slabs, rows * slabs, cols * modes
    wide = freqs * kx
    ahead, row_ahead, row_behind, behind = (
        jnp.asarray(t) for t in packed_tables(all_rows, all_cols, slabs, modes, freqs, all_kx)
    )

    def pick(table, axis):
        return pl.BlockSpec((1,) + table.shape[1:], lambda g: (lax.axis_index(axis), 0, 0))

    cells = pl.BlockSpec((block, rows, cols), lambda g: (g, 0, 0))
    scalars = pl.BlockSpec(memory_space=pltpu.SMEM)
    field = jax.ShapeDtypeStruct(source_field.shape, jnp.float32)
    room = lambda size: pltpu.CompilerParams(dimension_semantics=("arbitrary",), vmem_limit_bytes=size * MIB)
    f32 = jnp.float32

    weight = spectral_weight.transpose(0, 2, 3, 4, 1)
    limit = width_limit.reshape(1, outs)

    dma, vmem = pltpu.SemaphoreType.DMA, pltpu.VMEM
    in_vmem, anywhere = pl.BlockSpec(memory_space=pltpu.VMEM), pl.BlockSpec(memory_space=pl.ANY)
    piece = (groups * kx, LANES)
    common = [vmem((slabs,) + piece, f32), vmem((slabs,) + piece, f32), vmem((slabs,) + piece, f32)]
    pair = [dma((2, slabs))] * 4
    comm = lambda ident, room: pltpu.CompilerParams(
        collective_id=ident, has_side_effects=True, vmem_limit_bytes=room * MIB
    )
    flat = lambda lines: (2 * wide // LANES, lines, LANES)

    in_hbm = lambda array: pltpu.with_memory_space_constraint(array, pltpu.HBM)
    held = lambda array: pltpu.with_memory_space_constraint(array, pltpu.VMEM)
    modes_shape = (owners,) + piece
    out_modes, turned, spec, source_held, weights = pl.pallas_call(
        functools.partial(forward_kernel, span, slabs, kx),
        in_specs=[anywhere, anywhere, anywhere, anywhere, in_vmem, in_vmem],
        out_specs=[in_vmem, anywhere, in_vmem, in_vmem, in_vmem],
        out_shape=[
            jax.ShapeDtypeStruct(modes_shape, f32), pltpu.HBM((channels, outs, 2 * wide), f32),
            jax.ShapeDtypeStruct(flat(channels), f32), pltpu.VMEM(field.shape, f32),
            jax.ShapeDtypeStruct((wide // LANES, channels, LANES), f32),
        ],
        scratch_shapes=[vmem(modes_shape, f32)] + common + [
            vmem(weight.shape, f32), vmem((channels, outs, 2 * wide), f32), vmem(flat(outs), f32), vmem(flat(outs // 2), f32), vmem(piece, f32),
            vmem((block * rows, LANES), f32), vmem(ahead.shape[1:], jnp.bfloat16), vmem(row_ahead.shape[1:], jnp.bfloat16),
            dma((2, groups)), dma((2, slabs, groups)), dma((2, slabs)), dma((2, slabs)), dma((2,)),
            dma((2 * groups,)), dma((groups,)), dma((2,)), dma((groups,)),
        ],
        compiler_params=comm(20, FORWARD),
        name="forward_modes",
    )(in_hbm(source_field), in_hbm(ahead), in_hbm(row_ahead), in_hbm(weight), limit, mode_limit.T)

    output, grad_sum, grad_partial, sums = pl.pallas_call(
        functools.partial(middle_packed, span, kx),
        grid=(groups,),
        in_specs=[
            in_vmem, cells, in_vmem, scalars, scalars, pick(ahead, "mode"), pick(row_ahead, "slab"),
            pick(row_behind, "slab"), pick(behind, "mode"),
        ],
        out_specs=[cells, in_vmem, in_vmem, in_vmem],
        out_shape=[field, pltpu.VMEM(field.shape, f32), jax.ShapeDtypeStruct(modes_shape, f32), jax.ShapeDtypeStruct((8, LANES), f32)],
        scratch_shapes=[
            vmem((2, block // 2, 2 * rows, cols), jnp.bfloat16), vmem((block * rows, LANES), f32), vmem((block, rows, cols), f32),
            vmem((block, rows, LANES), f32), vmem((block, rows, LANES), f32), vmem((block * rows, LANES), f32),
        ],
        input_output_aliases={0: 1},
        compiler_params=room(MIDDLE),
        name="middle",
    )(
        held(source_held), cotangent, out_modes, skip_gain, channel_bias,
        ahead, row_ahead, row_behind, behind,
    )

    back_modes, all_grads, totals = pl.pallas_call(
        functools.partial(backward_kernel, slabs, kx),
        in_specs=[in_vmem, in_vmem, anywhere, in_vmem],
        out_specs=[in_vmem] * 3,
        out_shape=[pltpu.HBM(modes_shape, f32), pltpu.HBM(flat(outs), f32), pltpu.HBM((8, LANES), f32)],
        scratch_shapes=common + [
            vmem((channels, outs, 2 * wide), f32), vmem(flat(channels), f32), vmem(piece, f32), vmem((8, LANES), f32),
            vmem((slabs, 8, LANES), f32), vmem((8, LANES), f32),
        ] + pair + [dma((2,)), dma((2,)), dma((2, slabs)), dma],
        compiler_params=comm(21, BACKWARD),
        name="backward_modes",
    )(in_hbm(grad_partial), in_hbm(sums), in_hbm(turned), in_hbm(weights))

    count = channels // groups
    whole = lambda array: pl.BlockSpec(array.shape, lambda g: (0,) * len(array.shape))
    line = jax.ShapeDtypeStruct((1, channels), f32)
    field_grad, weight_grad, gate_grad, bias_grad = pl.pallas_call(
        functools.partial(last_packed, span, kx),
        grid=(groups,),
        in_specs=[
            in_vmem, in_vmem, scalars, pick(row_behind, "slab"), pick(behind, "mode"),
            whole(all_grads), whole(spec), whole(limit), whole(totals),
        ],
        out_specs=[cells, pl.BlockSpec((count,) + weight.shape[1:], lambda g: (g, 0, 0, 0, 0)), whole(line), whole(line)],
        out_shape=[field, jax.ShapeDtypeStruct(weight.shape, f32), line, line],
        compiler_params=room(LAST),
        name="last",
    )(
        pltpu.with_memory_space_constraint(grad_sum, pltpu.VMEM), back_modes, skip_gain,
        row_behind, behind, all_grads, spec, limit, totals,
    )
    spectral_grad = weight_grad.transpose(0, 4, 1, 2, 3)
    return (output, field_grad, spectral_grad, gate_grad.reshape(-1), bias_grad.reshape(-1))


def solution(mesh):
    in_specs = (
        P(("member", "chan"), "slab", "mode"),
        P(("member", "chan"), "slab", "mode"),
        P(("member", "chan"), None, "mode", None, "slab"),
        P(("member", "chan")),
        P(("member", "chan")),
        P("member", None),
        P("member"),
    )
    out_specs = (
        P(("member", "chan"), "slab", "mode"),
        P(("member", "chan"), "slab", "mode"),
        P(("member", "chan"), None, "mode", None, "slab"),
        P(("member", "chan")),
        P(("member", "chan")),
    )
    return jax.shard_map(local, mesh=mesh, in_specs=in_specs, out_specs=out_specs, check_vma=False)
```
